768 devices in a mesh: lat: 96 (over y, z_hi, x), lon: 8 (over z_lo, core).
Axes of the slice: x: 4, y: 8, z: 12 (z_hi: 3, z_lo: 4; z = z_hi * 4 + z_lo), core: 2. Of those that a mesh axis runs over, the one named last changes fastest.
Arguments:
- right_side: float32 [1536, 5120], P('lat', 'lon'), may hold values from -34 to 34
- first_guess: float32 [1536, 5120], P('lat', 'lon'), may hold values from -3 to 3
- cell_mask: int32 [1536, 5120], P('lat', 'lon'), may hold values 0 or 1
- cond_east: float32 [1536, 5120], P('lat', 'lon'), may hold values from 0.5 to 2
- cond_north: float32 [1536, 5120], P('lat', 'lon'), may hold values from 0.5 to 2
- surface: float32 [1536, 5120], P('lat', 'lon'), may hold values from 0.02 to 0.5
- recycled: float32 [16, 1536, 5120], P(None, 'lat', 'lon'), may hold values from -0.0006418624 to 0.0006418624
Outputs:
- solution: float32 [1536, 5120], P('lat', 'lon')
- residual: float32 [1536, 5120], P('lat', 'lon')
The draws below stay inside these ranges and needn't reach their ends.
All inputs are finite; a program needn't handle non-finite values. No bound on the sum of `cell_mask` on one device may be relied on, other than what follows from the above.
Results may differ from the reference program's by a relative error of at most 0.0003.
Values sent between devices are 32-bit elements; how exact they have to be, the bound alone decides.
A program may use at most 32 MiB of HBM per device.

```python
import math
import jax
import jax.numpy as jnp
from jax import lax

K = 16
ITERS = 3
NY = 1536
NX = 5120


def basis_and_source(key):
    cells = NY * NX
    base = jax.random.fold_in(key, 7)
    key_phase, key_basis, key_weight, key_noise = jax.random.split(base, 4)
    phases = jax.random.uniform(key_phase, (2, K), jnp.float32, -3.1415927, 3.1415927)
    vector_index = jnp.arange(K)
    lat_wave = (vector_index % 4 + 1).astype(jnp.float32)
    lon_wave = (vector_index // 4 % 4).astype(jnp.float32)
    row_place = (jnp.arange(NY).astype(jnp.float32) + 0.5) / NY
    column_place = jnp.arange(NX).astype(jnp.float32) / NX
    lat_part = jnp.cos(3.1415927 * lat_wave[:, None] * row_place[None, :] + phases[0][:, None])
    lon_part = jnp.cos(6.2831853 * lon_wave[:, None] * column_place[None, :] + phases[1][:, None])
    pattern = lat_part[:, :, None] * lon_part[:, None, :]
    roughness = jnp.clip(jax.random.normal(key_basis, (K, NY, NX), jnp.float32), -4.0, 4.0)
    weights = jnp.clip(jax.random.normal(key_weight, (K,), jnp.float32), -2.5, 2.5) * 0.4
    noise = jnp.clip(jax.random.normal(key_noise, (NY, NX), jnp.float32), -4.0, 4.0)
    basis = pattern + 0.2 * roughness
    root = jnp.sqrt(jnp.float32(cells))
    source = noise + jnp.einsum('k,kyx->yx', weights, basis)
    return (basis / root, source)


def draw_recycled(key, part):
    return basis_and_source(key)[0].astype(jnp.float32)


def draw_right_side(key, part):
    return basis_and_source(key)[1].astype(jnp.float32)


def touch_ends(entries, own_key, low, high):
    longest = entries.shape.index(max(entries.shape))
    spots = []
    for shift in (0, 1):
        where = [jax.random.randint(jax.random.fold_in(own_key, axis), (), 0, length) for axis, length in enumerate(entries.shape)]
        where[longest] = (where[longest] + shift) % entries.shape[longest]
        spots.append(tuple(where))
    return entries.at[spots[0]].set(low).at[spots[1]].set(high)


def block_levels(rng, shape, cuts, low, top_value):
    gain = 1.0
    for axis_at, blocks in cuts:
        heights = jax.random.uniform(jax.random.fold_in(jax.random.fold_in(rng, 6), axis_at), (blocks,), jnp.float32, low / len(cuts), top_value / len(cuts))
        gain = gain * jnp.repeat(jnp.exp(heights), shape[axis_at] // blocks).reshape((-1,) + (1,) * (len(shape) - 1 - axis_at))
    return gain


def scatter_about(key, shape, width, bound, pieces=(), held_as=jnp.bfloat16):
    array = jax.random.normal(key, shape, jnp.float32) * width
    if len(pieces) > 0:
        array = block_levels(key, shape, pieces, -0.22, 0.18) * array
    return jnp.clip(array, min=-bound, max=bound).astype(held_as)


def setup_inputs(seed: int = 0) -> dict:
    key_of = jax.random.split(jax.random.key(seed), 8)
    right_side = draw_right_side(jax.random.fold_in(key_of[7], 71), 0)
    first_guess = scatter_about(key_of[1], (NY, NX), 0.5, 3.0, ((0, 96), (1, 8)), jnp.float32)
    cell_mask = touch_ends((jax.random.randint(key_of[2], (NY, NX), 0, 4) < 3).astype(jnp.int32), jax.random.fold_in(key_of[2], 1), 0, 1)
    cond_east = jnp.clip(jnp.exp(math.log(2.0) - 1.3862944 * jax.random.uniform(key_of[3], (NY, NX), jnp.float32) ** block_levels(key_of[3], (NY, NX), ((0, 96), (1, 8)), -0.2, 0.2)), 0.5, 2.0)
    cond_north = jnp.clip(jnp.exp(math.log(2.0) - 1.3862944 * jax.random.uniform(key_of[4], (NY, NX), jnp.float32) ** block_levels(key_of[4], (NY, NX), ((0, 96), (1, 8)), -0.2, 0.2)), 0.5, 2.0)
    surface = jnp.clip(jnp.exp(math.log(0.5) - 3.218876 * jax.random.uniform(key_of[5], (NY, NX), jnp.float32) ** block_levels(key_of[5], (NY, NX), ((0, 96), (1, 8)), -0.2, 0.2)), 0.02, 0.5)
    recycled = draw_recycled(jax.random.fold_in(key_of[7], 71), 0)
    return dict(right_side=right_side, first_guess=first_guess, cell_mask=cell_mask, cond_east=cond_east, cond_north=cond_north, surface=surface, recycled=recycled)


PRECISE = lax.Precision.HIGHEST

def neighbours(values):
    to_east = jnp.roll(values, -1, axis=-1)
    to_west = jnp.roll(values, 1, axis=-1)
    zero_row = jnp.zeros_like(values[..., :1, :])
    to_north = jnp.concatenate([values[..., 1:, :], zero_row], axis=-2)
    to_south = jnp.concatenate([zero_row, values[..., :-1, :]], axis=-2)
    return (to_east, to_west, to_north, to_south)

def faces(cell_mask, cond_east, cond_north, surface):
    wet_cells = cell_mask.astype(jnp.float32)
    wet_east = cond_east * wet_cells
    wet_north = cond_north * wet_cells
    ocean_e, ocean_w, ocean_n, ocean_s = neighbours(wet_cells)
    k_east = wet_east * ocean_e
    k_west = neighbours(wet_east)[1] * wet_cells
    k_north = wet_north * ocean_n
    k_south = neighbours(wet_north)[3] * wet_cells
    centre = surface * wet_cells + k_east + k_west + k_north + k_south + (1.0 - wet_cells)
    return (centre, k_east, k_west, k_north, k_south)

def operate(values, coeffs):
    centre, k_east, k_west, k_north, k_south = coeffs
    to_east, to_west, to_north, to_south = neighbours(values)
    return centre * values - (k_east * to_east + k_west * to_west + k_north * to_north + k_south * to_south)

def solve_small(factor, target):
    return jax.scipy.linalg.cho_solve((factor, True), target)

def reference(right_side, first_guess, cell_mask, cond_east, cond_north, surface, recycled):
    coeffs = faces(cell_mask, cond_east, cond_north, surface)
    basis_image = lax.map(lambda vector: operate(vector, coeffs), recycled)
    start_res = right_side - operate(first_guess, coeffs)
    gram = jnp.einsum('kyx,lyx->kl', recycled, basis_image, precision=PRECISE)
    start = jnp.einsum('kyx,yx->k', recycled, start_res, precision=PRECISE)
    factor = jnp.linalg.cholesky(0.5 * (gram + gram.T))
    coarse = solve_small(factor, start)
    solution = first_guess + jnp.einsum('kyx,k->yx', recycled, coarse, precision=PRECISE)
    residual = start_res - jnp.einsum('kyx,k->yx', basis_image, coarse, precision=PRECISE)
    direction = residual
    dir_image = residual
    curv = jnp.float32(1.0)
    prev_norm = jnp.float32(1.0)
    for turn_index in range(ITERS):
        image_res = operate(residual, coeffs)
        res_norm = jnp.sum(residual * residual)
        res_image = jnp.sum(residual * image_res)
        defl = jnp.einsum('kyx,yx->k', basis_image, residual, precision=PRECISE)
        coef = solve_small(factor, defl)
        along_basis = jnp.einsum('kyx,k->yx', recycled, coef, precision=PRECISE)
        along_image = jnp.einsum('kyx,k->yx', basis_image, coef, precision=PRECISE)
        if turn_index == 0:
            direction = residual - along_basis
            dir_image = image_res - along_image
            curv = res_image - jnp.sum(coef * defl)
        else:
            ratio = res_norm / prev_norm
            direction = residual - along_basis + ratio * direction
            dir_image = image_res - along_image + ratio * dir_image
            curv = res_image - jnp.sum(coef * defl) - ratio * ratio * curv
        step_len = res_norm / curv
        solution = solution + step_len * direction
        residual = residual - step_len * dir_image
        prev_norm = res_norm
    return (solution, residual)
```

```python
import functools

import jax
import jax.numpy as jnp
from jax import lax
from jax.experimental import pallas as pl
from jax.experimental.pallas import tpu as pltpu
from jax.sharding import Mesh
from jax.sharding import PartitionSpec as P

LAT = ("lat_0", "lat_1", "lat_2")
LON = ("lon_0", "lon_1")
AXES = LAT + LON
MESH = pl.DeviceIdType.MESH
HIGHEST = lax.Precision.HIGHEST

K = 16
DEPTH = 4
NY = 16
NX = 640
WIDE = NX + 128
ROWS = NY + 2 * DEPTH
NAT = NY + 16
WET, EAST, NORTH, SURF, RHS, GUESS = range(6)

f32 = jnp.float32


def far_first(n):
    return sorted(range(1, n), key=lambda d: -min(d, n - d))


def iota(shape, axis):
    return lax.broadcasted_iota(jnp.int32, shape, axis)


def kernel(
    sizes,
    rhs_hbm,
    guess_hbm,
    mask_hbm,
    east_hbm,
    north_hbm,
    surf_hbm,
    rec_hbm,
    x_out,
    r_out,
    vec,
    img1,
    img2,
    img3,
    nat,
    cen,
    ke,
    kw,
    kn,
    ks,
    st,
    res,
    mask_v,
    pack_vec,
    got_vec,
    pack_nat,
    got_nat,
    grams,
    ar_send,
    ar_a,
    ar_b,
    ar_c,
    comb,
    in_sem,
    halo_send,
    halo_recv,
    ssem_a,
    ssem_b,
    ssem_c,
    rsem_a,
    rsem_b,
    rsem_c,
):
    ny_dev, nzh, nx_dev, nzl, ncore = sizes
    my_y = lax.axis_index("lat_0")
    my_zh = lax.axis_index("lat_1")
    my_x = lax.axis_index("lat_2")
    my_zl = lax.axis_index("lon_0")
    my_c = lax.axis_index("lon_1")
    n_lat = ny_dev * nzh * nx_dev
    n_lon = nzl * ncore
    my_lat = (my_y * nzh + my_zh) * nx_dev + my_x
    my_lon = my_zl * ncore + my_c
    na, nb, nc = nx_dev * ncore, ny_dev, nzh * nzl
    my_a = my_x * ncore + my_c
    my_z = my_zh * nzl + my_zl

    def at_lat(index):
        index = lax.rem(index + n_lat, n_lat)
        rest = index // nx_dev
        return (rest // nzh, lax.rem(rest, nzh), lax.rem(index, nx_dev), my_zl, my_c)

    def at_lon(index):
        index = lax.rem(index + n_lon, n_lon)
        return (my_y, my_zh, my_x, index // ncore, lax.rem(index, ncore))

    def at_a(index):
        return (my_y, my_zh, index // ncore, my_zl, lax.rem(index, ncore))

    def at_b(index):
        return (index, my_zh, my_x, my_zl, my_c)

    def at_c(index):
        return (my_y, index // nzl, my_x, lax.rem(index, nzl), my_c)

    plain = (
        (east_hbm, EAST),
        (north_hbm, NORTH),
        (surf_hbm, SURF),
        (rhs_hbm, RHS),
        (guess_hbm, GUESS),
    )
    loads = [pltpu.make_async_copy(mask_hbm, mask_v, in_sem.at[0])]
    for i, (src, field) in enumerate(plain):
        loads.append(
            pltpu.make_async_copy(
                src, nat.at[field, pl.ds(8, NY), pl.ds(0, NX)], in_sem.at[1 + i]
            )
        )
    for k in range(K):
        loads.append(
            pltpu.make_async_copy(
                rec_hbm.at[k], vec.at[pl.ds(DEPTH, NY), k, pl.ds(0, NX)], in_sem.at[6 + k]
            )
        )
    for load in loads:
        load.start()

    nat[:, 0:8, :] = jnp.zeros((6, 8, WIDE), f32)
    nat[:, 24:32, :] = jnp.zeros((6, 8, WIDE), f32)
    nat[:, 8:24, NX:] = jnp.zeros((6, NY, 128), f32)
    res[...] = jnp.zeros(res.shape, f32)

    barrier = pltpu.get_barrier_semaphore()
    peers = [at_lat(my_lat + 1), at_lat(my_lat - 1), at_lon(my_lon + 1), at_lon(my_lon - 1)]
    for n, me, at in ((nc, my_z, at_c), (nb, my_y, at_b), (na, my_a, at_a)):
        for d in far_first(n):
            peers.append(at(lax.rem(me + d, n)))
    for peer in peers:
        pl.semaphore_signal(barrier, inc=1, device_id=peer, device_id_type=MESH)
    for load in loads:
        load.wait()
    nat[WET, 8:24, 0:NX] = mask_v[...].astype(f32)
    pl.semaphore_wait(barrier, len(peers))

    def remote(src, dst, at, slot):
        return pltpu.make_async_remote_copy(
            src_ref=src,
            dst_ref=dst,
            send_sem=halo_send.at[slot],
            recv_sem=halo_recv.at[slot],
            device_id=at,
            device_id_type=MESH,
        )

    north_of, south_of = at_lat(my_lat + 1), at_lat(my_lat - 1)
    east_of, west_of = at_lon(my_lon + 1), at_lon(my_lon - 1)
    lanes = pl.ds(0, NX)
    lat_copies = [
        remote(
            vec.at[pl.ds(NY, DEPTH), :, lanes], vec.at[pl.ds(0, DEPTH), :, lanes], north_of, 0
        ),
        remote(
            vec.at[pl.ds(DEPTH, DEPTH), :, lanes],
            vec.at[pl.ds(NY + DEPTH, DEPTH), :, lanes],
            south_of,
            1,
        ),
        remote(
            nat.at[:, pl.ds(20, DEPTH), lanes], nat.at[:, pl.ds(4, DEPTH), lanes], north_of, 2
        ),
        remote(
            nat.at[:, pl.ds(8, DEPTH), lanes], nat.at[:, pl.ds(24, DEPTH), lanes], south_of, 3
        ),
    ]
    for copy in lat_copies:
        copy.start()
    for copy in lat_copies:
        copy.wait()

    lane16 = iota((K, 128), 1)

    def pack_row(e, carry):
        to_west, to_east = carry
        mine = (lane16 >= DEPTH * e) & (lane16 < DEPTH * e + DEPTH)
        first = pltpu.roll(vec[e, :, 0:128], DEPTH * e, 1)
        last = pltpu.roll(vec[e, :, NX - 128 : NX], lax.rem(DEPTH * e + DEPTH, 128), 1)
        return jnp.where(mine, first, to_west), jnp.where(mine, last, to_east)

    zero16 = jnp.zeros((K, 128), f32)
    to_west, to_east = lax.fori_loop(0, ROWS, pack_row, (zero16, zero16))
    pack_vec[0] = to_west
    pack_vec[1] = to_east
    lane_n = iota((NAT, 128), 1)
    west_n = jnp.zeros((NAT, 128), f32)
    east_n = jnp.zeros((NAT, 128), f32)
    for i in range(6):
        mine = (lane_n >= DEPTH * i) & (lane_n < DEPTH * i + DEPTH)
        first = nat[i, :, 0:128]
        if i:
            first = pltpu.roll(first, DEPTH * i, 1)
        last = pltpu.roll(nat[i, :, NX - 128 : NX], DEPTH * i + DEPTH, 1)
        west_n = jnp.where(mine, first, west_n)
        east_n = jnp.where(mine, last, east_n)
    pack_nat[0] = west_n
    pack_nat[1] = east_n
    lon_copies = [
        remote(pack_vec.at[0], got_vec.at[0], west_of, 4),
        remote(pack_vec.at[1], got_vec.at[1], east_of, 5),
        remote(pack_nat.at[0], got_nat.at[0], west_of, 6),
        remote(pack_nat.at[1], got_nat.at[1], east_of, 7),
    ]
    for copy in lon_copies:
        copy.start()
    for copy in lon_copies:
        copy.wait()

    def unpack_row(e, carry):
        from_east = pltpu.roll(got_vec[0], lax.rem(128 - DEPTH * e, 128), 1)
        from_west = pltpu.roll(got_vec[1], 128 - DEPTH - DEPTH * e, 1)
        vec[e, :, NX:] = jnp.where(
            lane16 < DEPTH, from_east, jnp.where(lane16 >= 128 - DEPTH, from_west, 0.0)
        )
        return carry

    lax.fori_loop(0, ROWS, unpack_row, 0)
    for i in range(6):
        from_east = got_nat[0]
        if i:
            from_east = pltpu.roll(from_east, 128 - DEPTH * i, 1)
        from_west = pltpu.roll(got_nat[1], 128 - DEPTH - DEPTH * i, 1)
        nat[i, :, NX:] = jnp.where(
            lane_n < DEPTH, from_east, jnp.where(lane_n >= 128 - DEPTH, from_west, 0.0)
        )

    row_n = iota((NAT, WIDE), 0)
    beyond = ((row_n < 8) & (my_lat == 0)) | ((row_n >= 24) & (my_lat == n_lat - 1))

    def east(v):
        return pltpu.roll(v, WIDE - 1, 1)

    def west(v):
        return pltpu.roll(v, 1, 1)

    def north(v):
        return pltpu.roll(v, NAT - 1, 0)

    def south(v):
        return pltpu.roll(v, 1, 0)

    wet = jnp.where(beyond, 0.0, nat[WET])
    k_east = nat[EAST] * wet * east(wet)
    k_north = nat[NORTH] * wet * north(wet)
    k_west = west(k_east)
    k_south = south(k_north)
    ke[...] = k_east
    kw[...] = k_west
    kn[...] = k_north
    ks[...] = k_south
    cen[...] = nat[SURF] * wet + k_east + k_west + k_north + k_south + (1.0 - wet)

    def operate(v):
        return cen[...] * v - (
            ke[...] * east(v) + kw[...] * west(v) + kn[...] * north(v) + ks[...] * south(v)
        )

    def operate_vectors(src, dst, first, last):
        def row(e, carry):
            at = pl.ds(e + 4, 1)
            v = src[e]
            dst[e] = cen[at, :] * v - (
                ke[at, :] * east(v)
                + kw[at, :] * west(v)
                + kn[at, :] * src[e + 1]
                + ks[at, :] * src[e - 1]
            )
            return carry

        lax.fori_loop(first, last + 1, row, 0)

    st[...] = nat[RHS] - operate(nat[GUESS])
    operate_vectors(vec, img1, 1, 22)
    operate_vectors(img1, img2, 3, 20)
    operate_vectors(img2, img3, 4, 19)

    def fold(v):
        total = v[:, 0:128]
        for i in range(1, NX // 128):
            total = total + v[:, 128 * i : 128 * i + 128]
        return total

    def gram_row(y, carry):
        acc, start = carry
        e = y + DEPTH
        w, b1, b2, b3 = (ref[e, :, 0:NX] for ref in (vec, img1, img2, img3))
        left = jnp.concatenate([w, b1, b2], axis=0)
        right = jnp.concatenate([w, b1, b2, b3], axis=0)
        acc = acc + lax.dot_general(
            left, right, (((1,), (1,)), ((), ())), precision=HIGHEST, preferred_element_type=f32
        )
        return acc, start + fold(w * st[pl.ds(y + 8, 1), 0:NX])

    acc, start = lax.fori_loop(0, NY, gram_row, (jnp.zeros((3 * K, 4 * K), f32), zero16))
    grams[...] = jnp.zeros(grams.shape, f32)
    grams[:, 0 : 4 * K] = acc

    def block(i, j, lane):
        v = grams[K * i : K * i + K, :]
        v = jnp.where((lane16 >= K * j) & (lane16 < K * j + K), v, 0.0)
        shift = (lane - K * j) % 128
        return pltpu.roll(v, shift, 1) if shift else v

    payload = 0.5 * (block(0, 1, 0) + block(1, 0, 0))
    payload = payload + block(1, 1, 16) + block(1, 2, 32) + block(2, 2, 48) + block(2, 3, 64)
    payload = jnp.where(lane16 == 80, jnp.sum(start, axis=1, keepdims=True), payload)

    def phase(turn, step, value, buf, ssem, rsem, n, me, at):
        ar_send[turn, step] = value
        buf[turn, me] = value
        for d in far_first(n):
            pltpu.make_async_remote_copy(
                src_ref=ar_send.at[turn, step],
                dst_ref=buf.at[turn, me],
                send_sem=ssem.at[turn, d],
                recv_sem=rsem.at[turn, me],
                device_id=at(lax.rem(me + d, n)),
                device_id_type=MESH,
            ).start()
        for d in range(1, n):
            peer = lax.rem(me + d, n)
            pltpu.make_async_remote_copy(
                src_ref=ar_send.at[turn, step],
                dst_ref=buf.at[turn, peer],
                send_sem=ssem.at[turn, d],
                recv_sem=rsem.at[turn, peer],
                device_id=at(peer),
                device_id_type=MESH,
            ).wait()
        total = buf[turn, 0]
        for i in range(1, n):
            total = total + buf[turn, i]
        return total

    def all_reduce(turn, value):
        value = phase(turn, 0, value, ar_a, ssem_a, rsem_a, na, my_a, at_a)
        value = phase(turn, 1, value, ar_b, ssem_b, rsem_b, nb, my_y, at_b)
        return phase(turn, 2, value, ar_c, ssem_c, rsem_c, nc, my_z, at_c)

    sums = all_reduce(0, payload)

    sub16 = iota((K, 128), 0)
    aug = jnp.where(lane16 < K, sums, 0.0)
    aug = jnp.where(lane16 == sub16 + K, 1.0, aug)
    aug = jnp.where(lane16 == 2 * K, sums[:, 80:81], aug)
    for i in range(K):
        pivot_row = aug[i : i + 1, :] / aug[i : i + 1, i : i + 1]
        aug = jnp.where(sub16 == i, pivot_row, aug - aug[:, i : i + 1] * pivot_row)
    coarse = aug[:, 2 * K : 2 * K + 1]

    def at_zero(v, lane):
        v = jnp.where((lane16 >= lane) & (lane16 < lane + K), v, 0.0)
        return pltpu.roll(v, (128 - lane) % 128, 1) if lane else v

    inverse = at_zero(aug, K)
    g2, g3, g4, g5 = (at_zero(sums, lane) for lane in (16, 32, 48, 64))

    def residual_row(e, carry):
        along = jnp.sum(coarse * img1[e], axis=0, keepdims=True)
        res[0, pl.ds(e + 4, 1), :] = st[pl.ds(e + 4, 1), :] - along
        return carry

    lax.fori_loop(1, 23, residual_row, 0)
    for i in range(3):
        res[i + 1] = operate(res[i])

    def moment_row(y, carry):
        e = y + DEPTH
        b1, b2 = img1[e, :, 0:NX], img2[e, :, 0:NX]
        r0, r1, r2, r3 = (res[i, pl.ds(y + 8, 1), 0:NX] for i in range(4))
        terms = (b1 * r0, b1 * r1, b1 * r2, b2 * r2, b2 * r3)
        return tuple(total + fold(term) for total, term in zip(carry, terms))

    defl = lax.fori_loop(0, NY, moment_row, (zero16,) * 5)
    payload = zero16
    for i, total in enumerate(defl):
        payload = jnp.where(lane16 == i, jnp.sum(total, axis=1, keepdims=True), payload)
    inner = [res[i, 8:24, 0:NX] for i in range(4)]
    for i, (a, b) in enumerate(((0, 0), (0, 1), (1, 1), (1, 2), (2, 2), (2, 3))):
        dot = jnp.sum(fold(inner[a] * inner[b]), axis=1, keepdims=True)
        payload = jnp.where(lane16 == 5 + i, dot, payload)

    sums = all_reduce(1, payload)
    d = [sums[:, i : i + 1] for i in range(5)]
    t = [jnp.sum(sums[:, 5 + i : 6 + i], axis=0, keepdims=True) for i in range(6)]

    def apply(mat, col):
        row = jnp.sum(jnp.where(lane16 == sub16, col, 0.0), axis=0, keepdims=True)
        return jnp.sum(mat * row, axis=1, keepdims=True)

    def dot(a, b):
        return jnp.sum(a * b, axis=0, keepdims=True)

    mu0 = apply(inverse, d[0])
    g2_0, g3_0, g4_0, g5_0 = (apply(g, mu0) for g in (g2, g3, g4, g5))
    defl1 = d[1] - g2_0
    mu1 = apply(inverse, defl1)
    g2_1, g3_1 = apply(g2, mu1), apply(g3, mu1)
    defl2 = d[2] - g3_0 - g2_1
    mu2 = apply(inverse, defl2)
    m = [
        t[0],
        t[1] - dot(mu0, d[0]),
        t[2] - 2.0 * dot(mu0, d[1]) + dot(mu0, g2_0),
        t[3] - 2.0 * dot(mu0, d[2]) + dot(mu0, g3_0) - dot(mu1, defl1),
        t[4]
        - 2.0 * (dot(mu0, d[3]) + dot(mu1, d[2]))
        + dot(mu0, g4_0)
        + 2.0 * dot(mu1, g3_0)
        + dot(mu1, g2_1),
        t[5]
        - 2.0 * (dot(mu0, d[4]) + dot(mu1, d[3]))
        + dot(mu0, g5_0)
        + 2.0 * dot(mu1, g4_0)
        + dot(mu1, g3_1)
        - dot(mu2, defl2),
    ]

    def form(poly, shift):
        total = 0.0
        for i, a in enumerate(poly):
            for j, b in enumerate(poly):
                total = total + a * b * m[i + j + shift]
        return total

    one = jnp.ones((1, 1), f32)
    zero = jnp.zeros((1, 1), f32)
    r_poly = [one]
    y_poly = [zero]
    zeta = [zero, zero, zero]
    curv = prev_norm = one
    for turn in range(3):
        norm = form(r_poly, 0)
        r_image = form(r_poly, 1)
        if turn == 0:
            y_poly = list(r_poly)
            curv = r_image
        else:
            ratio = norm / prev_norm
            y_poly = [a + ratio * b for a, b in zip(r_poly, y_poly + [zero])]
            curv = r_image - ratio * ratio * curv
        step_len = norm / curv
        for i, a in enumerate(y_poly):
            zeta[i] = zeta[i] + step_len * a
        r_poly = [
            a - step_len * b for a, b in zip(r_poly + [zero], [zero] + list(y_poly))
        ]
        prev_norm = norm

    nu2 = zeta[2] * mu0
    nu1 = zeta[1] * mu0 + zeta[2] * mu1
    nu0 = zeta[0] * mu0 + zeta[1] * mu1 + zeta[2] * mu2
    x_w = coarse - nu0

    def final_row(y, carry):
        e = y + DEPTH
        w, b1, b2, b3 = (ref[e, :, 0:NX] for ref in (vec, img1, img2, img3))
        at = pl.ds(y, 1)
        comb[0, at, :] = jnp.sum(x_w * w - nu1 * b1 - nu2 * b2, axis=0, keepdims=True)
        comb[1, at, :] = jnp.sum(nu0 * b1 + nu1 * b2 + nu2 * b3, axis=0, keepdims=True)
        return carry

    lax.fori_loop(0, NY, final_row, 0)
    x_out[...] = (
        nat[GUESS, 8:24, 0:NX]
        + comb[0]
        + (zeta[0] * inner[0] + zeta[1] * inner[1] + zeta[2] * inner[2])
    )
    r_out[...] = inner[0] - (
        zeta[0] * inner[1] + zeta[1] * inner[2] + zeta[2] * inner[3] - comb[1]
    )


def shards(right_side, first_guess, cell_mask, cond_east, cond_north, surface, recycled):
    sizes = tuple(lax.axis_size(axis) for axis in AXES)
    ny_dev, nzh, nx_dev, nzl, ncore = sizes
    na, nb, nc = nx_dev * ncore, ny_dev, nzh * nzl
    field = jax.ShapeDtypeStruct((NY, NX), f32)
    vmem = pltpu.VMEM
    dma = pltpu.SemaphoreType.DMA
    plain = vmem((NAT, WIDE), f32)
    return pl.pallas_call(
        functools.partial(kernel, sizes),
        out_shape=(field, field),
        in_specs=[pl.BlockSpec(memory_space=pl.ANY)] * 7,
        out_specs=(pl.BlockSpec(memory_space=pltpu.VMEM),) * 2,
        scratch_shapes=[vmem((ROWS, K, WIDE), f32)] * 4
        + [vmem((6, NAT, WIDE), f32)]
        + [plain] * 6
        + [
            vmem((4, NAT, WIDE), f32),
            vmem((NY, NX), jnp.int32),
            vmem((2, K, 128), f32),
            vmem((2, K, 128), f32),
            vmem((2, NAT, 128), f32),
            vmem((2, NAT, 128), f32),
            vmem((3 * K, 128), f32),
            vmem((2, 3, K, 128), f32),
            vmem((2, na, K, 128), f32),
            vmem((2, nb, K, 128), f32),
            vmem((2, nc, K, 128), f32),
            vmem((2, NY, NX), f32),
            dma((22,)),
            dma((8,)),
            dma((8,)),
            dma((2, na)),
            dma((2, nb)),
            dma((2, nc)),
            dma((2, na)),
            dma((2, nb)),
            dma((2, nc)),
        ],
        compiler_params=pltpu.CompilerParams(collective_id=0, has_side_effects=True),
    )(right_side, first_guess, cell_mask, cond_east, cond_north, surface, recycled)


def finer_mesh(mesh):
    return Mesh(mesh.devices.reshape(8, 3, 4, 4, 2), AXES)


def solution(mesh):
    in_specs = (P(LAT, LON),) * 6 + (P(None, LAT, LON),)
    out_specs = (P(LAT, LON), P(LAT, LON))
    return jax.shard_map(
        shards, mesh=finer_mesh(mesh), in_specs=in_specs, out_specs=out_specs, check_vma=False
    )
```

```python
import functools

import jax
import jax.numpy as jnp
from jax import lax
from jax.experimental import pallas as pl
from jax.experimental.pallas import tpu as pltpu
from jax.sharding import Mesh
from jax.sharding import PartitionSpec as P

LAT = ("lat_0", "lat_1", "lat_2")
LON = ("lon_0", "lon_1")
AXES = LAT + LON
MESH = pl.DeviceIdType.MESH
HIGHEST = lax.Precision.HIGHEST

K = 16
DEPTH = 3
NY = 16
NX = 640
WIDE = NX + 128
ROWS = NY + 2
NAT = NY + 16
WET, NORTH, GUESS, EAST, SURF, RHS = range(6)

f32 = jnp.float32


def far_first(n):
    return sorted(range(1, n), key=lambda d: -min(d, n - d))


def iota(shape, axis):
    return lax.broadcasted_iota(jnp.int32, shape, axis)


def kernel(
    sizes,
    rhs_hbm,
    guess_hbm,
    mask_hbm,
    east_hbm,
    north_hbm,
    surf_hbm,
    rec_hbm,
    x_out,
    r_out,
    vec,
    img1,
    img2,
    nat,
    land,
    coef,
    st,
    res,
    mask_v,
    pack_vec,
    got_vec,
    pack_nat,
    got_nat,
    got_tile,
    got_corner,
    ar_send,
    ar_a,
    ar_b,
    ar_c,
    ar_d,
    ar_e,
    comb,
    in_sem,
    halo_send,
    halo_recv,
    ssem_a,
    ssem_b,
    ssem_c,
    ssem_d,
    ssem_e,
    rsem_a,
    rsem_b,
    rsem_c,
    rsem_d,
    rsem_e,
):
    ny_dev, nzh, nx_dev, nzl, ncore = sizes
    my_y = lax.axis_index("lat_0")
    my_zh = lax.axis_index("lat_1")
    my_x = lax.axis_index("lat_2")
    my_zl = lax.axis_index("lon_0")
    my_c = lax.axis_index("lon_1")
    n_lat = ny_dev * nzh * nx_dev
    n_lon = nzl * ncore
    my_lat = (my_y * nzh + my_zh) * nx_dev + my_x
    my_lon = my_zl * ncore + my_c
    na, nb, nc = nx_dev * ncore, ny_dev, nzh * nzl
    nd, ne = nx_dev * ny_dev, nzh * nzl * ncore
    my_a = my_x * ncore + my_c
    my_z = my_zh * nzl + my_zl
    my_d = my_y * nx_dev + my_x
    my_e = my_z * ncore + my_c

    def at_cell(up, right):
        lat = lax.rem(my_lat + (up + n_lat), n_lat)
        lon = lax.rem(my_lon + (right + n_lon), n_lon)
        rest = lat // nx_dev
        return (
            rest // nzh,
            lax.rem(rest, nzh),
            lax.rem(lat, nx_dev),
            lon // ncore,
            lax.rem(lon, ncore),
        )

    def at_a(index):
        return (my_y, my_zh, index // ncore, my_zl, lax.rem(index, ncore))

    def at_b(index):
        return (index, my_zh, my_x, my_zl, my_c)

    def at_c(index):
        return (my_y, index // nzl, my_x, lax.rem(index, nzl), my_c)

    def at_d(index):
        return (index // nx_dev, my_zh, lax.rem(index, nx_dev), my_zl, my_c)

    def at_e(index):
        z = index // ncore
        return (my_y, z // nzl, my_x, lax.rem(z, nzl), lax.rem(index, ncore))

    north_of, south_of = at_cell(1, 0), at_cell(-1, 0)
    east_of, west_of = at_cell(0, 1), at_cell(0, -1)
    corners = (at_cell(1, 1), at_cell(1, -1), at_cell(-1, 1), at_cell(-1, -1))

    plain = (
        (east_hbm, EAST),
        (north_hbm, NORTH),
        (surf_hbm, SURF),
        (rhs_hbm, RHS),
        (guess_hbm, GUESS),
    )
    loads = [pltpu.make_async_copy(mask_hbm, mask_v, in_sem.at[0])]
    for i, (src, field) in enumerate(plain):
        loads.append(
            pltpu.make_async_copy(
                src, nat.at[field, pl.ds(8, NY), pl.ds(0, NX)], in_sem.at[1 + i]
            )
        )
    for k in range(K):
        loads.append(
            pltpu.make_async_copy(
                rec_hbm.at[k], vec.at[pl.ds(1, NY), k, pl.ds(0, NX)], in_sem.at[6 + k]
            )
        )
    for load in loads:
        load.start()

    nat[:, 0:8, :] = jnp.zeros((6, 8, WIDE), f32)
    nat[:, 24:32, :] = jnp.zeros((6, 8, WIDE), f32)
    nat[:, 8:24, NX:] = jnp.zeros((6, NY, 128), f32)
    res[:, 0:8, :] = jnp.zeros((4, 8, WIDE), f32)
    res[:, 24:32, :] = jnp.zeros((4, 8, WIDE), f32)

    barrier = pltpu.get_barrier_semaphore()
    peers = [north_of, south_of, *corners, east_of, west_of]
    for n, me, at in ((ne, my_e, at_e), (nd, my_d, at_d), (na, my_a, at_a)):
        for d in far_first(n):
            peers.append(at(lax.rem(me + d, n)))
    for peer in peers:
        pl.semaphore_signal(barrier, inc=1, device_id=peer, device_id_type=MESH)
    for load in loads:
        load.wait()
    nat[WET, 8:24, 0:NX] = mask_v[...].astype(f32)

    def remote(src, dst, at, slot):
        return pltpu.make_async_remote_copy(
            src_ref=src,
            dst_ref=dst,
            send_sem=halo_send.at[slot],
            recv_sem=halo_recv.at[slot],
            device_id=at,
            device_id_type=MESH,
        )

    def start_all(copies):
        for copy in copies:
            copy.start()

    def wait_all(copies):
        for copy in copies:
            copy.wait()

    lanes = pl.ds(0, NX)
    lane16 = iota((K, 128), 1)
    sub16 = iota((K, 128), 0)
    lane_n = iota((NAT, 128), 1)
    zero16 = jnp.zeros((K, 128), f32)

    def pack_vectors(ref, turn):
        def row(y, carry):
            to_west, to_east = carry
            first = pltpu.roll(ref[y + 1, :, 0:128], y, 1)
            last = pltpu.roll(ref[y + 1, :, NX - 128 : NX], y + 1, 1)
            mine = lane16 == y
            return jnp.where(mine, first, to_west), jnp.where(mine, last, to_east)

        to_west, to_east = lax.fori_loop(0, NY, row, (zero16, zero16), unroll=4)
        pack_vec[turn, 0] = to_west
        pack_vec[turn, 1] = to_east

    def unpack_vectors(ref, turn):
        def row(y, carry):
            from_east = pltpu.roll(got_vec[turn, 0], lax.rem(128 - y, 128), 1)
            from_west = pltpu.roll(got_vec[turn, 1], 127 - y, 1)
            ref[y + 1, :, NX:] = jnp.where(
                lane16 == 0, from_east, jnp.where(lane16 == 127, from_west, 0.0)
            )
            return carry

        lax.fori_loop(0, NY, row, 0, unroll=4)

    def vector_rows(ref, slot):
        return [
            remote(ref.at[NY, :, lanes], ref.at[0, :, lanes], north_of, slot),
            remote(ref.at[1, :, lanes], ref.at[NY + 1, :, lanes], south_of, slot + 1),
        ]

    def vector_columns(turn, slot):
        return [
            remote(pack_vec.at[turn, 0], got_vec.at[turn, 0], west_of, slot),
            remote(pack_vec.at[turn, 1], got_vec.at[turn, 1], east_of, slot + 1),
        ]

    def landed(first, count, near, far):
        for i in range(first, first + count):
            nat[i, 8 - far : 9 - near, 0:NX] = land[i, 8 - far : 9 - near, :]
            nat[i, 23 + near : 24 + far, 0:NX] = land[i, 23 + near : 24 + far, :]

    def pack_plain(turn):
        to_west = jnp.zeros((NAT, 128), f32)
        to_east = jnp.zeros((NAT, 128), f32)
        for i in range(5):
            mine = (lane_n >= DEPTH * i) & (lane_n < DEPTH * i + DEPTH)
            first = nat[i, :, 0:128]
            if i:
                first = pltpu.roll(first, DEPTH * i, 1)
            last = pltpu.roll(nat[i, :, NX - 128 : NX], DEPTH * i + DEPTH, 1)
            to_west = jnp.where(mine, first, to_west)
            to_east = jnp.where(mine, last, to_east)
        pack_nat[turn, 0] = to_west
        pack_nat[turn, 1] = to_east

    def unpack_plain(turn):
        for i in range(5):
            from_east = got_nat[turn, 0]
            if i:
                from_east = pltpu.roll(from_east, 128 - DEPTH * i, 1)
            from_west = pltpu.roll(got_nat[turn, 1], 128 - DEPTH - DEPTH * i, 1)
            nat[i, :, NX:] = jnp.where(
                lane_n < DEPTH, from_east, jnp.where(lane_n >= 128 - DEPTH, from_west, 0.0)
            )

    def plain_columns(turn, slot):
        return [
            remote(pack_nat.at[turn, 0], got_nat.at[turn, 0], west_of, slot),
            remote(pack_nat.at[turn, 1], got_nat.at[turn, 1], east_of, slot + 1),
        ]

    def plain_rows(first, count, near, far, slot):
        fields, n = pl.ds(first, count), far - near + 1
        return [
            remote(
                nat.at[fields, pl.ds(24 - far, n), lanes],
                land.at[fields, pl.ds(8 - far, n)],
                north_of,
                slot,
            ),
            remote(
                nat.at[fields, pl.ds(7 + near, n), lanes],
                land.at[fields, pl.ds(23 + near, n)],
                south_of,
                slot + 1,
            ),
        ]

    pack_vectors(vec, 0)
    pack_plain(0)
    pl.semaphore_wait(barrier, len(peers))

    near_rows = plain_rows(0, 3, 1, 1, 0)
    vec_rows = vector_rows(vec, 2)
    vec_columns = vector_columns(0, 4)
    near_columns = plain_columns(0, 6)
    start_all(near_rows)
    start_all(vec_rows)
    start_all(near_columns)
    start_all(vec_columns)

    def east(v):
        return pltpu.roll(v, WIDE - 1, 1)

    def west(v):
        return pltpu.roll(v, 1, 1)

    def north(v):
        return pltpu.roll(v, NAT - 1, 0)

    def south(v):
        return pltpu.roll(v, 1, 0)

    def coefficients():
        row_n = iota((NAT, WIDE), 0)
        beyond = ((row_n < 8) & (my_lat == 0)) | ((row_n >= 24) & (my_lat == n_lat - 1))
        wet = jnp.where(beyond, 0.0, nat[WET])
        k_east = nat[EAST] * wet * east(wet)
        k_north = nat[NORTH] * wet * north(wet)
        k_west = west(k_east)
        k_south = south(k_north)
        coef[1] = k_east
        coef[2] = k_west
        coef[3] = k_north
        coef[4] = k_south
        coef[0] = nat[SURF] * wet + k_east + k_west + k_north + k_south + (1.0 - wet)

    def operate(v):
        return coef[0] * v - (
            coef[1] * east(v) + coef[2] * west(v) + coef[3] * north(v) + coef[4] * south(v)
        )

    def image_row(src, dst, y):
        at = pl.ds(y + 8, 1)
        v = src[y + 1]
        out = coef[0, at, :] * v - (
            coef[1, at, :] * east(v)
            + coef[2, at, :] * west(v)
            + coef[3, at, :] * src[y + 2]
            + coef[4, at, :] * src[y]
        )
        dst[y + 1, :, 0:NX] = out[:, 0:NX]
        return out[:, 0:NX]

    def fold(v):
        total = v[:, 0:128]
        for i in range(1, NX // 128):
            total = total + v[:, 128 * i : 128 * i + 128]
        return total

    def contract(a, b):
        return lax.dot_general(
            a, b, (((1,), (1,)), ((), ())), precision=HIGHEST, preferred_element_type=f32
        )

    def first_pair(rows, carry):
        acc, w_s, b_s = carry
        both = []
        for y in rows:
            w = vec[y + 1, :, 0:NX]
            b = image_row(vec, img1, y)
            s = st[pl.ds(y + 8, 1), 0:NX]
            w_s = w_s + fold(w * s)
            b_s = b_s + fold(b * s)
            both.append(jnp.concatenate([w, b], axis=0))
        both = jnp.concatenate(both, axis=1)
        return acc + contract(both, both), w_s, b_s

    def start_residual():
        st[...] = nat[RHS] - operate(nat[GUESS])

    wait_all(near_columns)
    unpack_plain(0)
    coefficients()
    start_residual()
    wait_all(vec_columns)
    unpack_vectors(vec, 0)
    carry = (jnp.zeros((2 * K, 2 * K), f32), zero16, zero16)
    carry = lax.fori_loop(
        0, NY // 2 - 1, lambda i, c: first_pair((2 * i + 1, 2 * i + 2), c), carry
    )
    wait_all(near_rows)
    landed(0, 3, 1, 1)
    wait_all(vec_rows)
    coefficients()
    start_residual()
    acc, w_s, b_s = first_pair((0, NY - 1), carry)

    def put(block, lane):
        wide = jnp.concatenate([block, jnp.zeros((K, 128 - block.shape[1]), f32)], axis=1)
        return pltpu.roll(wide, lane, 1) if lane else wide

    def column(payload, lane, total):
        return jnp.where(lane16 == lane, jnp.sum(total, axis=1, keepdims=True), payload)

    def pack(v, width):
        per, shift = 128 // width, width
        while shift < 128:
            v = v + pltpu.roll(v, shift, 1)
            shift *= 2
        v = jnp.where(lane16 // width == lax.rem(sub16, per), v, 0.0)
        return [
            jnp.sum(jnp.where(sub16 // per == i, v, 0.0), axis=0, keepdims=True)
            for i in range(K // per)
        ]

    def unpack(rows, width):
        per, shift = 128 // width, width
        v = jnp.broadcast_to(rows[0], (K, 128))
        for i in range(1, K // per):
            v = jnp.where(sub16 // per == i, rows[i], v)
        v = jnp.where(lane16 // width == lax.rem(sub16, per), v, 0.0)
        while shift < 128:
            v = v + pltpu.roll(v, shift, 1)
            shift *= 2
        return jnp.where(lane16 < width, v, 0.0)

    def send_phase(phase, value):
        send, buf, ssem, rsem, n, me, at, count = phase
        if count == 1:
            send[0:1, :] = value
            src, dst = send.at[pl.ds(0, 1)], buf.at[pl.ds(me, 1)]
        else:
            for i, row in enumerate(value):
                send[i : i + 1, :] = row
            src, dst = send.at[pl.ds(0, count)], buf.at[me, pl.ds(0, count)]
        for d in far_first(n):
            pltpu.make_async_remote_copy(
                src_ref=src,
                dst_ref=dst,
                send_sem=ssem.at[d],
                recv_sem=rsem.at[me],
                device_id=at(lax.rem(me + d, n)),
                device_id_type=MESH,
            ).start()
        if count == 1:
            buf[pl.ds(me, 1), :] = value
        else:
            for i, row in enumerate(value):
                buf[me, i : i + 1, :] = row

    def wait_phase(phase):
        send, buf, ssem, rsem, n, me, at, count = phase
        for d in range(1, n):
            peer = lax.rem(me + d, n)
            if count == 1:
                src, dst = send.at[pl.ds(0, 1)], buf.at[pl.ds(peer, 1)]
            else:
                src, dst = send.at[pl.ds(0, count)], buf.at[peer, pl.ds(0, count)]
            pltpu.make_async_remote_copy(
                src_ref=src,
                dst_ref=dst,
                send_sem=ssem.at[d],
                recv_sem=rsem.at[peer],
                device_id=at(peer),
                device_id_type=MESH,
            ).wait()
        if count == 1:
            return jnp.sum(buf[...], axis=0, keepdims=True)
        total = buf[0]
        for i in range(1, n):
            total = total + buf[i]
        return [total[i : i + 1, :] for i in range(count)]

    def three_phases(turn, count):
        return (
            (ar_send.at[turn, 0], ar_a.at[turn], ssem_a.at[turn], rsem_a.at[turn], na, my_a, at_a, count),
            (ar_send.at[turn, 1], ar_b.at[turn], ssem_b.at[turn], rsem_b.at[turn], nb, my_y, at_b, count),
            (ar_send.at[turn, 2], ar_c.at[turn], ssem_c.at[turn], rsem_c.at[turn], nc, my_z, at_c, count),
        )

    two_phases = (
        (ar_send.at[2, 0], ar_d, ssem_d, rsem_d, nd, my_d, at_d, 1),
        (ar_send.at[2, 1], ar_e, ssem_e, rsem_e, ne, my_e, at_e, 1),
    )

    def all_reduce(phases, value, between):
        for step, phase in enumerate(phases):
            send_phase(phase, value)
            if between[step] is not None:
                between[step]()
            value = wait_phase(phase)
        return value

    g3_phases = three_phases(1, 2)
    deep_rows = plain_rows(0, 2, 2, DEPTH, 8) + plain_rows(3, 2, 1, DEPTH, 10)
    deep_columns = plain_columns(1, 12)
    img_rows = vector_rows(img1, 14)
    img_columns = vector_columns(1, 16)

    def between_a():
        start_all(deep_rows)
        start_all(img_rows)
        pack_vectors(img1, 1)
        start_all(img_columns)

    def between_b():
        wait_all(deep_rows)
        landed(0, 2, 2, DEPTH)
        landed(3, 2, 1, DEPTH)
        pack_plain(1)
        start_all(deep_columns)
        wait_all(img_columns)
        unpack_vectors(img1, 1)

    kept = {}

    def second_pair(rows, acc):
        left, right = [], []
        for y in rows:
            left.append(img1[y + 1, :, 0:NX])
            right.append(image_row(img1, img2, y))
        left, right = jnp.concatenate(left, axis=1), jnp.concatenate(right, axis=1)
        return acc + contract(left, right)

    def between_c():
        acc = jnp.zeros((K, K), f32)
        acc = lax.fori_loop(
            0, NY // 2 - 1, lambda i, c: second_pair((2 * i + 1, 2 * i + 2), c), acc
        )
        wait_all(img_rows)
        kept["g3"] = second_pair((0, NY - 1), acc)
        send_phase(g3_phases[0], pack(put(kept["g3"], 0), K))
        wait_all(deep_columns)
        unpack_plain(1)
        coefficients()

    grams = 0.5 * (put(acc[0:K, K:], 0) + put(acc[K:, 0:K], 0)) + put(acc[K:, K:], K)
    rows = pack(grams, 2 * K) + pack(column(column(zero16, 0, w_s), 1, b_s), 8)
    rows = all_reduce(three_phases(0, 5), rows, (between_a, between_b, between_c))
    grams = unpack(rows[0:4], 2 * K)
    starts = unpack(rows[4:5], 8)


    def at_zero(v, lane):
        v = jnp.where((lane16 >= lane) & (lane16 < lane + K), v, 0.0)
        return pltpu.roll(v, (128 - lane) % 128, 1) if lane else v

    aug = jnp.where(lane16 < K, grams, 0.0)
    aug = jnp.where(lane16 == sub16 + K, 1.0, aug)
    aug = jnp.where(lane16 == 2 * K, starts[:, 0:1], aug)
    for i in range(K):
        pivot_row = aug[i : i + 1, :] / aug[i : i + 1, i : i + 1]
        aug = jnp.where(sub16 == i, pivot_row, aug - aug[:, i : i + 1] * pivot_row)
    coarse = aug[:, 2 * K : 2 * K + 1]
    inverse = at_zero(aug, K)
    g2 = at_zero(grams, K)

    def apply(mat, col):
        row = jnp.sum(jnp.where(lane16 == sub16, col, 0.0), axis=0, keepdims=True)
        return jnp.sum(mat * row, axis=1, keepdims=True)

    def dot(a, b):
        return jnp.sum(a * b, axis=0, keepdims=True)

    mu0 = apply(inverse, starts[:, 1:2] - apply(g2, coarse))


    def residual_row(y):
        at = pl.ds(y + 8, 1)
        r = st[at, 0:NX] - jnp.sum(coarse * img1[y + 1, :, 0:NX], axis=0, keepdims=True)
        comb[0, pl.ds(y, 1), :] = r
        res[0, at, 0:NX] = r - jnp.sum(mu0 * vec[y + 1, :, 0:NX], axis=0, keepdims=True)

    for y in range(DEPTH):
        residual_row(y)
        residual_row(NY - DEPTH + y)
    first = res.at[0]
    dir_rows = [
        remote(first.at[pl.ds(20, 4), lanes], first.at[pl.ds(4, 4), lanes], north_of, 18),
        remote(first.at[pl.ds(8, 4), lanes], first.at[pl.ds(24, 4), lanes], south_of, 19),
    ]
    left, right = pl.ds(0, 128), pl.ds(NX - 128, 128)
    dir_corners = [
        remote(first.at[pl.ds(16, 8), right], got_corner.at[0], corners[0], 20),
        remote(first.at[pl.ds(16, 8), left], got_corner.at[1], corners[1], 21),
        remote(first.at[pl.ds(8, 8), right], got_corner.at[2], corners[2], 22),
        remote(first.at[pl.ds(8, 8), left], got_corner.at[3], corners[3], 23),
    ]
    dir_columns = [
        remote(first.at[pl.ds(8, NY), left], got_tile.at[0], west_of, 24),
        remote(first.at[pl.ds(8, NY), right], got_tile.at[1], east_of, 25),
    ]
    residual_row(DEPTH)
    residual_row(NY - DEPTH - 1)
    start_all(dir_rows)

    def inner_row(y, carry):
        residual_row(y)
        return carry

    lax.fori_loop(DEPTH + 1, NY - DEPTH - 1, inner_row, 0, unroll=4)
    start_all(dir_corners)
    start_all(dir_columns)
    g3_rows = wait_phase(g3_phases[0])
    send_phase(g3_phases[1], g3_rows)
    wait_all(dir_columns)
    wait_all(dir_corners)
    wait_all(dir_rows)
    lane8 = lane16[0:8]

    def edge_columns(from_east, from_west, lane):
        return jnp.where(
            lane < DEPTH, from_east, jnp.where(lane >= 128 - DEPTH, from_west, 0.0)
        )

    res[0, 8:24, NX:] = edge_columns(got_tile[0], got_tile[1], lane16)
    res[0, 0:8, NX:] = edge_columns(got_corner[1], got_corner[0], lane8)
    res[0, 24:32, NX:] = edge_columns(got_corner[3], got_corner[2], lane8)
    for i in range(3):
        res[i + 1] = operate(res[i])

    def moment_row(y, carry):
        e = y + 1
        b1, b2 = img1[e, :, 0:NX], img2[e, :, 0:NX]
        v1, a1 = (res[i, pl.ds(y + 8, 1), 0:NX] for i in (1, 2))
        terms = (b1 * v1, b1 * a1, b2 * a1)
        return tuple(total + fold(term) for total, term in zip(carry, terms))

    defl = lax.fori_loop(0, NY, moment_row, (zero16,) * 3, unroll=2)
    payload = zero16
    for i, total in enumerate(defl):
        payload = column(payload, i, total)
    inner = [comb[0]] + [res[i, 8:24, 0:NX] for i in (1, 2, 3)]
    for i, (a, b) in enumerate(((0, 0), (0, 1), (1, 1), (1, 2), (2, 2), (2, 3))):
        total = jnp.sum(fold(inner[a] * inner[b]), axis=0, keepdims=True)
        total = jnp.sum(total, axis=1, keepdims=True)
        payload = jnp.where((lane16 == 3) & (sub16 == i), total, payload)

    def before_scalars():
        def row(y, carry):
            at = pl.ds(y + 8, 1)
            along = jnp.sum(coarse * vec[y + 1, :, 0:NX], axis=0, keepdims=True)
            st[at, 0:NX] = nat[GUESS, at, 0:NX] + along
            return carry

        lax.fori_loop(0, NY, row, 0, unroll=4)
        send_phase(g3_phases[2], wait_phase(g3_phases[1]))

    def last_gram():
        kept["g3"] = unpack(wait_phase(g3_phases[2]), K)

    row = all_reduce(two_phases, pack(payload, 8)[0], (before_scalars, last_gram))
    sums = unpack([row], 8)

    g3 = kept["g3"]
    e = [sums[:, i : i + 1] for i in range(3)]
    t = [sums[i : i + 1, 3:4] for i in range(6)]
    mu1 = apply(inverse, e[0])
    g2_1, g3_1 = apply(g2, mu1), apply(g3, mu1)
    defl2 = e[1] - g2_1
    mu2 = apply(inverse, defl2)
    m = [
        t[0],
        t[1],
        t[2],
        t[3] - dot(mu1, e[0]),
        t[4] - 2.0 * dot(mu1, e[1]) + dot(mu1, g2_1),
        t[5] - 2.0 * dot(mu1, e[2]) + dot(mu1, g3_1) - dot(mu2, defl2),
    ]

    def form(poly, shift):
        total = 0.0
        for i, a in enumerate(poly):
            for j, b in enumerate(poly):
                total = total + a * b * m[i + j + shift]
        return total

    one = jnp.ones((1, 1), f32)
    zero = jnp.zeros((1, 1), f32)
    r_poly = [one]
    y_poly = [zero]
    zeta = [zero, zero, zero]
    curv = prev_norm = one
    for turn in range(3):
        norm = form(r_poly, 0)
        r_image = form(r_poly, 1)
        if turn == 0:
            y_poly = list(r_poly)
            curv = r_image
        else:
            ratio = norm / prev_norm
            y_poly = [a + ratio * b for a, b in zip(r_poly, y_poly + [zero])]
            curv = r_image - ratio * ratio * curv
        step_len = norm / curv
        for i, a in enumerate(y_poly):
            zeta[i] = zeta[i] + step_len * a
        r_poly = [
            a - step_len * b for a, b in zip(r_poly + [zero], [zero] + list(y_poly))
        ]
        prev_norm = norm

    along_w = zeta[1] * mu1 + zeta[2] * mu2
    along_b = zeta[2] * mu1

    def final_row(y, carry):
        w, b1, b2 = (ref[y + 1, :, 0:NX] for ref in (vec, img1, img2))
        at = pl.ds(y, 1)
        comb[1, at, :] = jnp.sum(along_w * w + along_b * b1, axis=0, keepdims=True)
        comb[2, at, :] = jnp.sum(along_w * b1 + along_b * b2, axis=0, keepdims=True)
        return carry

    lax.fori_loop(0, NY, final_row, 0, unroll=4)
    p0, v1, a1, a2 = (res[i, 8:24, 0:NX] for i in range(4))
    x_out[...] = (
        st[8:24, 0:NX] + (zeta[0] * p0 + zeta[1] * v1 + zeta[2] * a1) - comb[1]
    )
    r_out[...] = comb[0] - (zeta[0] * v1 + zeta[1] * a1 + zeta[2] * a2) + comb[2]


def shards(right_side, first_guess, cell_mask, cond_east, cond_north, surface, recycled):
    sizes = tuple(lax.axis_size(axis) for axis in AXES)
    ny_dev, nzh, nx_dev, nzl, ncore = sizes
    na, nb, nc = nx_dev * ncore, ny_dev, nzh * nzl
    nd, ne = nx_dev * ny_dev, nzh * nzl * ncore
    field = jax.ShapeDtypeStruct((NY, NX), f32)
    vmem = pltpu.VMEM
    dma = pltpu.SemaphoreType.DMA
    return pl.pallas_call(
        functools.partial(kernel, sizes),
        out_shape=(field, field),
        in_specs=[pl.BlockSpec(memory_space=pl.ANY)] * 7,
        out_specs=(pl.BlockSpec(memory_space=pltpu.VMEM),) * 2,
        scratch_shapes=[
            vmem((ROWS, K, WIDE), f32),
            vmem((ROWS, K, WIDE), f32),
            vmem((ROWS, K, NX), f32),
            vmem((6, NAT, WIDE), f32),
            vmem((5, NAT, NX), f32),
            vmem((5, NAT, WIDE), f32),
            vmem((NAT, WIDE), f32),
            vmem((4, NAT, WIDE), f32),
            vmem((NY, NX), jnp.int32),
            vmem((2, 2, K, 128), f32),
            vmem((2, 2, K, 128), f32),
            vmem((2, 2, NAT, 128), f32),
            vmem((2, 2, NAT, 128), f32),
            vmem((2, NY, 128), f32),
            vmem((4, 8, 128), f32),
            vmem((3, 3, 8, 128), f32),
            vmem((2, na, 8, 128), f32),
            vmem((2, nb, 8, 128), f32),
            vmem((2, nc, 8, 128), f32),
            vmem((nd, 128), f32),
            vmem((ne, 128), f32),
            vmem((3, NY, NX), f32),
            dma((22,)),
            dma((26,)),
            dma((26,)),
            dma((2, na)),
            dma((2, nb)),
            dma((2, nc)),
            dma((nd,)),
            dma((ne,)),
            dma((2, na)),
            dma((2, nb)),
            dma((2, nc)),
            dma((nd,)),
            dma((ne,)),
        ],
        compiler_params=pltpu.CompilerParams(collective_id=0, has_side_effects=True),
    )(right_side, first_guess, cell_mask, cond_east, cond_north, surface, recycled)


def finer_mesh(mesh):
    return Mesh(mesh.devices.reshape(8, 3, 4, 4, 2), AXES)


def solution(mesh):
    in_specs = (P(LAT, LON),) * 6 + (P(None, LAT, LON),)
    out_specs = (P(LAT, LON), P(LAT, LON))
    return jax.shard_map(
        shards, mesh=finer_mesh(mesh), in_specs=in_specs, out_specs=out_specs, check_vma=False
    )
```

```python
import functools

import jax
import jax.numpy as jnp
from jax import lax
from jax.experimental import pallas as pl
from jax.experimental.pallas import tpu as pltpu
from jax.sharding import Mesh
from jax.sharding import PartitionSpec as P

LAT = ("lat_0", "lat_1", "lat_2")
LON = ("lon_0", "lon_1")
AXES = LAT + LON
MESH = pl.DeviceIdType.MESH
HIGHEST = lax.Precision.HIGHEST

K = 16
DEPTH = 4
NY = 16
NX = 640
WIDE = NX + 128
ROWS = NY + 2 * DEPTH
NAT = NY + 16
WET, NORTH, GUESS, EAST, SURF, RHS = range(6)

f32 = jnp.float32


def far_first(n):
    return sorted(range(1, n), key=lambda d: -min(d, n - d))


def iota(shape, axis):
    return lax.broadcasted_iota(jnp.int32, shape, axis)


def kernel(
    sizes,
    rhs_hbm,
    guess_hbm,
    mask_hbm,
    east_hbm,
    north_hbm,
    surf_hbm,
    rec_hbm,
    x_out,
    r_out,
    vec,
    img1,
    img2,
    nat,
    land,
    coef,
    st,
    res,
    mask_v,
    pack_vec,
    got_vec,
    pack_nat,
    got_nat,
    ar_send,
    ar_a,
    ar_b,
    ar_c,
    ar_d,
    ar_e,
    comb,
    relay,
    in_sem,
    halo_send,
    halo_recv,
    ssem_a,
    ssem_b,
    ssem_c,
    ssem_d,
    ssem_e,
    rsem_a,
    rsem_b,
    rsem_c,
    rsem_d,
    rsem_e,
):
    ny_dev, nzh, nx_dev, nzl, ncore = sizes
    my_y = lax.axis_index("lat_0")
    my_zh = lax.axis_index("lat_1")
    my_x = lax.axis_index("lat_2")
    my_zl = lax.axis_index("lon_0")
    my_c = lax.axis_index("lon_1")
    n_lat = ny_dev * nzh * nx_dev
    n_lon = nzl * ncore
    my_lat = (my_y * nzh + my_zh) * nx_dev + my_x
    my_lon = my_zl * ncore + my_c
    na, nb, nc = nx_dev * ncore, ny_dev, nzh * nzl
    nd, ne = nx_dev * ny_dev, nzh * nzl * ncore
    my_a = my_x * ncore + my_c
    my_z = my_zh * nzl + my_zl
    my_d = my_y * nx_dev + my_x
    my_e = my_z * ncore + my_c

    def at_cell(up, right):
        lat = lax.rem(my_lat + (up + n_lat), n_lat)
        lon = lax.rem(my_lon + (right + n_lon), n_lon)
        rest = lat // nx_dev
        return (
            rest // nzh,
            lax.rem(rest, nzh),
            lax.rem(lat, nx_dev),
            lon // ncore,
            lax.rem(lon, ncore),
        )

    def at_a(index):
        return (my_y, my_zh, index // ncore, my_zl, lax.rem(index, ncore))

    def at_b(index):
        return (index, my_zh, my_x, my_zl, my_c)

    def at_c(index):
        return (my_y, index // nzl, my_x, lax.rem(index, nzl), my_c)

    def at_d(index):
        return (index // nx_dev, my_zh, lax.rem(index, nx_dev), my_zl, my_c)

    def at_e(index):
        z = index // ncore
        return (my_y, z // nzl, my_x, lax.rem(z, nzl), lax.rem(index, ncore))

    north_of, south_of = at_cell(1, 0), at_cell(-1, 0)
    east_of, west_of = at_cell(0, 1), at_cell(0, -1)
    corners = (at_cell(1, 1), at_cell(1, -1), at_cell(-1, 1), at_cell(-1, -1))

    barrier = pltpu.get_barrier_semaphore()
    peers = [north_of, south_of, *corners, east_of, west_of]
    for n, me, at in ((ne, my_e, at_e), (nd, my_d, at_d), (na, my_a, at_a)):
        for d in far_first(n):
            peers.append(at(lax.rem(me + d, n)))
    for peer in peers:
        pl.semaphore_signal(barrier, inc=1, device_id=peer, device_id_type=MESH)

    plain = (
        (east_hbm, EAST),
        (north_hbm, NORTH),
        (surf_hbm, SURF),
        (rhs_hbm, RHS),
        (guess_hbm, GUESS),
    )
    loads = [pltpu.make_async_copy(mask_hbm, mask_v, in_sem.at[0])]
    for i, (src, field) in enumerate(plain):
        loads.append(
            pltpu.make_async_copy(
                src, nat.at[field, pl.ds(8, NY), pl.ds(0, NX)], in_sem.at[1 + i]
            )
        )
    for k in range(K):
        loads.append(
            pltpu.make_async_copy(
                rec_hbm.at[k], vec.at[pl.ds(DEPTH, NY), k, pl.ds(0, NX)], in_sem.at[6 + k]
            )
        )
    for load in loads:
        load.start()

    nat[:, 0:8, :] = jnp.zeros((6, 8, WIDE), f32)
    nat[:, 24:32, :] = jnp.zeros((6, 8, WIDE), f32)
    nat[:, 8:24, NX:] = jnp.zeros((6, NY, 128), f32)
    res[:, 0:8, :] = jnp.zeros((5, 8, WIDE), f32)
    res[:, 24:32, :] = jnp.zeros((5, 8, WIDE), f32)

    for load in loads:
        load.wait()
    nat[WET, 8:24, 0:NX] = mask_v[...].astype(f32)

    def remote(src, dst, at, slot):
        return pltpu.make_async_remote_copy(
            src_ref=src,
            dst_ref=dst,
            send_sem=halo_send.at[slot],
            recv_sem=halo_recv.at[slot],
            device_id=at,
            device_id_type=MESH,
        )

    def start_all(copies):
        for copy in copies:
            copy.start()

    def wait_all(copies):
        for copy in copies:
            copy.wait()

    lanes = pl.ds(0, NX)
    lane16 = iota((K, 128), 1)
    sub16 = iota((K, 128), 0)
    zero16 = jnp.zeros((K, 128), f32)

    def pack_vectors():
        def row(y, carry):
            to_west, to_east = carry
            e, lane = y + DEPTH, DEPTH * y
            first = pltpu.roll(vec[e, :, 0:128], lane, 1)
            last = pltpu.roll(vec[e, :, NX - 128 : NX], lane + DEPTH, 1)
            mine = (lane16 >= lane) & (lane16 < lane + DEPTH)
            return jnp.where(mine, first, to_west), jnp.where(mine, last, to_east)

        to_west, to_east = lax.fori_loop(0, NY, row, (zero16, zero16), unroll=4)
        pack_vec[0] = to_west
        pack_vec[1] = to_east

    def edge_columns(from_east, from_west, lane):
        return jnp.where(
            lane < DEPTH, from_east, jnp.where(lane >= 128 - DEPTH, from_west, 0.0)
        )

    def unpack_vectors(first, count, y0, place):
        def row(i, carry):
            lane = DEPTH * (y0 + i)
            from_east = pltpu.roll(got_vec[place], lax.rem(128 - lane, 128), 1)
            from_west = pltpu.roll(got_vec[place + 1], 128 - DEPTH - lane, 1)
            vec[first + i, :, NX:] = edge_columns(from_east, from_west, lane16)
            return carry

        lax.fori_loop(0, count, row, 0, unroll=4)

    def pack_plain():
        to_west, to_east = zero16, zero16
        for i in range(6):
            lane = DEPTH * i
            first, last = nat[i, 8:24, 0:128], nat[i, 8:24, NX - 128 : NX]
            if i:
                first = pltpu.roll(first, lane, 1)
            last = pltpu.roll(last, lane + DEPTH, 1)
            mine = (lane16 >= lane) & (lane16 < lane + DEPTH)
            to_west = jnp.where(mine, first, to_west)
            to_east = jnp.where(mine, last, to_east)
        pack_nat[0] = to_west
        pack_nat[1] = to_east

    def unpack_plain(first, count, y0, place):
        lane = lane16[0:count]
        for i in range(6):
            from_east = got_nat[place, y0 : y0 + count, :]
            from_west = got_nat[place + 1, y0 : y0 + count, :]
            if i:
                from_east = pltpu.roll(from_east, 128 - DEPTH * i, 1)
            from_west = pltpu.roll(from_west, 128 - DEPTH - DEPTH * i, 1)
            nat[i, first : first + count, NX:] = edge_columns(from_east, from_west, lane)

    def landed(first, count, near, far):
        for i in range(first, first + count):
            nat[i, 8 - far : 9 - near, 0:NX] = land[i, 8 - far : 9 - near, :]
            nat[i, 23 + near : 24 + far, 0:NX] = land[i, 23 + near : 24 + far, :]

    def vector_rows(near, far, slot):
        n = far - near + 1
        return [
            remote(
                vec.at[pl.ds(20 - far, n), :, lanes],
                vec.at[pl.ds(4 - far, n), :, lanes],
                north_of,
                slot,
            ),
            remote(
                vec.at[pl.ds(3 + near, n), :, lanes],
                vec.at[pl.ds(19 + near, n), :, lanes],
                south_of,
                slot + 1,
            ),
        ]

    def far_rows():
        ahead, behind = lax.rem(my_zh + 1, nzh), lax.rem(my_zh + (nzh - 1), nzh)
        next_y = jnp.where(my_zh == nzh - 1, lax.rem(my_y + 1, ny_dev), my_y)
        last_y = jnp.where(my_zh == 0, lax.rem(my_y + (ny_dev - 1), ny_dev), my_y)
        ways = (
            (
                my_x == nx_dev - 1,
                my_x == 0,
                vec.at[pl.ds(16, 2), :, lanes],
                vec.at[pl.ds(0, 2), :, lanes],
                north_of,
                (next_y, my_zh, 0, my_zl, my_c),
                (my_y, ahead, my_x, my_zl, my_c),
            ),
            (
                my_x == 0,
                my_x == nx_dev - 1,
                vec.at[pl.ds(6, 2), :, lanes],
                vec.at[pl.ds(22, 2), :, lanes],
                south_of,
                (last_y, my_zh, nx_dev - 1, my_zl, my_c),
                (my_y, behind, my_x, my_zl, my_c),
            ),
        )

        def copy(src, dst, at, send_slot, recv_slot):
            return pltpu.make_async_remote_copy(
                src_ref=src,
                dst_ref=dst,
                send_sem=halo_send.at[send_slot],
                recv_sem=halo_recv.at[recv_slot],
                device_id=at,
                device_id_type=MESH,
            )

        hops = []
        for i, (crosses, forwards, src, dst, straight, first_hop, last_hop) in enumerate(ways):
            held = relay.at[i]
            hops.append(
                (
                    crosses,
                    forwards,
                    copy(src, dst, straight, 22 + i, 22 + i),
                    copy(src, held, first_hop, 24 + i, 24 + i),
                    copy(held, dst, last_hop, 26 + i, 22 + i),
                )
            )

        def begin():
            for crosses, _, straight, first, _ in hops:
                pl.when(jnp.logical_not(crosses))(straight.start)
                pl.when(crosses)(first.start)

        def forward():
            for _, forwards, _, first, last in hops:

                @pl.when(forwards)
                def _():
                    first.wait_recv()
                    last.start()

        def finish():
            for crosses, forwards, straight, first, last in hops:
                pl.when(jnp.logical_not(crosses))(straight.wait_send)
                pl.when(crosses)(first.wait_send)
                pl.when(forwards)(last.wait_send)
                straight.wait_recv()

        return begin, forward, finish

    def columns(pack, got, slot):
        return [
            remote(pack.at[0], got.at[0], west_of, slot),
            remote(pack.at[1], got.at[1], east_of, slot + 1),
        ]

    def corner_columns(pack, got, slot, south_rows, north_rows):
        north_east, north_west, south_east, south_west = corners
        return [
            remote(pack.at[0, south_rows], got.at[2, south_rows], south_west, slot),
            remote(pack.at[1, south_rows], got.at[3, south_rows], south_east, slot + 1),
            remote(pack.at[0, north_rows], got.at[4, north_rows], north_west, slot + 2),
            remote(pack.at[1, north_rows], got.at[5, north_rows], north_east, slot + 3),
        ]

    def plain_rows(first, count, near, far, slot):
        fields, n = pl.ds(first, count), far - near + 1
        return [
            remote(
                nat.at[fields, pl.ds(24 - far, n), lanes],
                land.at[fields, pl.ds(8 - far, n)],
                north_of,
                slot,
            ),
            remote(
                nat.at[fields, pl.ds(7 + near, n), lanes],
                land.at[fields, pl.ds(23 + near, n)],
                south_of,
                slot + 1,
            ),
        ]

    pack_vectors()
    pack_plain()
    pl.semaphore_wait(barrier, len(peers))

    near_rows = plain_rows(0, 3, 1, 1, 0)
    vec_rows = vector_rows(1, 1, 2)
    vec_columns = columns(pack_vec, got_vec, 4)
    near_columns = columns(pack_nat, got_nat, 6)
    all_rows = pl.ds(0, NY)
    far = far_rows()
    deep = (
        corner_columns(pack_nat, got_nat, 18, pl.ds(0, 8), pl.ds(8, 8))
        + plain_rows(0, 3, 2, DEPTH, 8)
        + plain_rows(3, 3, 1, DEPTH - 1, 10)
        + corner_columns(pack_vec, got_vec, 14, all_rows, all_rows)
        + vector_rows(2, 2, 12)
    )
    start_all(near_columns)
    start_all(vec_columns)
    start_all(near_rows)
    start_all(vec_rows)

    def east(v):
        return pltpu.roll(v, WIDE - 1, 1)

    def west(v):
        return pltpu.roll(v, 1, 1)

    def north(v):
        return pltpu.roll(v, NAT - 1, 0)

    def south(v):
        return pltpu.roll(v, 1, 0)

    def coefficients():
        row_n = iota((NAT, WIDE), 0)
        beyond = ((row_n < 8) & (my_lat == 0)) | ((row_n >= 24) & (my_lat == n_lat - 1))
        wet = jnp.where(beyond, 0.0, nat[WET])
        k_east = nat[EAST] * wet * east(wet)
        k_north = nat[NORTH] * wet * north(wet)
        k_west = west(k_east)
        k_south = south(k_north)
        coef[1] = k_east
        coef[2] = k_west
        coef[3] = k_north
        coef[4] = k_south
        coef[0] = nat[SURF] * wet + k_east + k_west + k_north + k_south + (1.0 - wet)

    def operate(v):
        return coef[0] * v - (
            coef[1] * east(v) + coef[2] * west(v) + coef[3] * north(v) + coef[4] * south(v)
        )

    def image_row(src, e):
        at = pl.ds(e + 4, 1)
        v = src[e]
        return coef[0, at, :] * v - (
            coef[1, at, :] * east(v)
            + coef[2, at, :] * west(v)
            + coef[3, at, :] * src[e + 1]
            + coef[4, at, :] * src[e - 1]
        )

    def fold(v):
        total = v[:, 0:128]
        for i in range(1, NX // 128):
            total = total + v[:, 128 * i : 128 * i + 128]
        return total

    def contract(a, b):
        return lax.dot_general(
            a, b, (((1,), (1,)), ((), ())), precision=HIGHEST, preferred_element_type=f32
        )

    def first_pair(rows, carry):
        acc, w_s, b_s = carry
        both = []
        for y in rows:
            w = vec[y + DEPTH, :, 0:NX]
            image = image_row(vec, y + DEPTH)
            img1[y + DEPTH] = image
            b = image[:, 0:NX]
            s = st[pl.ds(y + 8, 1), 0:NX]
            w_s = w_s + fold(w * s)
            b_s = b_s + fold(b * s)
            both.append(jnp.concatenate([w, b], axis=0))
        both = jnp.concatenate(both, axis=1)
        return acc + contract(both, both), w_s, b_s

    def start_residual():
        st[...] = nat[RHS] - operate(nat[GUESS])

    wait_all(near_columns)
    unpack_plain(8, NY, 0, 0)
    coefficients()
    start_residual()
    wait_all(vec_columns)
    unpack_vectors(DEPTH, NY, 0, 0)
    far[0]()
    carry = (jnp.zeros((2 * K, 2 * K), f32), zero16, zero16)
    carry = lax.fori_loop(
        0, NY // 2 - 1, lambda i, c: first_pair((2 * i + 1, 2 * i + 2), c), carry
    )
    start_all(deep)
    wait_all(near_rows)
    landed(0, 3, 1, 1)
    wait_all(vec_rows)
    coefficients()
    start_residual()
    acc, w_s, b_s = first_pair((0, NY - 1), carry)

    def put(block, lane):
        wide = jnp.concatenate([block, jnp.zeros((K, 128 - block.shape[1]), f32)], axis=1)
        return pltpu.roll(wide, lane, 1) if lane else wide

    def column(payload, lane, total):
        return jnp.where(lane16 == lane, jnp.sum(total, axis=1, keepdims=True), payload)

    def pack(v, width):
        per, shift = 128 // width, width
        while shift < 128:
            v = v + pltpu.roll(v, shift, 1)
            shift *= 2
        v = jnp.where(lane16 // width == lax.rem(sub16, per), v, 0.0)
        return [
            jnp.sum(jnp.where(sub16 // per == i, v, 0.0), axis=0, keepdims=True)
            for i in range(K // per)
        ]

    def unpack(rows, width):
        per, shift = 128 // width, width
        v = jnp.broadcast_to(rows[0], (K, 128))
        for i in range(1, K // per):
            v = jnp.where(sub16 // per == i, rows[i], v)
        v = jnp.where(lane16 // width == lax.rem(sub16, per), v, 0.0)
        while shift < 128:
            v = v + pltpu.roll(v, shift, 1)
            shift *= 2
        return jnp.where(lane16 < width, v, 0.0)

    def send_phase(phase, value):
        send, buf, ssem, rsem, n, me, at, count = phase
        if count == 1:
            send[0:1, :] = value
            src, dst = send.at[pl.ds(0, 1)], buf.at[pl.ds(me, 1)]
        else:
            for i, row in enumerate(value):
                send[i : i + 1, :] = row
            src, dst = send.at[pl.ds(0, count)], buf.at[me, pl.ds(0, count)]
        for d in far_first(n):
            pltpu.make_async_remote_copy(
                src_ref=src,
                dst_ref=dst,
                send_sem=ssem.at[d],
                recv_sem=rsem.at[me],
                device_id=at(lax.rem(me + d, n)),
                device_id_type=MESH,
            ).start()
        if count == 1:
            buf[pl.ds(me, 1), :] = value
        else:
            for i, row in enumerate(value):
                buf[me, i : i + 1, :] = row

    def wait_phase(phase):
        send, buf, ssem, rsem, n, me, at, count = phase
        for d in range(1, n):
            peer = lax.rem(me + d, n)
            if count == 1:
                src, dst = send.at[pl.ds(0, 1)], buf.at[pl.ds(peer, 1)]
            else:
                src, dst = send.at[pl.ds(0, count)], buf.at[peer, pl.ds(0, count)]
            pltpu.make_async_remote_copy(
                src_ref=src,
                dst_ref=dst,
                send_sem=ssem.at[d],
                recv_sem=rsem.at[peer],
                device_id=at(peer),
                device_id_type=MESH,
            ).wait()
        if count == 1:
            return jnp.sum(buf[...], axis=0, keepdims=True)
        total = buf[0]
        for i in range(1, n):
            total = total + buf[i]
        return [total[i : i + 1, :] for i in range(count)]

    def three_phases(turn, count):
        return (
            (ar_send.at[turn, 0], ar_a.at[turn], ssem_a.at[turn], rsem_a.at[turn], na, my_a, at_a, count),
            (ar_send.at[turn, 1], ar_b.at[turn], ssem_b.at[turn], rsem_b.at[turn], nb, my_y, at_b, count),
            (ar_send.at[turn, 2], ar_c.at[turn], ssem_c.at[turn], rsem_c.at[turn], nc, my_z, at_c, count),
        )

    two_phases = (
        (ar_send.at[2, 0], ar_d, ssem_d, rsem_d, nd, my_d, at_d, 1),
        (ar_send.at[2, 1], ar_e, ssem_e, rsem_e, ne, my_e, at_e, 1),
    )

    def all_reduce(phases, value, between):
        for step, phase in enumerate(phases):
            send_phase(phase, value)
            if between[step] is not None:
                between[step]()
            value = wait_phase(phase)
        return value

    g3_phases = three_phases(1, 2)
    kept = {}

    def second_pair(rows, acc):
        left, right = [], []
        for y in rows:
            left.append(img1[y + DEPTH, :, 0:NX])
            right.append(image_row(img1, y + DEPTH)[:, 0:NX])
            img2[y] = right[-1]
        left, right = jnp.concatenate(left, axis=1), jnp.concatenate(right, axis=1)
        return acc + contract(left, right)

    def between_a():
        acc = jnp.zeros((K, K), f32)
        kept["g3"] = lax.fori_loop(
            0, NY // 2 - 1, lambda i, c: second_pair((2 * i + 1, 2 * i + 2), c), acc
        )

    def between_c():
        wait_all(deep)
        far[2]()
        landed(0, 3, 2, DEPTH)
        landed(3, 3, 1, DEPTH - 1)
        unpack_plain(24, 8, 0, 2)
        unpack_plain(0, 8, 8, 4)
        unpack_vectors(NY + DEPTH, DEPTH, 0, 2)
        unpack_vectors(0, DEPTH, NY - DEPTH, 4)
        coefficients()
        start_residual()

        def outer_row(i, carry):
            img1[i + 1] = image_row(vec, i + 1)
            img1[i + 19] = image_row(vec, i + 19)
            return carry

        lax.fori_loop(0, DEPTH, outer_row, 0)
        acc = second_pair((0, NY - 1), kept["g3"])
        send_phase(g3_phases[0], pack(put(acc, 0), K))

    grams = 0.5 * (put(acc[0:K, K:], 0) + put(acc[K:, 0:K], 0)) + put(acc[K:, K:], K)
    rows = pack(grams, 2 * K) + pack(column(column(zero16, 0, w_s), 1, b_s), 8)
    rows = all_reduce(three_phases(0, 5), rows, (between_a, far[1], between_c))
    grams = unpack(rows[0:4], 2 * K)
    starts = unpack(rows[4:5], 8)


    def at_zero(v, lane):
        v = jnp.where((lane16 >= lane) & (lane16 < lane + K), v, 0.0)
        return pltpu.roll(v, (128 - lane) % 128, 1) if lane else v

    aug = jnp.where(lane16 < K, grams, 0.0)
    aug = jnp.where(lane16 == sub16 + K, 1.0, aug)
    aug = jnp.where(lane16 == 2 * K, starts[:, 0:1], aug)
    for i in range(K):
        pivot_row = aug[i : i + 1, :] / aug[i : i + 1, i : i + 1]
        aug = jnp.where(sub16 == i, pivot_row, aug - aug[:, i : i + 1] * pivot_row)
    coarse = aug[:, 2 * K : 2 * K + 1]
    inverse = at_zero(aug, K)
    g1, g2 = at_zero(grams, 0), at_zero(grams, K)

    def apply(mat, col):
        row = jnp.sum(jnp.where(lane16 == sub16, col, 0.0), axis=0, keepdims=True)
        return jnp.sum(mat * row, axis=1, keepdims=True)

    def dot(a, b):
        return jnp.sum(a * b, axis=0, keepdims=True)

    coarse = coarse + apply(inverse, starts[:, 0:1] - apply(g1, coarse))
    mu0 = apply(inverse, starts[:, 1:2] - apply(g2, coarse))


    def residual_row(e, carry):
        at = pl.ds(e + 4, 1)
        r = st[at, :] - jnp.sum(coarse * img1[e], axis=0, keepdims=True)
        res[4, at, :] = r
        res[0, at, :] = r - jnp.sum(mu0 * vec[e], axis=0, keepdims=True)
        return carry

    lax.fori_loop(1, ROWS - 1, residual_row, 0, unroll=2)
    send_phase(g3_phases[1], wait_phase(g3_phases[0]))
    for i in range(3):
        res[i + 1] = operate(res[i])

    def moment_row(y, carry):
        b1, b2 = img1[y + DEPTH, :, 0:NX], img2[y]
        v1, a1 = (res[i, pl.ds(y + 8, 1), 0:NX] for i in (1, 2))
        terms = (b1 * v1, b1 * a1, b2 * a1)
        return tuple(total + fold(term) for total, term in zip(carry, terms))

    defl = lax.fori_loop(0, NY, moment_row, (zero16,) * 3, unroll=2)
    payload = zero16
    for i, total in enumerate(defl):
        payload = column(payload, i, total)
    inner = [res[i, 8:24, 0:NX] for i in (4, 1, 2, 3)]
    for i, (a, b) in enumerate(((0, 0), (0, 1), (1, 1), (1, 2), (2, 2), (2, 3))):
        total = jnp.sum(fold(inner[a] * inner[b]), axis=0, keepdims=True)
        total = jnp.sum(total, axis=1, keepdims=True)
        payload = jnp.where((lane16 == 3) & (sub16 == i), total, payload)

    def before_scalars():
        def row(y, carry):
            at = pl.ds(y + 8, 1)
            along = jnp.sum(coarse * vec[y + DEPTH, :, 0:NX], axis=0, keepdims=True)
            st[at, 0:NX] = nat[GUESS, at, 0:NX] + along
            return carry

        lax.fori_loop(0, NY, row, 0, unroll=4)
        send_phase(g3_phases[2], wait_phase(g3_phases[1]))

    def last_gram():
        kept["g3"] = unpack(wait_phase(g3_phases[2]), K)

    row = all_reduce(two_phases, pack(payload, 8)[0], (before_scalars, last_gram))
    sums = unpack([row], 8)

    g3 = kept["g3"]
    e = [sums[:, i : i + 1] for i in range(3)]
    t = [sums[i : i + 1, 3:4] for i in range(6)]
    mu1 = apply(inverse, e[0])
    g2_1, g3_1 = apply(g2, mu1), apply(g3, mu1)
    defl2 = e[1] - g2_1
    mu2 = apply(inverse, defl2)
    m = [
        t[0],
        t[1],
        t[2],
        t[3] - dot(mu1, e[0]),
        t[4] - 2.0 * dot(mu1, e[1]) + dot(mu1, g2_1),
        t[5] - 2.0 * dot(mu1, e[2]) + dot(mu1, g3_1) - dot(mu2, defl2),
    ]

    def form(poly, shift):
        total = 0.0
        for i, a in enumerate(poly):
            for j, b in enumerate(poly):
                total = total + a * b * m[i + j + shift]
        return total

    one = jnp.ones((1, 1), f32)
    zero = jnp.zeros((1, 1), f32)
    r_poly = [one]
    y_poly = [zero]
    zeta = [zero, zero, zero]
    curv = prev_norm = one
    for turn in range(3):
        norm = form(r_poly, 0)
        r_image = form(r_poly, 1)
        if turn == 0:
            y_poly = list(r_poly)
            curv = r_image
        else:
            ratio = norm / prev_norm
            y_poly = [a + ratio * b for a, b in zip(r_poly, y_poly + [zero])]
            curv = r_image - ratio * ratio * curv
        step_len = norm / curv
        for i, a in enumerate(y_poly):
            zeta[i] = zeta[i] + step_len * a
        r_poly = [
            a - step_len * b for a, b in zip(r_poly + [zero], [zero] + list(y_poly))
        ]
        prev_norm = norm

    along_w = zeta[1] * mu1 + zeta[2] * mu2
    along_b = zeta[2] * mu1

    def final_row(y, carry):
        w, b1, b2 = vec[y + DEPTH, :, 0:NX], img1[y + DEPTH, :, 0:NX], img2[y]
        at = pl.ds(y, 1)
        comb[0, at, :] = jnp.sum(along_w * w + along_b * b1, axis=0, keepdims=True)
        comb[1, at, :] = jnp.sum(along_w * b1 + along_b * b2, axis=0, keepdims=True)
        return carry

    lax.fori_loop(0, NY, final_row, 0, unroll=4)
    p0, v1, a1, a2, r0 = (res[i, 8:24, 0:NX] for i in range(5))
    x_out[...] = (
        st[8:24, 0:NX] + (zeta[0] * p0 + zeta[1] * v1 + zeta[2] * a1) - comb[0]
    )
    r_out[...] = r0 - (zeta[0] * v1 + zeta[1] * a1 + zeta[2] * a2) + comb[1]


def shards(right_side, first_guess, cell_mask, cond_east, cond_north, surface, recycled):
    sizes = tuple(lax.axis_size(axis) for axis in AXES)
    ny_dev, nzh, nx_dev, nzl, ncore = sizes
    na, nb, nc = nx_dev * ncore, ny_dev, nzh * nzl
    nd, ne = nx_dev * ny_dev, nzh * nzl * ncore
    field = jax.ShapeDtypeStruct((NY, NX), f32)
    vmem = pltpu.VMEM
    dma = pltpu.SemaphoreType.DMA
    return pl.pallas_call(
        functools.partial(kernel, sizes),
        out_shape=(field, field),
        in_specs=[pl.BlockSpec(memory_space=pl.ANY)] * 7,
        out_specs=(pl.BlockSpec(memory_space=pltpu.VMEM),) * 2,
        scratch_shapes=[
            vmem((ROWS, K, WIDE), f32),
            vmem((ROWS, K, WIDE), f32),
            vmem((NY, K, NX), f32),
            vmem((6, NAT, WIDE), f32),
            vmem((6, NAT, NX), f32),
            vmem((5, NAT, WIDE), f32),
            vmem((NAT, WIDE), f32),
            vmem((5, NAT, WIDE), f32),
            vmem((NY, NX), jnp.int32),
            vmem((2, K, 128), f32),
            vmem((6, K, 128), f32),
            vmem((2, NY, 128), f32),
            vmem((6, NY, 128), f32),
            vmem((3, 3, 8, 128), f32),
            vmem((2, na, 8, 128), f32),
            vmem((2, nb, 8, 128), f32),
            vmem((2, nc, 8, 128), f32),
            vmem((nd, 128), f32),
            vmem((ne, 128), f32),
            vmem((2, NY, NX), f32),
            vmem((2, 2, K, NX), f32),
            dma((22,)),
            dma((28,)),
            dma((28,)),
            dma((2, na)),
            dma((2, nb)),
            dma((2, nc)),
            dma((nd,)),
            dma((ne,)),
            dma((2, na)),
            dma((2, nb)),
            dma((2, nc)),
            dma((nd,)),
            dma((ne,)),
        ],
        compiler_params=pltpu.CompilerParams(collective_id=0, has_side_effects=True),
    )(right_side, first_guess, cell_mask, cond_east, cond_north, surface, recycled)


def finer_mesh(mesh):
    return Mesh(mesh.devices.reshape(8, 3, 4, 4, 2), AXES)


def solution(mesh):
    in_specs = (P(LAT, LON),) * 6 + (P(None, LAT, LON),)
    out_specs = (P(LAT, LON), P(LAT, LON))
    return jax.shard_map(
        shards, mesh=finer_mesh(mesh), in_specs=in_specs, out_specs=out_specs, check_vma=False
    )
```

```python
import functools

import jax
import jax.numpy as jnp
from jax import lax
from jax.experimental import pallas as pl
from jax.experimental.pallas import tpu as pltpu
from jax.sharding import Mesh
from jax.sharding import PartitionSpec as P

LAT = ("lat_0", "lat_1", "lat_2")
LON = ("lon_0", "lon_1")
AXES = LAT + LON
MESH = pl.DeviceIdType.MESH
HIGHEST = lax.Precision.HIGHEST

K = 16
DEPTH = 4
SHIFT = 4.0
NY = 16
NX = 640
WIDE = NX + 128
ROWS = NY + 2 * DEPTH
NAT = NY + 16
WET, NORTH, GUESS, EAST, SURF, RHS = range(6)

f32 = jnp.float32


def far_first(n):
    return sorted(range(1, n), key=lambda d: -min(d, n - d))


def iota(shape, axis):
    return lax.broadcasted_iota(jnp.int32, shape, axis)


def kernel(
    sizes,
    rhs_hbm,
    guess_hbm,
    mask_hbm,
    east_hbm,
    north_hbm,
    surf_hbm,
    rec_hbm,
    out,
    vec,
    img1,
    img2,
    nat,
    land,
    coef,
    st,
    res,
    mask_v,
    pack_vec,
    got_vec,
    pack_nat,
    got_nat,
    ar_send,
    ar_a,
    ar_b,
    ar_c,
    ar_d,
    ar_e,
    comb,
    relay,
    in_sem,
    halo_send,
    halo_recv,
    ssem_a,
    ssem_b,
    ssem_c,
    ssem_d,
    ssem_e,
    rsem_a,
    rsem_b,
    rsem_c,
    rsem_d,
    rsem_e,
):
    ny_dev, nzh, nx_dev, nzl, ncore = sizes
    my_y = lax.axis_index("lat_0")
    my_zh = lax.axis_index("lat_1")
    my_x = lax.axis_index("lat_2")
    my_zl = lax.axis_index("lon_0")
    my_c = lax.axis_index("lon_1")
    n_lat = ny_dev * nzh * nx_dev
    n_lon = nzl * ncore
    my_lat = (my_y * nzh + my_zh) * nx_dev + my_x
    my_lon = my_zl * ncore + my_c
    na, nb, nc = nx_dev * ncore, ny_dev, nzh * nzl
    nd, ne = nx_dev * ny_dev, nzh * nzl * ncore
    my_a = my_x * ncore + my_c
    my_z = my_zh * nzl + my_zl
    my_d = my_y * nx_dev + my_x
    my_e = my_z * ncore + my_c

    def at_cell(up, right):
        lat = lax.rem(my_lat + (up + n_lat), n_lat)
        lon = lax.rem(my_lon + (right + n_lon), n_lon)
        rest = lat // nx_dev
        return (
            rest // nzh,
            lax.rem(rest, nzh),
            lax.rem(lat, nx_dev),
            lon // ncore,
            lax.rem(lon, ncore),
        )

    def at_a(index):
        return (my_y, my_zh, index // ncore, my_zl, lax.rem(index, ncore))

    def at_b(index):
        return (index, my_zh, my_x, my_zl, my_c)

    def at_c(index):
        return (my_y, index // nzl, my_x, lax.rem(index, nzl), my_c)

    def at_d(index):
        return (index // nx_dev, my_zh, lax.rem(index, nx_dev), my_zl, my_c)

    def at_e(index):
        z = index // ncore
        return (my_y, z // nzl, my_x, lax.rem(z, nzl), lax.rem(index, ncore))

    north_of, south_of = at_cell(1, 0), at_cell(-1, 0)
    east_of, west_of = at_cell(0, 1), at_cell(0, -1)
    corners = (at_cell(1, 1), at_cell(1, -1), at_cell(-1, 1), at_cell(-1, -1))

    barrier = pltpu.get_barrier_semaphore()
    peers = [north_of, south_of, *corners, east_of, west_of]
    for n, me, at in ((ne, my_e, at_e), (nd, my_d, at_d), (na, my_a, at_a)):
        for d in far_first(n):
            peers.append(at(lax.rem(me + d, n)))
    for peer in peers:
        pl.semaphore_signal(barrier, inc=1, device_id=peer, device_id_type=MESH)

    plain = (
        (east_hbm, EAST),
        (north_hbm, NORTH),
        (surf_hbm, SURF),
        (rhs_hbm, RHS),
        (guess_hbm, GUESS),
    )
    loads = [pltpu.make_async_copy(mask_hbm, mask_v, in_sem.at[0])]
    for i, (src, field) in enumerate(plain):
        loads.append(
            pltpu.make_async_copy(
                src, nat.at[field, pl.ds(8, NY), pl.ds(0, NX)], in_sem.at[1 + i]
            )
        )
    for k in range(K):
        loads.append(
            pltpu.make_async_copy(
                rec_hbm.at[k], vec.at[pl.ds(DEPTH, NY), k, pl.ds(0, NX)], in_sem.at[6 + k]
            )
        )
    for load in loads:
        load.start()

    nat[:, 0:8, :] = jnp.zeros((6, 8, WIDE), f32)
    nat[:, 24:32, :] = jnp.zeros((6, 8, WIDE), f32)
    nat[:, 8:24, NX:] = jnp.zeros((6, NY, 128), f32)
    res[:, 0:8, :] = jnp.zeros((5, 8, WIDE), f32)
    res[:, 24:32, :] = jnp.zeros((5, 8, WIDE), f32)

    for load in loads:
        load.wait()
    nat[WET, 8:24, 0:NX] = mask_v[...].astype(f32)

    def remote(src, dst, at, slot):
        return pltpu.make_async_remote_copy(
            src_ref=src,
            dst_ref=dst,
            send_sem=halo_send.at[slot],
            recv_sem=halo_recv.at[slot],
            device_id=at,
            device_id_type=MESH,
        )

    def start_all(copies):
        for copy in copies:
            copy.start()

    def wait_all(copies):
        for copy in copies:
            copy.wait()

    lanes = pl.ds(0, NX)
    lane16 = iota((K, 128), 1)
    sub16 = iota((K, 128), 0)
    zero16 = jnp.zeros((K, 128), f32)

    def pack_vectors():
        def row(y, carry):
            to_west, to_east = carry
            e, lane = y + DEPTH, DEPTH * y
            first = pltpu.roll(vec[e, :, 0:128], lane, 1)
            last = pltpu.roll(vec[e, :, NX - 128 : NX], lane + DEPTH, 1)
            mine = (lane16 >= lane) & (lane16 < lane + DEPTH)
            return jnp.where(mine, first, to_west), jnp.where(mine, last, to_east)

        to_west, to_east = lax.fori_loop(0, NY, row, (zero16, zero16), unroll=4)
        pack_vec[0] = to_west
        pack_vec[1] = to_east

    def edge_columns(from_east, from_west, lane):
        return jnp.where(
            lane < DEPTH, from_east, jnp.where(lane >= 128 - DEPTH, from_west, 0.0)
        )

    def unpack_vectors(first, count, y0, place):
        def row(i, carry):
            lane = DEPTH * (y0 + i)
            from_east = pltpu.roll(got_vec[place], lax.rem(128 - lane, 128), 1)
            from_west = pltpu.roll(got_vec[place + 1], 128 - DEPTH - lane, 1)
            vec[first + i, :, NX:] = edge_columns(from_east, from_west, lane16)
            return carry

        lax.fori_loop(0, count, row, 0, unroll=4)

    def pack_plain():
        to_west, to_east = zero16, zero16
        for i in range(6):
            lane = DEPTH * i
            first, last = nat[i, 8:24, 0:128], nat[i, 8:24, NX - 128 : NX]
            if i:
                first = pltpu.roll(first, lane, 1)
            last = pltpu.roll(last, lane + DEPTH, 1)
            mine = (lane16 >= lane) & (lane16 < lane + DEPTH)
            to_west = jnp.where(mine, first, to_west)
            to_east = jnp.where(mine, last, to_east)
        pack_nat[0] = to_west
        pack_nat[1] = to_east

    def unpack_plain(first, count, y0, place):
        lane = lane16[0:count]
        for i in range(6):
            from_east = got_nat[place, y0 : y0 + count, :]
            from_west = got_nat[place + 1, y0 : y0 + count, :]
            if i:
                from_east = pltpu.roll(from_east, 128 - DEPTH * i, 1)
            from_west = pltpu.roll(from_west, 128 - DEPTH - DEPTH * i, 1)
            nat[i, first : first + count, NX:] = edge_columns(from_east, from_west, lane)

    def landed(first, count, near, far):
        for i in range(first, first + count):
            nat[i, 8 - far : 9 - near, 0:NX] = land[i, 8 - far : 9 - near, :]
            nat[i, 23 + near : 24 + far, 0:NX] = land[i, 23 + near : 24 + far, :]

    def vector_rows(near, far, slot):
        n = far - near + 1
        return [
            remote(
                vec.at[pl.ds(20 - far, n), :, lanes],
                vec.at[pl.ds(4 - far, n), :, lanes],
                north_of,
                slot,
            ),
            remote(
                vec.at[pl.ds(3 + near, n), :, lanes],
                vec.at[pl.ds(19 + near, n), :, lanes],
                south_of,
                slot + 1,
            ),
        ]

    def far_rows():
        ahead, behind = lax.rem(my_zh + 1, nzh), lax.rem(my_zh + (nzh - 1), nzh)
        next_y = jnp.where(my_zh == nzh - 1, lax.rem(my_y + 1, ny_dev), my_y)
        last_y = jnp.where(my_zh == 0, lax.rem(my_y + (ny_dev - 1), ny_dev), my_y)
        ways = (
            (
                my_x == nx_dev - 1,
                my_x == 0,
                vec.at[pl.ds(16, 2), :, lanes],
                vec.at[pl.ds(0, 2), :, lanes],
                north_of,
                (next_y, my_zh, 0, my_zl, my_c),
                (my_y, ahead, my_x, my_zl, my_c),
            ),
            (
                my_x == 0,
                my_x == nx_dev - 1,
                vec.at[pl.ds(6, 2), :, lanes],
                vec.at[pl.ds(22, 2), :, lanes],
                south_of,
                (last_y, my_zh, nx_dev - 1, my_zl, my_c),
                (my_y, behind, my_x, my_zl, my_c),
            ),
        )

        def copy(src, dst, at, send_slot, recv_slot):
            return pltpu.make_async_remote_copy(
                src_ref=src,
                dst_ref=dst,
                send_sem=halo_send.at[send_slot],
                recv_sem=halo_recv.at[recv_slot],
                device_id=at,
                device_id_type=MESH,
            )

        hops = []
        for i, (crosses, forwards, src, dst, straight, first_hop, last_hop) in enumerate(ways):
            held = relay.at[i]
            hops.append(
                (
                    crosses,
                    forwards,
                    copy(src, dst, straight, 22 + i, 22 + i),
                    copy(src, held, first_hop, 24 + i, 24 + i),
                    copy(held, dst, last_hop, 26 + i, 22 + i),
                )
            )

        def begin():
            for crosses, _, straight, first, _ in hops:
                pl.when(jnp.logical_not(crosses))(straight.start)
                pl.when(crosses)(first.start)

        def forward():
            for _, forwards, _, first, last in hops:

                @pl.when(forwards)
                def _():
                    first.wait_recv()
                    last.start()

        def finish():
            for crosses, forwards, straight, first, last in hops:
                pl.when(jnp.logical_not(crosses))(straight.wait_send)
                pl.when(crosses)(first.wait_send)
                pl.when(forwards)(last.wait_send)
                straight.wait_recv()

        return begin, forward, finish

    def columns(pack, got, slot):
        return [
            remote(pack.at[0], got.at[0], west_of, slot),
            remote(pack.at[1], got.at[1], east_of, slot + 1),
        ]

    def corner_columns(pack, got, slot, south_rows, north_rows):
        north_east, north_west, south_east, south_west = corners
        return [
            remote(pack.at[0, south_rows], got.at[2, south_rows], south_west, slot),
            remote(pack.at[1, south_rows], got.at[3, south_rows], south_east, slot + 1),
            remote(pack.at[0, north_rows], got.at[4, north_rows], north_west, slot + 2),
            remote(pack.at[1, north_rows], got.at[5, north_rows], north_east, slot + 3),
        ]

    def plain_rows(first, count, near, far, slot):
        fields, n = pl.ds(first, count), far - near + 1
        return [
            remote(
                nat.at[fields, pl.ds(24 - far, n), lanes],
                land.at[fields, pl.ds(8 - far, n)],
                north_of,
                slot,
            ),
            remote(
                nat.at[fields, pl.ds(7 + near, n), lanes],
                land.at[fields, pl.ds(23 + near, n)],
                south_of,
                slot + 1,
            ),
        ]

    pack_vectors()
    pack_plain()
    pl.semaphore_wait(barrier, len(peers))

    near_rows = plain_rows(0, 3, 1, 1, 0)
    vec_rows = vector_rows(1, 1, 2)
    vec_columns = columns(pack_vec, got_vec, 4)
    near_columns = columns(pack_nat, got_nat, 6)
    all_rows = pl.ds(0, NY)
    far = far_rows()
    deep = (
        corner_columns(pack_nat, got_nat, 18, pl.ds(0, 8), pl.ds(8, 8))
        + plain_rows(0, 3, 2, DEPTH, 8)
        + plain_rows(3, 3, 1, DEPTH - 1, 10)
        + corner_columns(pack_vec, got_vec, 14, all_rows, all_rows)
        + vector_rows(2, 2, 12)
    )
    start_all(near_columns)
    start_all(vec_columns)
    start_all(near_rows)
    start_all(vec_rows)

    def east(v):
        return pltpu.roll(v, WIDE - 1, 1)

    def west(v):
        return pltpu.roll(v, 1, 1)

    def north(v):
        return pltpu.roll(v, NAT - 1, 0)

    def south(v):
        return pltpu.roll(v, 1, 0)

    def coefficients():
        row_n = iota((NAT, WIDE), 0)
        beyond = ((row_n < 8) & (my_lat == 0)) | ((row_n >= 24) & (my_lat == n_lat - 1))
        wet = jnp.where(beyond, 0.0, nat[WET])
        k_east = nat[EAST] * wet * east(wet)
        k_north = nat[NORTH] * wet * north(wet)
        k_west = west(k_east)
        k_south = south(k_north)
        coef[1] = k_east
        coef[2] = k_west
        coef[3] = k_north
        coef[4] = k_south
        coef[0] = nat[SURF] * wet + k_east + k_west + k_north + k_south + (1.0 - wet)

    def operate(v):
        return coef[0] * v - (
            coef[1] * east(v) + coef[2] * west(v) + coef[3] * north(v) + coef[4] * south(v)
        )

    def image_row(src, e):
        at = pl.ds(e + 4, 1)
        v = src[e]
        return coef[0, at, :] * v - (
            coef[1, at, :] * east(v)
            + coef[2, at, :] * west(v)
            + coef[3, at, :] * src[e + 1]
            + coef[4, at, :] * src[e - 1]
        )

    def fold(v):
        total = v[:, 0:128]
        for i in range(1, NX // 128):
            total = total + v[:, 128 * i : 128 * i + 128]
        return total

    def contract(a, b):
        return lax.dot_general(
            a, b, (((1,), (1,)), ((), ())), precision=HIGHEST, preferred_element_type=f32
        )

    def first_pair(rows, carry):
        acc, w_s, b_s = carry
        both = []
        for y in rows:
            w = vec[y + DEPTH, :, 0:NX]
            image = image_row(vec, y + DEPTH)
            img1[y + DEPTH] = image
            b = image[:, 0:NX]
            s = st[pl.ds(y + 8, 1), 0:NX]
            w_s = w_s + fold(w * s)
            b_s = b_s + fold(b * s)
            both.append(jnp.concatenate([w, b], axis=0))
        both = jnp.concatenate(both, axis=1)
        return acc + contract(both, both), w_s, b_s

    def start_residual():
        st[...] = nat[RHS] - operate(nat[GUESS])

    wait_all(near_columns)
    unpack_plain(8, NY, 0, 0)
    coefficients()
    start_residual()
    wait_all(vec_columns)
    unpack_vectors(DEPTH, NY, 0, 0)
    far[0]()
    carry = (jnp.zeros((2 * K, 2 * K), f32), zero16, zero16)
    carry = lax.fori_loop(
        0, NY // 2 - 1, lambda i, c: first_pair((2 * i + 1, 2 * i + 2), c), carry
    )
    start_all(deep)
    far[1]()
    wait_all(near_rows)
    landed(0, 3, 1, 1)
    wait_all(vec_rows)
    coefficients()
    start_residual()
    acc, w_s, b_s = first_pair((0, NY - 1), carry)

    def put(block, lane):
        wide = jnp.concatenate([block, jnp.zeros((K, 128 - block.shape[1]), f32)], axis=1)
        return pltpu.roll(wide, lane, 1) if lane else wide

    def column(payload, lane, total):
        return jnp.where(lane16 == lane, jnp.sum(total, axis=1, keepdims=True), payload)

    def pack(v, width):
        per, shift = 128 // width, width
        while shift < 128:
            v = v + pltpu.roll(v, shift, 1)
            shift *= 2
        v = jnp.where(lane16 // width == lax.rem(sub16, per), v, 0.0)
        return [
            jnp.sum(jnp.where(sub16 // per == i, v, 0.0), axis=0, keepdims=True)
            for i in range(K // per)
        ]

    def unpack(rows, width):
        per, shift = 128 // width, width
        v = jnp.broadcast_to(rows[0], (K, 128))
        for i in range(1, K // per):
            v = jnp.where(sub16 // per == i, rows[i], v)
        v = jnp.where(lane16 // width == lax.rem(sub16, per), v, 0.0)
        while shift < 128:
            v = v + pltpu.roll(v, shift, 1)
            shift *= 2
        return jnp.where(lane16 < width, v, 0.0)

    def send_phase(phase, value):
        send, buf, ssem, rsem, n, me, at, count = phase
        if count == 1:
            send[0:1, :] = value
            src, dst = send.at[pl.ds(0, 1)], buf.at[pl.ds(me, 1)]
        else:
            for i, row in enumerate(value):
                send[i : i + 1, :] = row
            src, dst = send.at[pl.ds(0, count)], buf.at[me, pl.ds(0, count)]
        for d in far_first(n):
            pltpu.make_async_remote_copy(
                src_ref=src,
                dst_ref=dst,
                send_sem=ssem.at[d],
                recv_sem=rsem.at[me],
                device_id=at(lax.rem(me + d, n)),
                device_id_type=MESH,
            ).start()
        if count == 1:
            buf[pl.ds(me, 1), :] = value
        else:
            for i, row in enumerate(value):
                buf[me, i : i + 1, :] = row

    def wait_phase(phase):
        send, buf, ssem, rsem, n, me, at, count = phase
        for d in range(1, n):
            peer = lax.rem(me + d, n)
            if count == 1:
                src, dst = send.at[pl.ds(0, 1)], buf.at[pl.ds(peer, 1)]
            else:
                src, dst = send.at[pl.ds(0, count)], buf.at[peer, pl.ds(0, count)]
            pltpu.make_async_remote_copy(
                src_ref=src,
                dst_ref=dst,
                send_sem=ssem.at[d],
                recv_sem=rsem.at[peer],
                device_id=at(peer),
                device_id_type=MESH,
            ).wait()
        if count == 1:
            return jnp.sum(buf[...], axis=0, keepdims=True)
        total = buf[0]
        for i in range(1, n):
            total = total + buf[i]
        return [total[i : i + 1, :] for i in range(count)]

    def three_phases(turn, count):
        return (
            (ar_send.at[turn, 0], ar_a.at[turn], ssem_a.at[turn], rsem_a.at[turn], na, my_a, at_a, count),
            (ar_send.at[turn, 1], ar_b.at[turn], ssem_b.at[turn], rsem_b.at[turn], nb, my_y, at_b, count),
            (ar_send.at[turn, 2], ar_c.at[turn], ssem_c.at[turn], rsem_c.at[turn], nc, my_z, at_c, count),
        )

    two_phases = (
        (ar_send.at[2, 0], ar_d, ssem_d, rsem_d, nd, my_d, at_d, 1),
        (ar_send.at[2, 1], ar_e, ssem_e, rsem_e, ne, my_e, at_e, 1),
    )

    def all_reduce(phases, value, between):
        for step, phase in enumerate(phases):
            send_phase(phase, value)
            if between[step] is not None:
                between[step]()
            value = wait_phase(phase)
        return value

    g3_phases = three_phases(1, 2)
    kept = {}

    def second_pair(rows, acc):
        left, right = [], []
        for y in rows:
            left.append(img1[y + DEPTH, :, 0:NX])
            right.append(image_row(img1, y + DEPTH)[:, 0:NX])
            img2[y] = right[-1]
        left, right = jnp.concatenate(left, axis=1), jnp.concatenate(right, axis=1)
        return acc + contract(left, right)

    def between_a():
        acc = jnp.zeros((K, K), f32)
        kept["g3"] = lax.fori_loop(
            0, NY // 2 - 1, lambda i, c: second_pair((2 * i + 1, 2 * i + 2), c), acc
        )

    def between_c():
        wait_all(deep)
        far[2]()
        landed(0, 3, 2, DEPTH)
        landed(3, 3, 1, DEPTH - 1)
        unpack_plain(24, 8, 0, 2)
        unpack_plain(0, 8, 8, 4)
        unpack_vectors(NY + DEPTH, DEPTH, 0, 2)
        unpack_vectors(0, DEPTH, NY - DEPTH, 4)
        coefficients()
        start_residual()

        def outer_row(i, carry):
            img1[i + 1] = image_row(vec, i + 1)
            img1[i + 19] = image_row(vec, i + 19)
            return carry

        lax.fori_loop(0, DEPTH, outer_row, 0)
        acc = second_pair((0, NY - 1), kept["g3"])
        send_phase(g3_phases[0], pack(put(acc, 0), K))

    grams = 0.5 * (put(acc[0:K, K:], 0) + put(acc[K:, 0:K], 0)) + put(acc[K:, K:], K)
    rows = pack(grams, 2 * K) + pack(column(column(zero16, 0, w_s), 1, b_s), 8)
    rows = all_reduce(three_phases(0, 5), rows, (between_a, None, between_c))
    grams = unpack(rows[0:4], 2 * K)
    starts = unpack(rows[4:5], 8)


    def at_zero(v, lane):
        v = jnp.where((lane16 >= lane) & (lane16 < lane + K), v, 0.0)
        return pltpu.roll(v, (128 - lane) % 128, 1) if lane else v

    aug = jnp.where(lane16 < K, grams, 0.0)
    aug = jnp.where(lane16 == sub16 + K, 1.0, aug)
    aug = jnp.where(lane16 == 2 * K, starts[:, 0:1], aug)
    for i in range(K):
        pivot_row = aug[i : i + 1, :] / aug[i : i + 1, i : i + 1]
        aug = jnp.where(sub16 == i, pivot_row, aug - aug[:, i : i + 1] * pivot_row)
    coarse = aug[:, 2 * K : 2 * K + 1]
    inverse = at_zero(aug, K)
    g1, g2 = at_zero(grams, 0), at_zero(grams, K)

    def as_row(col):
        return jnp.sum(jnp.where(lane16 == sub16, col, 0.0), axis=0, keepdims=True)

    def row_times(mat, row):
        return jnp.sum(mat * row, axis=1, keepdims=True)

    def times_column(mat, col):
        return jnp.sum(mat * col, axis=0, keepdims=True)

    def apply(mat, col):
        return row_times(mat, as_row(col))

    def dot(a, b):
        return jnp.sum(a * b, axis=0, keepdims=True)

    w_row, b_row = as_row(starts[:, 0:1]), as_row(starts[:, 1:2])
    coarse = coarse + row_times(inverse, w_row - times_column(g1, coarse))
    mu0 = row_times(inverse, b_row - times_column(g2, coarse))


    def residual_row(e, carry):
        at = pl.ds(e + 4, 1)
        r = st[at, :] - jnp.sum(coarse * img1[e], axis=0, keepdims=True)
        res[4, at, :] = r
        res[0, at, :] = r - jnp.sum(mu0 * vec[e], axis=0, keepdims=True)
        return carry

    lax.fori_loop(1, ROWS - 1, residual_row, 0, unroll=2)
    send_phase(g3_phases[1], wait_phase(g3_phases[0]))
    for i, base in enumerate((4, 1, 2)):
        res[i + 1] = operate(res[i]) - SHIFT * res[base]

    def moment_row(y, carry):
        b1, b2 = img1[y + DEPTH, :, 0:NX], img2[y]
        v1, a1 = (res[i, pl.ds(y + 8, 1), 0:NX] for i in (1, 2))
        terms = (b1 * v1, b1 * a1, b2 * a1)
        return tuple(total + fold(term) for total, term in zip(carry, terms))

    defl = lax.fori_loop(0, NY, moment_row, (zero16,) * 3, unroll=2)
    payload = zero16
    for i, total in enumerate(defl):
        payload = column(payload, i, total)
    inner = [res[i, 8:24, 0:NX] for i in (4, 1, 2, 3)]
    for i, (a, b) in enumerate(((0, 0), (0, 1), (1, 1), (1, 2), (2, 2), (2, 3))):
        total = jnp.sum(fold(inner[a] * inner[b]), axis=0, keepdims=True)
        total = jnp.sum(total, axis=1, keepdims=True)
        payload = jnp.where((lane16 == 3) & (sub16 == i), total, payload)

    def before_scalars():
        def row(y, carry):
            at = pl.ds(y + 8, 1)
            along = jnp.sum(coarse * vec[y + DEPTH, :, 0:NX], axis=0, keepdims=True)
            st[at, 0:NX] = nat[GUESS, at, 0:NX] + along
            return carry

        lax.fori_loop(0, NY, row, 0, unroll=4)
        send_phase(g3_phases[2], wait_phase(g3_phases[1]))

    def last_gram():
        kept["g3"] = unpack(wait_phase(g3_phases[2]), K)

    row = all_reduce(two_phases, pack(payload, 8)[0], (before_scalars, last_gram))
    sums = unpack([row], 8)

    g3 = kept["g3"]
    e = [sums[:, i : i + 1] for i in range(3)]
    t = [sums[i : i + 1, 3:4] for i in range(6)]
    mu1 = apply(inverse, e[0])
    g2_1, g3_1 = apply(g2, mu1), apply(g3, mu1)
    defl2 = e[1] - g2_1
    mu2 = apply(inverse, defl2)
    m = [
        t[0],
        t[1],
        t[2],
        t[3] - dot(mu1, e[0]),
        t[4] - 2.0 * dot(mu1, e[1]) + dot(mu1, g2_1),
        t[5]
        - 2.0 * dot(mu1, e[2] - SHIFT * e[1])
        + dot(mu1, g3_1 - SHIFT * g2_1)
        - dot(mu2, defl2),
    ]

    def form(poly, shift):
        total = 0.0
        for i, a in enumerate(poly):
            for j, b in enumerate(poly):
                total = total + a * b * m[i + j + shift]
        return total

    one = jnp.ones((1, 1), f32)
    zero = jnp.zeros((1, 1), f32)
    r_poly = [one]
    y_poly = [zero]
    zeta = [zero, zero, zero]
    curv = prev_norm = one
    for turn in range(3):
        norm = form(r_poly, 0)
        r_image = form(r_poly, 1) + SHIFT * norm
        if turn == 0:
            y_poly = list(r_poly)
            curv = r_image
        else:
            ratio = norm / prev_norm
            y_poly = [a + ratio * b for a, b in zip(r_poly, y_poly + [zero])]
            curv = r_image - ratio * ratio * curv
        step_len = norm / curv
        for i, a in enumerate(y_poly):
            zeta[i] = zeta[i] + step_len * a
        y_image = [a + SHIFT * b for a, b in zip([zero] + y_poly, y_poly + [zero])]
        r_poly = [a - step_len * b for a, b in zip(r_poly + [zero], y_image)]
        prev_norm = norm

    along_w = zeta[1] * mu1 + zeta[2] * mu2
    along_b = zeta[2] * mu1
    res_b = (r_poly[2] - SHIFT * r_poly[3]) * mu1 + r_poly[3] * mu2
    res_bb = r_poly[3] * mu1

    def final_row(y, carry):
        w, b1, b2 = vec[y + DEPTH, :, 0:NX], img1[y + DEPTH, :, 0:NX], img2[y]
        at = pl.ds(y, 1)
        comb[0, at, :] = jnp.sum(along_w * w + along_b * b1, axis=0, keepdims=True)
        comb[1, at, :] = jnp.sum(res_b * b1 + res_bb * b2, axis=0, keepdims=True)
        return carry

    lax.fori_loop(0, NY, final_row, 0, unroll=4)
    p0, v1, a1, a2, r0 = (res[i, 8:24, 0:NX] for i in range(5))
    out[0] = (
        st[8:24, 0:NX] + (zeta[0] * p0 + zeta[1] * v1 + zeta[2] * a1) - comb[0]
    )
    out[1] = (
        r_poly[0] * r0 + (r_poly[1] * v1 + r_poly[2] * a1 + r_poly[3] * a2) - comb[1]
    )


def shards(right_side, first_guess, cell_mask, cond_east, cond_north, surface, recycled):
    sizes = tuple(lax.axis_size(axis) for axis in AXES)
    ny_dev, nzh, nx_dev, nzl, ncore = sizes
    na, nb, nc = nx_dev * ncore, ny_dev, nzh * nzl
    nd, ne = nx_dev * ny_dev, nzh * nzl * ncore
    vmem = pltpu.VMEM
    dma = pltpu.SemaphoreType.DMA
    both = pl.pallas_call(
        functools.partial(kernel, sizes),
        out_shape=jax.ShapeDtypeStruct((2, NY, NX), f32),
        in_specs=[pl.BlockSpec(memory_space=pl.ANY)] * 7,
        out_specs=pl.BlockSpec(memory_space=pltpu.VMEM),
        scratch_shapes=[
            vmem((ROWS, K, WIDE), f32),
            vmem((ROWS, K, WIDE), f32),
            vmem((NY, K, NX), f32),
            vmem((6, NAT, WIDE), f32),
            vmem((6, NAT, NX), f32),
            vmem((5, NAT, WIDE), f32),
            vmem((NAT, WIDE), f32),
            vmem((5, NAT, WIDE), f32),
            vmem((NY, NX), jnp.int32),
            vmem((2, K, 128), f32),
            vmem((6, K, 128), f32),
            vmem((2, NY, 128), f32),
            vmem((6, NY, 128), f32),
            vmem((3, 3, 8, 128), f32),
            vmem((2, na, 8, 128), f32),
            vmem((2, nb, 8, 128), f32),
            vmem((2, nc, 8, 128), f32),
            vmem((nd, 128), f32),
            vmem((ne, 128), f32),
            vmem((2, NY, NX), f32),
            vmem((2, 2, K, NX), f32),
            dma((22,)),
            dma((28,)),
            dma((28,)),
            dma((2, na)),
            dma((2, nb)),
            dma((2, nc)),
            dma((nd,)),
            dma((ne,)),
            dma((2, na)),
            dma((2, nb)),
            dma((2, nc)),
            dma((nd,)),
            dma((ne,)),
        ],
        compiler_params=pltpu.CompilerParams(collective_id=0, has_side_effects=True),
    )(right_side, first_guess, cell_mask, cond_east, cond_north, surface, recycled)
    return both[0], both[1]


def finer_mesh(mesh):
    return Mesh(mesh.devices.reshape(8, 3, 4, 4, 2), AXES)


def solution(mesh):
    in_specs = (P(LAT, LON),) * 6 + (P(None, LAT, LON),)
    out_specs = (P(LAT, LON), P(LAT, LON))
    return jax.shard_map(
        shards, mesh=finer_mesh(mesh), in_specs=in_specs, out_specs=out_specs, check_vma=False
    )
```

```python
import functools

import jax
import jax.numpy as jnp
from jax import lax
from jax.experimental import pallas as pl
from jax.experimental.pallas import tpu as pltpu
from jax.sharding import Mesh
from jax.sharding import PartitionSpec as P

LAT = ("lat_0", "lat_1", "lat_2")
LON = ("lon_0", "lon_1")
AXES = LAT + LON
MESH = pl.DeviceIdType.MESH
HIGHEST = lax.Precision.HIGHEST

K = 16
DEPTH = 4
SHIFT = 4.0
NY = 16
NX = 640
WIDE = NX + 128
ROWS = NY + 2 * DEPTH
NAT = NY + 16
WET, NORTH, GUESS, EAST, SURF, RHS = range(6)

f32 = jnp.float32


def far_first(n):
    return sorted(range(1, n), key=lambda d: -min(d, n - d))


def iota(shape, axis):
    return lax.broadcasted_iota(jnp.int32, shape, axis)


def kernel(
    sizes,
    rhs_hbm,
    guess_hbm,
    mask_hbm,
    east_hbm,
    north_hbm,
    surf_hbm,
    rec_hbm,
    out,
    vec,
    img1,
    img2,
    nat,
    land,
    coef,
    st,
    res,
    mask_v,
    pack_vec,
    got_vec,
    pack_nat,
    got_nat,
    ar_send,
    ar_a,
    ar_b,
    ar_c,
    ar_d,
    ar_e,
    comb,
    relay,
    in_sem,
    halo_send,
    halo_recv,
    ssem_a,
    ssem_b,
    ssem_c,
    ssem_d,
    ssem_e,
    rsem_a,
    rsem_b,
    rsem_c,
    rsem_d,
    rsem_e,
):
    ny_dev, nzh, nx_dev, nzl, ncore = sizes
    my_y = lax.axis_index("lat_0")
    my_zh = lax.axis_index("lat_1")
    my_x = lax.axis_index("lat_2")
    my_zl = lax.axis_index("lon_0")
    my_c = lax.axis_index("lon_1")
    n_lat = ny_dev * nzh * nx_dev
    n_lon = nzl * ncore
    my_lat = (my_y * nzh + my_zh) * nx_dev + my_x
    my_lon = my_zl * ncore + my_c
    na, nb, nc = nx_dev * ncore, ny_dev, nzh * nzl
    nd, ne = nx_dev * ny_dev, nzh * nzl * ncore
    my_a = my_x * ncore + my_c
    my_z = my_zh * nzl + my_zl
    my_d = my_y * nx_dev + my_x
    my_e = my_z * ncore + my_c

    def at_cell(up, right):
        lat = lax.rem(my_lat + (up + n_lat), n_lat)
        lon = lax.rem(my_lon + (right + n_lon), n_lon)
        rest = lat // nx_dev
        return (
            rest // nzh,
            lax.rem(rest, nzh),
            lax.rem(lat, nx_dev),
            lon // ncore,
            lax.rem(lon, ncore),
        )

    def at_a(index):
        return (my_y, my_zh, index // ncore, my_zl, lax.rem(index, ncore))

    def at_b(index):
        return (index, my_zh, my_x, my_zl, my_c)

    def at_c(index):
        return (my_y, index // nzl, my_x, lax.rem(index, nzl), my_c)

    def at_d(index):
        return (index // nx_dev, my_zh, lax.rem(index, nx_dev), my_zl, my_c)

    def at_e(index):
        z = index // ncore
        return (my_y, z // nzl, my_x, lax.rem(z, nzl), lax.rem(index, ncore))

    north_of, south_of = at_cell(1, 0), at_cell(-1, 0)
    east_of, west_of = at_cell(0, 1), at_cell(0, -1)
    corners = (at_cell(1, 1), at_cell(1, -1), at_cell(-1, 1), at_cell(-1, -1))

    plain = (
        (east_hbm, EAST),
        (north_hbm, NORTH),
        (surf_hbm, SURF),
        (rhs_hbm, RHS),
        (guess_hbm, GUESS),
    )
    loads = [pltpu.make_async_copy(mask_hbm, mask_v, in_sem.at[0])]
    for i, (src, field) in enumerate(plain):
        loads.append(
            pltpu.make_async_copy(
                src, nat.at[field, pl.ds(8, NY), pl.ds(0, NX)], in_sem.at[1 + i]
            )
        )
    for k in range(K):
        loads.append(
            pltpu.make_async_copy(
                rec_hbm.at[k], vec.at[pl.ds(DEPTH, NY), k, pl.ds(0, NX)], in_sem.at[6 + k]
            )
        )
    for load in loads:
        load.start()

    barrier = pltpu.get_barrier_semaphore()
    peers = [north_of, south_of, *corners, east_of, west_of]
    groups = [
        [at(lax.rem(me + d, n)) for d in far_first(n)]
        for n, me, at in ((ne, my_e, at_e), (nd, my_d, at_d), (na, my_a, at_a))
    ]
    for i in range(max(len(group) for group in groups)):
        peers += [group[i] for group in groups if i < len(group)]
    for peer in peers:
        pl.semaphore_signal(barrier, inc=1, device_id=peer, device_id_type=MESH)

    nat[:, 0:8, :] = jnp.zeros((6, 8, WIDE), f32)
    nat[:, 24:32, :] = jnp.zeros((6, 8, WIDE), f32)
    nat[:, 8:24, NX:] = jnp.zeros((6, NY, 128), f32)
    res[:, 0:8, :] = jnp.zeros((5, 8, WIDE), f32)
    res[:, 24:32, :] = jnp.zeros((5, 8, WIDE), f32)

    for load in loads:
        load.wait()
    nat[WET, 8:24, 0:NX] = mask_v[...].astype(f32)

    def remote(src, dst, at, slot):
        return pltpu.make_async_remote_copy(
            src_ref=src,
            dst_ref=dst,
            send_sem=halo_send.at[slot],
            recv_sem=halo_recv.at[slot],
            device_id=at,
            device_id_type=MESH,
        )

    def start_all(copies):
        for copy in copies:
            copy.start()

    def wait_all(copies):
        for copy in copies:
            copy.wait()

    lanes = pl.ds(0, NX)
    lane16 = iota((K, 128), 1)
    sub16 = iota((K, 128), 0)
    zero16 = jnp.zeros((K, 128), f32)

    def pack_vectors():
        def row(y, carry):
            to_west, to_east = carry
            e, lane = y + DEPTH, DEPTH * y
            first = pltpu.roll(vec[e, :, 0:128], lane, 1)
            last = pltpu.roll(vec[e, :, NX - 128 : NX], lane + DEPTH, 1)
            mine = (lane16 >= lane) & (lane16 < lane + DEPTH)
            return jnp.where(mine, first, to_west), jnp.where(mine, last, to_east)

        to_west, to_east = lax.fori_loop(0, NY, row, (zero16, zero16), unroll=4)
        pack_vec[0] = to_west
        pack_vec[1] = to_east

    def edge_columns(from_east, from_west, lane):
        return jnp.where(
            lane < DEPTH, from_east, jnp.where(lane >= 128 - DEPTH, from_west, 0.0)
        )

    def unpack_vectors(first, count, y0, place):
        def row(i, carry):
            lane = DEPTH * (y0 + i)
            from_east = pltpu.roll(got_vec[place], lax.rem(128 - lane, 128), 1)
            from_west = pltpu.roll(got_vec[place + 1], 128 - DEPTH - lane, 1)
            vec[first + i, :, NX:] = edge_columns(from_east, from_west, lane16)
            return carry

        lax.fori_loop(0, count, row, 0, unroll=4)

    def pack_plain():
        to_west, to_east = zero16, zero16
        for i in range(6):
            lane = DEPTH * i
            first, last = nat[i, 8:24, 0:128], nat[i, 8:24, NX - 128 : NX]
            if i:
                first = pltpu.roll(first, lane, 1)
            last = pltpu.roll(last, lane + DEPTH, 1)
            mine = (lane16 >= lane) & (lane16 < lane + DEPTH)
            to_west = jnp.where(mine, first, to_west)
            to_east = jnp.where(mine, last, to_east)
        pack_nat[0] = to_west
        pack_nat[1] = to_east

    def unpack_plain(first, count, y0, place):
        lane = lane16[0:count]
        for i in range(6):
            from_east = got_nat[place, y0 : y0 + count, :]
            from_west = got_nat[place + 1, y0 : y0 + count, :]
            if i:
                from_east = pltpu.roll(from_east, 128 - DEPTH * i, 1)
            from_west = pltpu.roll(from_west, 128 - DEPTH - DEPTH * i, 1)
            nat[i, first : first + count, NX:] = edge_columns(from_east, from_west, lane)

    def landed(first, count, near, far):
        for i in range(first, first + count):
            nat[i, 8 - far : 9 - near, 0:NX] = land[i, 8 - far : 9 - near, :]
            nat[i, 23 + near : 24 + far, 0:NX] = land[i, 23 + near : 24 + far, :]

    def vector_rows(near, far, slot):
        n = far - near + 1
        return [
            remote(
                vec.at[pl.ds(20 - far, n), :, lanes],
                vec.at[pl.ds(4 - far, n), :, lanes],
                north_of,
                slot,
            ),
            remote(
                vec.at[pl.ds(3 + near, n), :, lanes],
                vec.at[pl.ds(19 + near, n), :, lanes],
                south_of,
                slot + 1,
            ),
        ]

    def far_rows():
        ahead, behind = lax.rem(my_zh + 1, nzh), lax.rem(my_zh + (nzh - 1), nzh)
        next_y = jnp.where(my_zh == nzh - 1, lax.rem(my_y + 1, ny_dev), my_y)
        last_y = jnp.where(my_zh == 0, lax.rem(my_y + (ny_dev - 1), ny_dev), my_y)
        ways = (
            (
                my_x == nx_dev - 1,
                my_x == 0,
                vec.at[pl.ds(16, 2), :, lanes],
                vec.at[pl.ds(0, 2), :, lanes],
                north_of,
                (next_y, my_zh, 0, my_zl, my_c),
                (my_y, ahead, my_x, my_zl, my_c),
            ),
            (
                my_x == 0,
                my_x == nx_dev - 1,
                vec.at[pl.ds(6, 2), :, lanes],
                vec.at[pl.ds(22, 2), :, lanes],
                south_of,
                (last_y, my_zh, nx_dev - 1, my_zl, my_c),
                (my_y, behind, my_x, my_zl, my_c),
            ),
        )

        def copy(src, dst, at, send_slot, recv_slot):
            return pltpu.make_async_remote_copy(
                src_ref=src,
                dst_ref=dst,
                send_sem=halo_send.at[send_slot],
                recv_sem=halo_recv.at[recv_slot],
                device_id=at,
                device_id_type=MESH,
            )

        hops = []
        for i, (crosses, forwards, src, dst, straight, first_hop, last_hop) in enumerate(ways):
            held = relay.at[i]
            hops.append(
                (
                    crosses,
                    forwards,
                    copy(src, dst, straight, 22 + i, 22 + i),
                    copy(src, held, first_hop, 24 + i, 24 + i),
                    copy(held, dst, last_hop, 26 + i, 22 + i),
                )
            )

        def begin():
            for crosses, _, straight, first, _ in hops:
                pl.when(jnp.logical_not(crosses))(straight.start)
                pl.when(crosses)(first.start)

        def forward():
            for _, forwards, _, first, last in hops:

                @pl.when(forwards)
                def _():
                    first.wait_recv()
                    last.start()

        def finish():
            for crosses, forwards, straight, first, last in hops:
                pl.when(jnp.logical_not(crosses))(straight.wait_send)
                pl.when(crosses)(first.wait_send)
                pl.when(forwards)(last.wait_send)
                straight.wait_recv()

        return begin, forward, finish

    def columns(pack, got, slot):
        return [
            remote(pack.at[0], got.at[0], west_of, slot),
            remote(pack.at[1], got.at[1], east_of, slot + 1),
        ]

    def corner_columns(pack, got, slot, south_rows, north_rows):
        north_east, north_west, south_east, south_west = corners
        return [
            remote(pack.at[0, south_rows], got.at[2, south_rows], south_west, slot),
            remote(pack.at[1, south_rows], got.at[3, south_rows], south_east, slot + 1),
            remote(pack.at[0, north_rows], got.at[4, north_rows], north_west, slot + 2),
            remote(pack.at[1, north_rows], got.at[5, north_rows], north_east, slot + 3),
        ]

    def plain_rows(first, count, near, far, slot):
        fields, n = pl.ds(first, count), far - near + 1
        return [
            remote(
                nat.at[fields, pl.ds(24 - far, n), lanes],
                land.at[fields, pl.ds(8 - far, n)],
                north_of,
                slot,
            ),
            remote(
                nat.at[fields, pl.ds(7 + near, n), lanes],
                land.at[fields, pl.ds(23 + near, n)],
                south_of,
                slot + 1,
            ),
        ]

    pack_vectors()
    pack_plain()
    pl.semaphore_wait(barrier, len(peers))

    near_rows = plain_rows(0, 3, 1, 1, 0)
    vec_rows = vector_rows(1, 1, 2)
    vec_columns = columns(pack_vec, got_vec, 4)
    near_columns = columns(pack_nat, got_nat, 6)
    all_rows = pl.ds(0, NY)
    far = far_rows()
    deep = (
        corner_columns(pack_nat, got_nat, 18, pl.ds(0, 8), pl.ds(8, 8))
        + plain_rows(0, 3, 2, DEPTH, 8)
        + plain_rows(3, 3, 1, DEPTH - 1, 10)
        + corner_columns(pack_vec, got_vec, 14, all_rows, all_rows)
        + vector_rows(2, 2, 12)
    )
    start_all(near_columns)
    start_all(vec_columns)
    start_all(near_rows)
    start_all(vec_rows)
    far[0]()

    def east(v):
        return pltpu.roll(v, WIDE - 1, 1)

    def west(v):
        return pltpu.roll(v, 1, 1)

    def north(v):
        return pltpu.roll(v, NAT - 1, 0)

    def south(v):
        return pltpu.roll(v, 1, 0)

    def coefficients():
        row_n = iota((NAT, WIDE), 0)
        beyond = ((row_n < 8) & (my_lat == 0)) | ((row_n >= 24) & (my_lat == n_lat - 1))
        wet = jnp.where(beyond, 0.0, nat[WET])
        k_east = nat[EAST] * wet * east(wet)
        k_north = nat[NORTH] * wet * north(wet)
        k_west = west(k_east)
        k_south = south(k_north)
        coef[1] = k_east
        coef[2] = k_west
        coef[3] = k_north
        coef[4] = k_south
        coef[0] = nat[SURF] * wet + k_east + k_west + k_north + k_south + (1.0 - wet)

    def operate(v):
        return coef[0] * v - (
            coef[1] * east(v) + coef[2] * west(v) + coef[3] * north(v) + coef[4] * south(v)
        )

    def image_row(src, e):
        at = pl.ds(e + 4, 1)
        v = src[e]
        return coef[0, at, :] * v - (
            coef[1, at, :] * east(v)
            + coef[2, at, :] * west(v)
            + coef[3, at, :] * src[e + 1]
            + coef[4, at, :] * src[e - 1]
        )

    def fold(v):
        total = v[:, 0:128]
        for i in range(1, NX // 128):
            total = total + v[:, 128 * i : 128 * i + 128]
        return total

    def contract(a, b):
        return lax.dot_general(
            a, b, (((1,), (1,)), ((), ())), precision=HIGHEST, preferred_element_type=f32
        )

    def first_pair(rows, carry):
        acc, w_s, b_s = carry
        both = []
        for y in rows:
            w = vec[y + DEPTH, :, 0:NX]
            image = image_row(vec, y + DEPTH)
            img1[y + DEPTH] = image
            b = image[:, 0:NX]
            s = st[pl.ds(y + 8, 1), 0:NX]
            w_s = w_s + fold(w * s)
            b_s = b_s + fold(b * s)
            both.append(jnp.concatenate([w, b], axis=0))
        both = jnp.concatenate(both, axis=1)
        return acc + contract(both, both), w_s, b_s

    def start_residual():
        st[...] = nat[RHS] - operate(nat[GUESS])

    wait_all(near_columns)
    unpack_plain(8, NY, 0, 0)
    coefficients()
    start_residual()
    wait_all(vec_columns)
    unpack_vectors(DEPTH, NY, 0, 0)
    carry = (jnp.zeros((2 * K, 2 * K), f32), zero16, zero16)
    carry = lax.fori_loop(
        0, NY // 2 - 1, lambda i, c: first_pair((2 * i + 1, 2 * i + 2), c), carry
    )
    start_all(deep)
    far[1]()
    wait_all(near_rows)
    landed(0, 3, 1, 1)
    wait_all(vec_rows)
    coefficients()
    start_residual()
    acc, w_s, b_s = first_pair((0, NY - 1), carry)

    def put(block, lane):
        wide = jnp.concatenate([block, jnp.zeros((K, 128 - block.shape[1]), f32)], axis=1)
        return pltpu.roll(wide, lane, 1) if lane else wide

    def column(payload, lane, total):
        return jnp.where(lane16 == lane, jnp.sum(total, axis=1, keepdims=True), payload)

    def pack(v, width):
        per, shift = 128 // width, width
        while shift < 128:
            v = v + pltpu.roll(v, shift, 1)
            shift *= 2
        v = jnp.where(lane16 // width == lax.rem(sub16, per), v, 0.0)
        return [
            jnp.sum(jnp.where(sub16 // per == i, v, 0.0), axis=0, keepdims=True)
            for i in range(K // per)
        ]

    def unpack(rows, width):
        per, shift = 128 // width, width
        v = jnp.broadcast_to(rows[0], (K, 128))
        for i in range(1, K // per):
            v = jnp.where(sub16 // per == i, rows[i], v)
        v = jnp.where(lane16 // width == lax.rem(sub16, per), v, 0.0)
        while shift < 128:
            v = v + pltpu.roll(v, shift, 1)
            shift *= 2
        return jnp.where(lane16 < width, v, 0.0)

    def send_phase(phase, value):
        send, buf, ssem, rsem, n, me, at, count = phase
        if count == 1:
            send[0:1, :] = value
            src, dst = send.at[pl.ds(0, 1)], buf.at[pl.ds(me, 1)]
        else:
            for i, row in enumerate(value):
                send[i : i + 1, :] = row
            src, dst = send.at[pl.ds(0, count)], buf.at[me, pl.ds(0, count)]
        for d in far_first(n):
            pltpu.make_async_remote_copy(
                src_ref=src,
                dst_ref=dst,
                send_sem=ssem.at[d],
                recv_sem=rsem.at[me],
                device_id=at(lax.rem(me + d, n)),
                device_id_type=MESH,
            ).start()
        if count == 1:
            buf[pl.ds(me, 1), :] = value
        else:
            for i, row in enumerate(value):
                buf[me, i : i + 1, :] = row

    def wait_phase(phase):
        send, buf, ssem, rsem, n, me, at, count = phase
        for d in range(1, n):
            peer = lax.rem(me + d, n)
            if count == 1:
                src, dst = send.at[pl.ds(0, 1)], buf.at[pl.ds(peer, 1)]
            else:
                src, dst = send.at[pl.ds(0, count)], buf.at[peer, pl.ds(0, count)]
            pltpu.make_async_remote_copy(
                src_ref=src,
                dst_ref=dst,
                send_sem=ssem.at[d],
                recv_sem=rsem.at[peer],
                device_id=at(peer),
                device_id_type=MESH,
            ).wait()
        if count == 1:
            return jnp.sum(buf[...], axis=0, keepdims=True)
        total = buf[0]
        for i in range(1, n):
            total = total + buf[i]
        return [total[i : i + 1, :] for i in range(count)]

    def three_phases(turn, count):
        return (
            (ar_send.at[turn, 0], ar_a.at[turn], ssem_a.at[turn], rsem_a.at[turn], na, my_a, at_a, count),
            (ar_send.at[turn, 1], ar_b.at[turn], ssem_b.at[turn], rsem_b.at[turn], nb, my_y, at_b, count),
            (ar_send.at[turn, 2], ar_c.at[turn], ssem_c.at[turn], rsem_c.at[turn], nc, my_z, at_c, count),
        )

    two_phases = (
        (ar_send.at[2, 0], ar_d, ssem_d, rsem_d, nd, my_d, at_d, 1),
        (ar_send.at[2, 1], ar_e, ssem_e, rsem_e, ne, my_e, at_e, 1),
    )

    def all_reduce(phases, value, between):
        for step, phase in enumerate(phases):
            send_phase(phase, value)
            if between[step] is not None:
                between[step]()
            value = wait_phase(phase)
        return value

    g3_phases = three_phases(1, 2)
    kept = {}

    def second_pair(rows, acc):
        left, right = [], []
        for y in rows:
            left.append(img1[y + DEPTH, :, 0:NX])
            right.append(image_row(img1, y + DEPTH)[:, 0:NX])
            img2[y] = right[-1]
        left, right = jnp.concatenate(left, axis=1), jnp.concatenate(right, axis=1)
        return acc + contract(left, right)

    def between_a():
        acc = jnp.zeros((K, K), f32)
        kept["g3"] = lax.fori_loop(
            0, NY // 2 - 1, lambda i, c: second_pair((2 * i + 1, 2 * i + 2), c), acc
        )

    def between_c():
        wait_all(deep)
        far[2]()
        landed(0, 3, 2, DEPTH)
        landed(3, 3, 1, DEPTH - 1)
        unpack_plain(24, 8, 0, 2)
        unpack_plain(0, 8, 8, 4)
        unpack_vectors(NY + DEPTH, DEPTH, 0, 2)
        unpack_vectors(0, DEPTH, NY - DEPTH, 4)
        coefficients()
        start_residual()

        def outer_row(i, carry):
            img1[i + 1] = image_row(vec, i + 1)
            img1[i + 19] = image_row(vec, i + 19)
            return carry

        lax.fori_loop(0, DEPTH, outer_row, 0)
        acc = second_pair((0, NY - 1), kept["g3"])
        send_phase(g3_phases[0], pack(put(acc, 0), K))

    grams = 0.5 * (put(acc[0:K, K:], 0) + put(acc[K:, 0:K], 0)) + put(acc[K:, K:], K)
    rows = pack(grams, 2 * K) + pack(column(column(zero16, 0, w_s), 1, b_s), 8)
    rows = all_reduce(three_phases(0, 5), rows, (between_a, None, between_c))
    grams = unpack(rows[0:4], 2 * K)
    starts = unpack(rows[4:5], 8)


    def at_zero(v, lane):
        v = jnp.where((lane16 >= lane) & (lane16 < lane + K), v, 0.0)
        return pltpu.roll(v, (128 - lane) % 128, 1) if lane else v

    aug = jnp.where(lane16 < K, grams, 0.0)
    aug = jnp.where(lane16 == sub16 + K, 1.0, aug)
    aug = jnp.where(lane16 == 2 * K, starts[:, 0:1], aug)
    pivots = jnp.broadcast_to(aug[:, 0:1], (K, 128))
    for i in range(K):
        scale = 1.0 / pivots[i : i + 1, :]
        pivot_row = aug[i : i + 1, :] * scale
        column_now = pivots
        if i + 1 < K:
            coming = jnp.broadcast_to(aug[:, i + 1 : i + 2], (K, 128))
            coming_row = coming[i : i + 1, :] * scale
            pivots = jnp.where(sub16 == i, coming_row, coming - column_now * coming_row)
        aug = jnp.where(sub16 == i, pivot_row, aug - column_now * pivot_row)
    coarse = aug[:, 2 * K : 2 * K + 1]
    inverse = at_zero(aug, K)
    g1, g2 = at_zero(grams, 0), at_zero(grams, K)

    def as_row(col):
        return jnp.sum(jnp.where(lane16 == sub16, col, 0.0), axis=0, keepdims=True)

    def row_times(mat, row):
        return jnp.sum(mat * row, axis=1, keepdims=True)

    def times_column(mat, col):
        return jnp.sum(mat * col, axis=0, keepdims=True)

    def apply(mat, col):
        return row_times(mat, as_row(col))

    def dot(a, b):
        return jnp.sum(a * b, axis=0, keepdims=True)

    w_row, b_row = as_row(starts[:, 0:1]), as_row(starts[:, 1:2])
    coarse = coarse + row_times(inverse, w_row - times_column(g1, coarse))
    mu0 = row_times(inverse, b_row - times_column(g2, coarse))


    def residual_row(e, carry):
        at = pl.ds(e + 4, 1)
        r = st[at, :] - jnp.sum(coarse * img1[e], axis=0, keepdims=True)
        res[4, at, :] = r
        res[0, at, :] = r - jnp.sum(mu0 * vec[e], axis=0, keepdims=True)
        return carry

    lax.fori_loop(1, ROWS - 1, residual_row, 0, unroll=11)
    send_phase(g3_phases[1], wait_phase(g3_phases[0]))
    for i, base in enumerate((4, 1, 2)):
        res[i + 1] = operate(res[i]) - SHIFT * res[base]

    def moment_row(y, carry):
        b1, b2 = img1[y + DEPTH, :, 0:NX], img2[y]
        v1, a1 = (res[i, pl.ds(y + 8, 1), 0:NX] for i in (1, 2))
        terms = (b1 * v1, b1 * a1, b2 * a1)
        return tuple(total + fold(term) for total, term in zip(carry, terms))

    defl = lax.fori_loop(0, NY, moment_row, (zero16,) * 3, unroll=4)
    payload = zero16
    for i, total in enumerate(defl):
        payload = column(payload, i, total)
    inner = [res[i, 8:24, 0:NX] for i in (4, 1, 2, 3)]
    for i, (a, b) in enumerate(((0, 0), (0, 1), (1, 1), (1, 2), (2, 2), (2, 3))):
        total = jnp.sum(fold(inner[a] * inner[b]), axis=0, keepdims=True)
        total = jnp.sum(total, axis=1, keepdims=True)
        payload = jnp.where((lane16 == 3) & (sub16 == i), total, payload)

    def before_scalars():
        def row(y, carry):
            at = pl.ds(y + 8, 1)
            along = jnp.sum(coarse * vec[y + DEPTH, :, 0:NX], axis=0, keepdims=True)
            st[at, 0:NX] = nat[GUESS, at, 0:NX] + along
            return carry

        lax.fori_loop(0, NY, row, 0, unroll=4)
        send_phase(g3_phases[2], wait_phase(g3_phases[1]))

    def last_gram():
        kept["g3"] = unpack(wait_phase(g3_phases[2]), K)

    row = all_reduce(two_phases, pack(payload, 8)[0], (before_scalars, last_gram))
    sums = unpack([row], 8)

    g3 = kept["g3"]
    e = [sums[:, i : i + 1] for i in range(3)]
    t = [sums[i : i + 1, 3:4] for i in range(6)]
    mu1 = apply(inverse, e[0])
    g2_1, g3_1 = apply(g2, mu1), apply(g3, mu1)
    defl2 = e[1] - g2_1
    mu2 = apply(inverse, defl2)
    m = [
        t[0],
        t[1],
        t[2],
        t[3] - dot(mu1, e[0]),
        t[4] - 2.0 * dot(mu1, e[1]) + dot(mu1, g2_1),
        t[5]
        - 2.0 * dot(mu1, e[2] - SHIFT * e[1])
        + dot(mu1, g3_1 - SHIFT * g2_1)
        - dot(mu2, defl2),
    ]

    def form(poly, shift):
        total = 0.0
        for i, a in enumerate(poly):
            for j, b in enumerate(poly):
                total = total + a * b * m[i + j + shift]
        return total

    one = jnp.ones((1, 1), f32)
    zero = jnp.zeros((1, 1), f32)
    r_poly = [one]
    y_poly = [zero]
    zeta = [zero, zero, zero]
    curv = prev_norm = one
    for turn in range(3):
        norm = form(r_poly, 0)
        r_image = form(r_poly, 1) + SHIFT * norm
        if turn == 0:
            y_poly = list(r_poly)
            curv = r_image
        else:
            ratio = norm / prev_norm
            y_poly = [a + ratio * b for a, b in zip(r_poly, y_poly + [zero])]
            curv = r_image - ratio * ratio * curv
        step_len = norm / curv
        for i, a in enumerate(y_poly):
            zeta[i] = zeta[i] + step_len * a
        y_image = [a + SHIFT * b for a, b in zip([zero] + y_poly, y_poly + [zero])]
        r_poly = [a - step_len * b for a, b in zip(r_poly + [zero], y_image)]
        prev_norm = norm

    along_w = zeta[1] * mu1 + zeta[2] * mu2
    along_b = zeta[2] * mu1
    res_b = (r_poly[2] - SHIFT * r_poly[3]) * mu1 + r_poly[3] * mu2
    res_bb = r_poly[3] * mu1

    def final_row(y, carry):
        w, b1, b2 = vec[y + DEPTH, :, 0:NX], img1[y + DEPTH, :, 0:NX], img2[y]
        at = pl.ds(y, 1)
        comb[0, at, :] = jnp.sum(along_w * w + along_b * b1, axis=0, keepdims=True)
        comb[1, at, :] = jnp.sum(res_b * b1 + res_bb * b2, axis=0, keepdims=True)
        return carry

    lax.fori_loop(0, NY, final_row, 0, unroll=8)
    p0, v1, a1, a2, r0 = (res[i, 8:24, 0:NX] for i in range(5))
    out[0] = (
        st[8:24, 0:NX] + (zeta[0] * p0 + zeta[1] * v1 + zeta[2] * a1) - comb[0]
    )
    out[1] = (
        r_poly[0] * r0 + (r_poly[1] * v1 + r_poly[2] * a1 + r_poly[3] * a2) - comb[1]
    )


def shards(right_side, first_guess, cell_mask, cond_east, cond_north, surface, recycled):
    sizes = tuple(lax.axis_size(axis) for axis in AXES)
    ny_dev, nzh, nx_dev, nzl, ncore = sizes
    na, nb, nc = nx_dev * ncore, ny_dev, nzh * nzl
    nd, ne = nx_dev * ny_dev, nzh * nzl * ncore
    vmem = pltpu.VMEM
    dma = pltpu.SemaphoreType.DMA
    both = pl.pallas_call(
        functools.partial(kernel, sizes),
        out_shape=jax.ShapeDtypeStruct((2, NY, NX), f32),
        in_specs=[pl.BlockSpec(memory_space=pl.ANY)] * 7,
        out_specs=pl.BlockSpec(memory_space=pltpu.VMEM),
        scratch_shapes=[
            vmem((ROWS, K, WIDE), f32),
            vmem((ROWS, K, WIDE), f32),
            vmem((NY, K, NX), f32),
            vmem((6, NAT, WIDE), f32),
            vmem((6, NAT, NX), f32),
            vmem((5, NAT, WIDE), f32),
            vmem((NAT, WIDE), f32),
            vmem((5, NAT, WIDE), f32),
            vmem((NY, NX), jnp.int32),
            vmem((2, K, 128), f32),
            vmem((6, K, 128), f32),
            vmem((2, NY, 128), f32),
            vmem((6, NY, 128), f32),
            vmem((3, 3, 8, 128), f32),
            vmem((2, na, 8, 128), f32),
            vmem((2, nb, 8, 128), f32),
            vmem((2, nc, 8, 128), f32),
            vmem((nd, 128), f32),
            vmem((ne, 128), f32),
            vmem((2, NY, NX), f32),
            vmem((2, 2, K, NX), f32),
            dma((22,)),
            dma((28,)),
            dma((28,)),
            dma((2, na)),
            dma((2, nb)),
            dma((2, nc)),
            dma((nd,)),
            dma((ne,)),
            dma((2, na)),
            dma((2, nb)),
            dma((2, nc)),
            dma((nd,)),
            dma((ne,)),
        ],
        compiler_params=pltpu.CompilerParams(collective_id=0, has_side_effects=True),
    )(right_side, first_guess, cell_mask, cond_east, cond_north, surface, recycled)
    return both[0], both[1]


def finer_mesh(mesh):
    return Mesh(mesh.devices.reshape(8, 3, 4, 4, 2), AXES)


def solution(mesh):
    in_specs = (P(LAT, LON),) * 6 + (P(None, LAT, LON),)
    out_specs = (P(LAT, LON), P(LAT, LON))
    return jax.shard_map(
        shards, mesh=finer_mesh(mesh), in_specs=in_specs, out_specs=out_specs, check_vma=False
    )
```

```python
import functools

import jax
import jax.numpy as jnp
from jax import lax
from jax.experimental import pallas as pl
from jax.experimental.pallas import tpu as pltpu
from jax.sharding import Mesh
from jax.sharding import PartitionSpec as P

LAT = ("lat_0", "lat_1", "lat_2")
LON = ("lon_0", "lon_1")
AXES = LAT + LON
MESH = pl.DeviceIdType.MESH
HIGHEST = lax.Precision.HIGHEST

K = 16
DEPTH = 4
SHIFT = 4.0
NY = 16
NX = 640
WIDE = NX + 128
ROWS = NY + 2 * DEPTH
NAT = NY + 16
WET, NORTH, GUESS, EAST, SURF, RHS = range(6)

f32 = jnp.float32


def far_first(n):
    return sorted(range(1, n), key=lambda d: -min(d, n - d))


def iota(shape, axis):
    return lax.broadcasted_iota(jnp.int32, shape, axis)


def kernel(
    sizes,
    rhs_hbm,
    guess_hbm,
    mask_hbm,
    east_hbm,
    north_hbm,
    surf_hbm,
    rec_hbm,
    out,
    vec,
    img1,
    img2,
    nat,
    land,
    coef,
    st,
    res,
    mask_v,
    pack_vec,
    got_vec,
    pack_nat,
    got_nat,
    ar_send,
    ar_a,
    ar_b,
    ar_c,
    ar_d,
    ar_e,
    comb,
    relay,
    in_sem,
    halo_send,
    halo_recv,
    ssem_a,
    ssem_b,
    ssem_c,
    ssem_d,
    ssem_e,
    rsem_a,
    rsem_b,
    rsem_c,
    rsem_d,
    rsem_e,
):
    ny_dev, nzh, nx_dev, nzl, ncore = sizes
    my_y = lax.axis_index("lat_0")
    my_zh = lax.axis_index("lat_1")
    my_x = lax.axis_index("lat_2")
    my_zl = lax.axis_index("lon_0")
    my_c = lax.axis_index("lon_1")
    n_lat = ny_dev * nzh * nx_dev
    n_lon = nzl * ncore
    my_lat = (my_y * nzh + my_zh) * nx_dev + my_x
    my_lon = my_zl * ncore + my_c
    na, nb, nc = nx_dev * ncore, ny_dev, nzh * nzl
    nd, ne = nx_dev * ny_dev, nzh * nzl * ncore
    my_a = my_x * ncore + my_c
    my_z = my_zh * nzl + my_zl
    my_d = my_y * nx_dev + my_x
    my_e = my_z * ncore + my_c

    def at_cell(up, right):
        lat = lax.rem(my_lat + (up + n_lat), n_lat)
        lon = lax.rem(my_lon + (right + n_lon), n_lon)
        rest = lat // nx_dev
        return (
            rest // nzh,
            lax.rem(rest, nzh),
            lax.rem(lat, nx_dev),
            lon // ncore,
            lax.rem(lon, ncore),
        )

    def at_a(index):
        return (my_y, my_zh, index // ncore, my_zl, lax.rem(index, ncore))

    def at_b(index):
        return (index, my_zh, my_x, my_zl, my_c)

    def at_c(index):
        return (my_y, index // nzl, my_x, lax.rem(index, nzl), my_c)

    def at_d(index):
        return (index // nx_dev, my_zh, lax.rem(index, nx_dev), my_zl, my_c)

    def at_e(index):
        z = index // ncore
        return (my_y, z // nzl, my_x, lax.rem(z, nzl), lax.rem(index, ncore))

    north_of, south_of = at_cell(1, 0), at_cell(-1, 0)
    east_of, west_of = at_cell(0, 1), at_cell(0, -1)
    corners = (at_cell(1, 1), at_cell(1, -1), at_cell(-1, 1), at_cell(-1, -1))

    plain = (
        (east_hbm, EAST),
        (north_hbm, NORTH),
        (surf_hbm, SURF),
        (rhs_hbm, RHS),
        (guess_hbm, GUESS),
    )
    loads = [pltpu.make_async_copy(mask_hbm, mask_v, in_sem.at[0])]
    for i, (src, field) in enumerate(plain):
        loads.append(
            pltpu.make_async_copy(
                src, nat.at[field, pl.ds(8, NY), pl.ds(0, NX)], in_sem.at[1 + i]
            )
        )
    for k in range(K):
        loads.append(
            pltpu.make_async_copy(
                rec_hbm.at[k], vec.at[pl.ds(DEPTH, NY), k, pl.ds(0, NX)], in_sem.at[6 + k]
            )
        )
    for load in loads:
        load.start()

    barrier = pltpu.get_barrier_semaphore()
    peers = [north_of, south_of, *corners, east_of, west_of]
    groups = [
        [at(lax.rem(me + d, n)) for d in far_first(n)]
        for n, me, at in ((ne, my_e, at_e), (nd, my_d, at_d), (na, my_a, at_a))
    ]
    for i in range(max(len(group) for group in groups)):
        peers += [group[i] for group in groups if i < len(group)]
    for peer in peers:
        pl.semaphore_signal(barrier, inc=1, device_id=peer, device_id_type=MESH)

    nat[:, 0:8, :] = jnp.zeros((6, 8, WIDE), f32)
    nat[:, 24:32, :] = jnp.zeros((6, 8, WIDE), f32)
    nat[:, 8:24, NX:] = jnp.zeros((6, NY, 128), f32)
    res[:, 0:8, :] = jnp.zeros((5, 8, WIDE), f32)
    res[:, 24:32, :] = jnp.zeros((5, 8, WIDE), f32)

    for load in loads:
        load.wait()
    nat[WET, 8:24, 0:NX] = mask_v[...].astype(f32)

    def remote(src, dst, at, slot):
        return pltpu.make_async_remote_copy(
            src_ref=src,
            dst_ref=dst,
            send_sem=halo_send.at[slot],
            recv_sem=halo_recv.at[slot],
            device_id=at,
            device_id_type=MESH,
        )

    def start_all(copies):
        for copy in copies:
            copy.start()

    def wait_all(copies):
        for copy in copies:
            copy.wait()

    lanes = pl.ds(0, NX)
    lane16 = iota((K, 128), 1)
    sub16 = iota((K, 128), 0)
    zero16 = jnp.zeros((K, 128), f32)

    def pack_vectors():
        def row(y, carry):
            to_west, to_east = carry
            e, lane = y + DEPTH, DEPTH * y
            first = pltpu.roll(vec[e, :, 0:128], lane, 1)
            last = pltpu.roll(vec[e, :, NX - 128 : NX], lane + DEPTH, 1)
            mine = (lane16 >= lane) & (lane16 < lane + DEPTH)
            return jnp.where(mine, first, to_west), jnp.where(mine, last, to_east)

        to_west, to_east = lax.fori_loop(0, NY, row, (zero16, zero16), unroll=4)
        pack_vec[0] = to_west
        pack_vec[1] = to_east

    def edge_columns(from_east, from_west, lane):
        return jnp.where(
            lane < DEPTH, from_east, jnp.where(lane >= 128 - DEPTH, from_west, 0.0)
        )

    def unpack_vectors(first, count, y0, place):
        def row(i, carry):
            lane = DEPTH * (y0 + i)
            from_east = pltpu.roll(got_vec[place], lax.rem(128 - lane, 128), 1)
            from_west = pltpu.roll(got_vec[place + 1], 128 - DEPTH - lane, 1)
            vec[first + i, :, NX:] = edge_columns(from_east, from_west, lane16)
            return carry

        lax.fori_loop(0, count, row, 0, unroll=4)

    def pack_plain():
        to_west, to_east = zero16, zero16
        for i in range(6):
            lane = DEPTH * i
            first, last = nat[i, 8:24, 0:128], nat[i, 8:24, NX - 128 : NX]
            if i:
                first = pltpu.roll(first, lane, 1)
            last = pltpu.roll(last, lane + DEPTH, 1)
            mine = (lane16 >= lane) & (lane16 < lane + DEPTH)
            to_west = jnp.where(mine, first, to_west)
            to_east = jnp.where(mine, last, to_east)
        pack_nat[0] = to_west
        pack_nat[1] = to_east

    def unpack_plain(first, count, y0, place):
        lane = lane16[0:count]
        for i in range(6):
            from_east = got_nat[place, y0 : y0 + count, :]
            from_west = got_nat[place + 1, y0 : y0 + count, :]
            if i:
                from_east = pltpu.roll(from_east, 128 - DEPTH * i, 1)
            from_west = pltpu.roll(from_west, 128 - DEPTH - DEPTH * i, 1)
            nat[i, first : first + count, NX:] = edge_columns(from_east, from_west, lane)

    def landed(first, count, near, far):
        for i in range(first, first + count):
            nat[i, 8 - far : 9 - near, 0:NX] = land[i, 8 - far : 9 - near, :]
            nat[i, 23 + near : 24 + far, 0:NX] = land[i, 23 + near : 24 + far, :]

    def vector_rows(near, far, slot):
        n = far - near + 1
        return [
            remote(
                vec.at[pl.ds(20 - far, n), :, lanes],
                vec.at[pl.ds(4 - far, n), :, lanes],
                north_of,
                slot,
            ),
            remote(
                vec.at[pl.ds(3 + near, n), :, lanes],
                vec.at[pl.ds(19 + near, n), :, lanes],
                south_of,
                slot + 1,
            ),
        ]

    def far_rows():
        ahead, behind = lax.rem(my_zh + 1, nzh), lax.rem(my_zh + (nzh - 1), nzh)
        next_y = jnp.where(my_zh == nzh - 1, lax.rem(my_y + 1, ny_dev), my_y)
        last_y = jnp.where(my_zh == 0, lax.rem(my_y + (ny_dev - 1), ny_dev), my_y)
        ways = (
            (
                my_x == nx_dev - 1,
                my_x == 0,
                vec.at[pl.ds(16, 2), :, lanes],
                vec.at[pl.ds(0, 2), :, lanes],
                north_of,
                (next_y, my_zh, 0, my_zl, my_c),
                (my_y, ahead, my_x, my_zl, my_c),
            ),
            (
                my_x == 0,
                my_x == nx_dev - 1,
                vec.at[pl.ds(6, 2), :, lanes],
                vec.at[pl.ds(22, 2), :, lanes],
                south_of,
                (last_y, my_zh, nx_dev - 1, my_zl, my_c),
                (my_y, behind, my_x, my_zl, my_c),
            ),
        )

        def copy(src, dst, at, send_slot, recv_slot):
            return pltpu.make_async_remote_copy(
                src_ref=src,
                dst_ref=dst,
                send_sem=halo_send.at[send_slot],
                recv_sem=halo_recv.at[recv_slot],
                device_id=at,
                device_id_type=MESH,
            )

        hops = []
        for i, (crosses, forwards, src, dst, straight, first_hop, last_hop) in enumerate(ways):
            held = relay.at[i]
            hops.append(
                (
                    crosses,
                    forwards,
                    copy(src, dst, straight, 22 + i, 22 + i),
                    copy(src, held, first_hop, 24 + i, 24 + i),
                    copy(held, dst, last_hop, 26 + i, 22 + i),
                )
            )

        def begin():
            for crosses, _, straight, first, _ in hops:
                pl.when(jnp.logical_not(crosses))(straight.start)
                pl.when(crosses)(first.start)

        def forward():
            for _, forwards, _, first, last in hops:

                @pl.when(forwards)
                def _():
                    first.wait_recv()
                    last.start()

        def finish():
            for crosses, forwards, straight, first, last in hops:
                pl.when(jnp.logical_not(crosses))(straight.wait_send)
                pl.when(crosses)(first.wait_send)
                pl.when(forwards)(last.wait_send)
                straight.wait_recv()

        return begin, forward, finish

    def columns(pack, got, slot):
        return [
            remote(pack.at[0], got.at[0], west_of, slot),
            remote(pack.at[1], got.at[1], east_of, slot + 1),
        ]

    def corner_columns(pack, got, slot, south_rows, north_rows):
        north_east, north_west, south_east, south_west = corners
        return [
            remote(pack.at[0, south_rows], got.at[2, south_rows], south_west, slot),
            remote(pack.at[1, south_rows], got.at[3, south_rows], south_east, slot + 1),
            remote(pack.at[0, north_rows], got.at[4, north_rows], north_west, slot + 2),
            remote(pack.at[1, north_rows], got.at[5, north_rows], north_east, slot + 3),
        ]

    def plain_rows(first, count, near, far, slot):
        fields, n = pl.ds(first, count), far - near + 1
        return [
            remote(
                nat.at[fields, pl.ds(24 - far, n), lanes],
                land.at[fields, pl.ds(8 - far, n)],
                north_of,
                slot,
            ),
            remote(
                nat.at[fields, pl.ds(7 + near, n), lanes],
                land.at[fields, pl.ds(23 + near, n)],
                south_of,
                slot + 1,
            ),
        ]

    pack_vectors()
    pack_plain()
    pl.semaphore_wait(barrier, len(peers))

    near_rows = plain_rows(0, 3, 1, 1, 0)
    vec_rows = vector_rows(1, 1, 2)
    vec_columns = columns(pack_vec, got_vec, 4)
    near_columns = columns(pack_nat, got_nat, 6)
    all_rows = pl.ds(0, NY)
    far = far_rows()
    deep = (
        corner_columns(pack_nat, got_nat, 18, pl.ds(0, 8), pl.ds(8, 8))
        + plain_rows(0, 3, 2, DEPTH, 8)
        + plain_rows(3, 3, 1, DEPTH - 1, 10)
        + corner_columns(pack_vec, got_vec, 14, all_rows, all_rows)
        + vector_rows(2, 2, 12)
    )
    start_all(near_columns)
    start_all(vec_columns)
    start_all(near_rows)
    start_all(vec_rows)
    far[0]()

    def east(v):
        return pltpu.roll(v, WIDE - 1, 1)

    def west(v):
        return pltpu.roll(v, 1, 1)

    def north(v):
        return pltpu.roll(v, NAT - 1, 0)

    def south(v):
        return pltpu.roll(v, 1, 0)

    def coefficients():
        row_n = iota((NAT, WIDE), 0)
        beyond = ((row_n < 8) & (my_lat == 0)) | ((row_n >= 24) & (my_lat == n_lat - 1))
        wet = jnp.where(beyond, 0.0, nat[WET])
        k_east = nat[EAST] * wet * east(wet)
        k_north = nat[NORTH] * wet * north(wet)
        k_west = west(k_east)
        k_south = south(k_north)
        coef[1] = k_east
        coef[2] = k_west
        coef[3] = k_north
        coef[4] = k_south
        coef[0] = nat[SURF] * wet + k_east + k_west + k_north + k_south + (1.0 - wet)

    def operate(v):
        return coef[0] * v - (
            coef[1] * east(v) + coef[2] * west(v) + coef[3] * north(v) + coef[4] * south(v)
        )

    def image_row(src, e):
        at = pl.ds(e + 4, 1)
        v = src[e]
        return coef[0, at, :] * v - (
            coef[1, at, :] * east(v)
            + coef[2, at, :] * west(v)
            + coef[3, at, :] * src[e + 1]
            + coef[4, at, :] * src[e - 1]
        )

    def fold(v):
        total = v[:, 0:128]
        for i in range(1, NX // 128):
            total = total + v[:, 128 * i : 128 * i + 128]
        return total

    def contract(a, b):
        return lax.dot_general(
            a, b, (((1,), (1,)), ((), ())), precision=HIGHEST, preferred_element_type=f32
        )

    def first_pair(rows, carry):
        acc, w_s, b_s = carry
        both = []
        for y in rows:
            w = vec[y + DEPTH, :, 0:NX]
            image = image_row(vec, y + DEPTH)
            img1[y + DEPTH] = image
            b = image[:, 0:NX]
            s = st[pl.ds(y + 8, 1), 0:NX]
            w_s = w_s + fold(w * s)
            b_s = b_s + fold(b * s)
            both.append(jnp.concatenate([w, b], axis=0))
        both = jnp.concatenate(both, axis=1)
        return acc + contract(both, both), w_s, b_s

    def start_residual():
        st[...] = nat[RHS] - operate(nat[GUESS])

    wait_all(near_columns)
    unpack_plain(8, NY, 0, 0)
    coefficients()
    start_residual()
    wait_all(vec_columns)
    unpack_vectors(DEPTH, NY, 0, 0)
    carry = (jnp.zeros((2 * K, 2 * K), f32), zero16, zero16)
    carry = lax.fori_loop(
        0, NY // 2 - 1, lambda i, c: first_pair((2 * i + 1, 2 * i + 2), c), carry
    )
    start_all(deep)
    far[1]()
    wait_all(near_rows)
    landed(0, 3, 1, 1)
    coefficients()
    start_residual()
    wait_all(vec_rows)
    acc, w_s, b_s = first_pair((0, NY - 1), carry)

    def put(block, lane):
        wide = jnp.concatenate([block, jnp.zeros((K, 128 - block.shape[1]), f32)], axis=1)
        return pltpu.roll(wide, lane, 1) if lane else wide

    def column(payload, lane, total):
        return jnp.where(lane16 == lane, jnp.sum(total, axis=1, keepdims=True), payload)

    def pack(v, width):
        per, shift = 128 // width, width
        while shift < 128:
            v = v + pltpu.roll(v, shift, 1)
            shift *= 2
        v = jnp.where(lane16 // width == lax.rem(sub16, per), v, 0.0)
        return [
            jnp.sum(jnp.where(sub16 // per == i, v, 0.0), axis=0, keepdims=True)
            for i in range(K // per)
        ]

    def unpack(rows, width):
        per, shift = 128 // width, width
        v = jnp.broadcast_to(rows[0], (K, 128))
        for i in range(1, K // per):
            v = jnp.where(sub16 // per == i, rows[i], v)
        v = jnp.where(lane16 // width == lax.rem(sub16, per), v, 0.0)
        while shift < 128:
            v = v + pltpu.roll(v, shift, 1)
            shift *= 2
        return jnp.where(lane16 < width, v, 0.0)

    def send_phase(phase, value):
        send, buf, ssem, rsem, n, me, at, count = phase
        if count == 1:
            send[0:1, :] = value
            src, dst = send.at[pl.ds(0, 1)], buf.at[pl.ds(me, 1)]
        else:
            for i, row in enumerate(value):
                send[i : i + 1, :] = row
            src, dst = send.at[pl.ds(0, count)], buf.at[me, pl.ds(0, count)]
        for d in far_first(n):
            pltpu.make_async_remote_copy(
                src_ref=src,
                dst_ref=dst,
                send_sem=ssem.at[d],
                recv_sem=rsem.at[me],
                device_id=at(lax.rem(me + d, n)),
                device_id_type=MESH,
            ).start()
        if count == 1:
            buf[pl.ds(me, 1), :] = value
        else:
            for i, row in enumerate(value):
                buf[me, i : i + 1, :] = row

    def wait_phase(phase):
        send, buf, ssem, rsem, n, me, at, count = phase
        for d in reversed(far_first(n)):
            peer = lax.rem(me + d, n)
            if count == 1:
                src, dst = send.at[pl.ds(0, 1)], buf.at[pl.ds(peer, 1)]
            else:
                src, dst = send.at[pl.ds(0, count)], buf.at[peer, pl.ds(0, count)]
            pltpu.make_async_remote_copy(
                src_ref=src,
                dst_ref=dst,
                send_sem=ssem.at[d],
                recv_sem=rsem.at[peer],
                device_id=at(peer),
                device_id_type=MESH,
            ).wait_recv()
        if count == 1:
            return jnp.sum(buf[...], axis=0, keepdims=True)
        total = buf[0]
        for i in range(1, n):
            total = total + buf[i]
        return [total[i : i + 1, :] for i in range(count)]

    def finish_sends(phase):
        send, buf, ssem, rsem, n, me, at, count = phase
        src = send.at[pl.ds(0, count)]
        for d in range(1, n):
            pltpu.make_async_remote_copy(
                src_ref=src,
                dst_ref=src,
                send_sem=ssem.at[d],
                recv_sem=rsem.at[me],
                device_id=at(lax.rem(me + d, n)),
                device_id_type=MESH,
            ).wait_send()

    def three_phases(turn, count):
        return (
            (ar_send.at[turn, 0], ar_a.at[turn], ssem_a.at[turn], rsem_a.at[turn], na, my_a, at_a, count),
            (ar_send.at[turn, 1], ar_b.at[turn], ssem_b.at[turn], rsem_b.at[turn], nb, my_y, at_b, count),
            (ar_send.at[turn, 2], ar_c.at[turn], ssem_c.at[turn], rsem_c.at[turn], nc, my_z, at_c, count),
        )

    two_phases = (
        (ar_send.at[2, 0], ar_d, ssem_d, rsem_d, nd, my_d, at_d, 1),
        (ar_send.at[2, 1], ar_e, ssem_e, rsem_e, ne, my_e, at_e, 1),
    )

    def all_reduce(phases, value, between):
        for step, phase in enumerate(phases):
            send_phase(phase, value)
            if between[step] is not None:
                between[step]()
            value = wait_phase(phase)
        return value

    first_phases = three_phases(0, 5)
    g3_phases = three_phases(1, 2)
    kept = {}

    def second_pair(rows, acc):
        left, right = [], []
        for y in rows:
            left.append(img1[y + DEPTH, :, 0:NX])
            right.append(image_row(img1, y + DEPTH)[:, 0:NX])
            img2[y] = right[-1]
        left, right = jnp.concatenate(left, axis=1), jnp.concatenate(right, axis=1)
        return acc + contract(left, right)

    def between_a():
        acc = jnp.zeros((K, K), f32)
        kept["g3"] = lax.fori_loop(
            0, NY // 2 - 1, lambda i, c: second_pair((2 * i + 1, 2 * i + 2), c), acc
        )

    def between_c():
        wait_all(deep)
        far[2]()
        landed(0, 3, 2, DEPTH)
        landed(3, 3, 1, DEPTH - 1)
        unpack_plain(24, 8, 0, 2)
        unpack_plain(0, 8, 8, 4)
        unpack_vectors(NY + DEPTH, DEPTH, 0, 2)
        unpack_vectors(0, DEPTH, NY - DEPTH, 4)
        coefficients()
        start_residual()

        def outer_row(i, carry):
            img1[i + 1] = image_row(vec, i + 1)
            img1[i + 19] = image_row(vec, i + 19)
            return carry

        lax.fori_loop(0, DEPTH, outer_row, 0)
        acc = second_pair((0, NY - 1), kept["g3"])
        send_phase(g3_phases[0], pack(put(acc, 0), K))
        finish_sends(first_phases[0])
        finish_sends(first_phases[1])

    grams = 0.5 * (put(acc[0:K, K:], 0) + put(acc[K:, 0:K], 0)) + put(acc[K:, K:], K)
    rows = pack(grams, 2 * K) + pack(column(column(zero16, 0, w_s), 1, b_s), 8)
    rows = all_reduce(first_phases, rows, (between_a, None, between_c))
    grams = unpack(rows[0:4], 2 * K)
    starts = unpack(rows[4:5], 8)


    def at_zero(v, lane):
        v = jnp.where((lane16 >= lane) & (lane16 < lane + K), v, 0.0)
        return pltpu.roll(v, (128 - lane) % 128, 1) if lane else v

    aug = jnp.where(lane16 < K, grams, 0.0)
    aug = jnp.where(lane16 == sub16 + K, 1.0, aug)
    aug = jnp.where(lane16 == 2 * K, starts[:, 0:1], aug)
    pivots = jnp.broadcast_to(aug[:, 0:1], (K, 128))
    for i in range(K):
        scale = 1.0 / pivots[i : i + 1, :]
        pivot_row = aug[i : i + 1, :] * scale
        column_now = pivots
        if i + 1 < K:
            coming = jnp.broadcast_to(aug[:, i + 1 : i + 2], (K, 128))
            coming_row = coming[i : i + 1, :] * scale
            pivots = jnp.where(sub16 == i, coming_row, coming - column_now * coming_row)
        aug = jnp.where(sub16 == i, pivot_row, aug - column_now * pivot_row)
    coarse = aug[:, 2 * K : 2 * K + 1]
    inverse = at_zero(aug, K)
    g1, g2 = at_zero(grams, 0), at_zero(grams, K)

    def as_row(col):
        return jnp.sum(jnp.where(lane16 == sub16, col, 0.0), axis=0, keepdims=True)

    def row_times(mat, row):
        return jnp.sum(mat * row, axis=1, keepdims=True)

    def times_column(mat, col):
        return jnp.sum(mat * col, axis=0, keepdims=True)

    def apply(mat, col):
        return row_times(mat, as_row(col))

    def dot(a, b):
        return jnp.sum(a * b, axis=0, keepdims=True)

    w_row, b_row = as_row(starts[:, 0:1]), as_row(starts[:, 1:2])
    coarse = coarse + row_times(inverse, w_row - times_column(g1, coarse))
    mu0 = row_times(inverse, b_row - times_column(g2, coarse))


    def residual_row(e, carry):
        at = pl.ds(e + 4, 1)
        r = st[at, :] - jnp.sum(coarse * img1[e], axis=0, keepdims=True)
        res[4, at, :] = r
        res[0, at, :] = r - jnp.sum(mu0 * vec[e], axis=0, keepdims=True)
        return carry

    lax.fori_loop(1, ROWS - 1, residual_row, 0, unroll=11)
    send_phase(g3_phases[1], wait_phase(g3_phases[0]))
    for i, base in enumerate((4, 1, 2)):
        res[i + 1] = operate(res[i]) - SHIFT * res[base]

    def moment_row(y, carry):
        b1, b2 = img1[y + DEPTH, :, 0:NX], img2[y]
        v1, a1 = (res[i, pl.ds(y + 8, 1), 0:NX] for i in (1, 2))
        terms = (b1 * v1, b1 * a1, b2 * a1)
        return tuple(total + fold(term) for total, term in zip(carry, terms))

    defl = lax.fori_loop(0, NY, moment_row, (zero16,) * 3, unroll=4)
    payload = zero16
    for i, total in enumerate(defl):
        payload = column(payload, i, total)
    inner = [res[i, 8:24, 0:NX] for i in (4, 1, 2, 3)]
    for i, (a, b) in enumerate(((0, 0), (0, 1), (1, 1), (1, 2), (2, 2), (2, 3))):
        total = jnp.sum(fold(inner[a] * inner[b]), axis=0, keepdims=True)
        total = jnp.sum(total, axis=1, keepdims=True)
        payload = jnp.where((lane16 == 3) & (sub16 == i), total, payload)

    def before_scalars():
        def row(y, carry):
            at = pl.ds(y + 8, 1)
            along = jnp.sum(coarse * vec[y + DEPTH, :, 0:NX], axis=0, keepdims=True)
            st[at, 0:NX] = nat[GUESS, at, 0:NX] + along
            return carry

        lax.fori_loop(0, NY, row, 0, unroll=4)
        send_phase(g3_phases[2], wait_phase(g3_phases[1]))
        for phase in (first_phases[2], g3_phases[0], g3_phases[1]):
            finish_sends(phase)

    def last_gram():
        kept["g3"] = unpack(wait_phase(g3_phases[2]), K)
        for phase in (g3_phases[2], *two_phases):
            finish_sends(phase)

    row = all_reduce(two_phases, pack(payload, 8)[0], (before_scalars, last_gram))
    sums = unpack([row], 8)

    g3 = kept["g3"]
    e = [sums[:, i : i + 1] for i in range(3)]
    t = [sums[i : i + 1, 3:4] for i in range(6)]
    mu1 = apply(inverse, e[0])
    g2_1, g3_1 = apply(g2, mu1), apply(g3, mu1)
    defl2 = e[1] - g2_1
    mu2 = apply(inverse, defl2)
    m = [
        t[0],
        t[1],
        t[2],
        t[3] - dot(mu1, e[0]),
        t[4] - 2.0 * dot(mu1, e[1]) + dot(mu1, g2_1),
        t[5]
        - 2.0 * dot(mu1, e[2] - SHIFT * e[1])
        + dot(mu1, g3_1 - SHIFT * g2_1)
        - dot(mu2, defl2),
    ]

    def form(poly, shift):
        total = 0.0
        for i, a in enumerate(poly):
            for j, b in enumerate(poly):
                total = total + a * b * m[i + j + shift]
        return total

    one = jnp.ones((1, 1), f32)
    zero = jnp.zeros((1, 1), f32)
    r_poly = [one]
    y_poly = [zero]
    zeta = [zero, zero, zero]
    curv = prev_norm = one
    for turn in range(3):
        norm = form(r_poly, 0)
        r_image = form(r_poly, 1) + SHIFT * norm
        if turn == 0:
            y_poly = list(r_poly)
            curv = r_image
        else:
            ratio = norm / prev_norm
            y_poly = [a + ratio * b for a, b in zip(r_poly, y_poly + [zero])]
            curv = r_image - ratio * ratio * curv
        step_len = norm / curv
        for i, a in enumerate(y_poly):
            zeta[i] = zeta[i] + step_len * a
        y_image = [a + SHIFT * b for a, b in zip([zero] + y_poly, y_poly + [zero])]
        r_poly = [a - step_len * b for a, b in zip(r_poly + [zero], y_image)]
        prev_norm = norm

    along_w = zeta[1] * mu1 + zeta[2] * mu2
    along_b = zeta[2] * mu1
    res_b = (r_poly[2] - SHIFT * r_poly[3]) * mu1 + r_poly[3] * mu2
    res_bb = r_poly[3] * mu1

    def final_row(y, carry):
        w, b1, b2 = vec[y + DEPTH, :, 0:NX], img1[y + DEPTH, :, 0:NX], img2[y]
        at = pl.ds(y, 1)
        comb[0, at, :] = jnp.sum(along_w * w + along_b * b1, axis=0, keepdims=True)
        comb[1, at, :] = jnp.sum(res_b * b1 + res_bb * b2, axis=0, keepdims=True)
        return carry

    lax.fori_loop(0, NY, final_row, 0, unroll=8)
    p0, v1, a1, a2, r0 = (res[i, 8:24, 0:NX] for i in range(5))
    out[0] = (
        st[8:24, 0:NX] + (zeta[0] * p0 + zeta[1] * v1 + zeta[2] * a1) - comb[0]
    )
    out[1] = (
        r_poly[0] * r0 + (r_poly[1] * v1 + r_poly[2] * a1 + r_poly[3] * a2) - comb[1]
    )


def shards(right_side, first_guess, cell_mask, cond_east, cond_north, surface, recycled):
    sizes = tuple(lax.axis_size(axis) for axis in AXES)
    ny_dev, nzh, nx_dev, nzl, ncore = sizes
    na, nb, nc = nx_dev * ncore, ny_dev, nzh * nzl
    nd, ne = nx_dev * ny_dev, nzh * nzl * ncore
    vmem = pltpu.VMEM
    dma = pltpu.SemaphoreType.DMA
    both = pl.pallas_call(
        functools.partial(kernel, sizes),
        out_shape=jax.ShapeDtypeStruct((2, NY, NX), f32),
        in_specs=[pl.BlockSpec(memory_space=pl.ANY)] * 7,
        out_specs=pl.BlockSpec(memory_space=pltpu.VMEM),
        scratch_shapes=[
            vmem((ROWS, K, WIDE), f32),
            vmem((ROWS, K, WIDE), f32),
            vmem((NY, K, NX), f32),
            vmem((6, NAT, WIDE), f32),
            vmem((6, NAT, NX), f32),
            vmem((5, NAT, WIDE), f32),
            vmem((NAT, WIDE), f32),
            vmem((5, NAT, WIDE), f32),
            vmem((NY, NX), jnp.int32),
            vmem((2, K, 128), f32),
            vmem((6, K, 128), f32),
            vmem((2, NY, 128), f32),
            vmem((6, NY, 128), f32),
            vmem((3, 3, 8, 128), f32),
            vmem((2, na, 8, 128), f32),
            vmem((2, nb, 8, 128), f32),
            vmem((2, nc, 8, 128), f32),
            vmem((nd, 128), f32),
            vmem((ne, 128), f32),
            vmem((2, NY, NX), f32),
            vmem((2, 2, K, NX), f32),
            dma((22,)),
            dma((28,)),
            dma((28,)),
            dma((2, na)),
            dma((2, nb)),
            dma((2, nc)),
            dma((nd,)),
            dma((ne,)),
            dma((2, na)),
            dma((2, nb)),
            dma((2, nc)),
            dma((nd,)),
            dma((ne,)),
        ],
        compiler_params=pltpu.CompilerParams(collective_id=0, has_side_effects=True),
    )(right_side, first_guess, cell_mask, cond_east, cond_north, surface, recycled)
    return both[0], both[1]


def finer_mesh(mesh):
    return Mesh(mesh.devices.reshape(8, 3, 4, 4, 2), AXES)


def solution(mesh):
    in_specs = (P(LAT, LON),) * 6 + (P(None, LAT, LON),)
    out_specs = (P(LAT, LON), P(LAT, LON))
    return jax.shard_map(
        shards, mesh=finer_mesh(mesh), in_specs=in_specs, out_specs=out_specs, check_vma=False
    )
```

```python
import functools

import jax
import jax.numpy as jnp
from jax import lax
from jax.experimental import pallas as pl
from jax.experimental.pallas import tpu as pltpu
from jax.sharding import Mesh
from jax.sharding import PartitionSpec as P

LAT = ("lat_0", "lat_1", "lat_2")
LON = ("lon_0", "lon_1")
AXES = LAT + LON
MESH = pl.DeviceIdType.MESH
HIGHEST = lax.Precision.HIGHEST

K = 16
DEPTH = 4
SHIFT = 4.0
NY = 16
NX = 640
WIDE = NX + 128
ROWS = NY + 2 * DEPTH
NAT = NY + 16
WET, NORTH, GUESS, EAST, SURF, RHS = range(6)

f32 = jnp.float32


def far_first(n):
    return sorted(range(1, n), key=lambda d: -min(d, n - d))


def iota(shape, axis):
    return lax.broadcasted_iota(jnp.int32, shape, axis)


def kernel(
    sizes,
    rhs_hbm,
    guess_hbm,
    mask_hbm,
    east_hbm,
    north_hbm,
    surf_hbm,
    rec_hbm,
    out,
    vec,
    img1,
    img2,
    nat,
    land,
    coef,
    st,
    res,
    mask_v,
    pack_vec,
    got_vec,
    pack_nat,
    got_nat,
    ar_send,
    ar_a,
    ar_b,
    ar_c,
    ar_d,
    ar_e,
    comb,
    relay,
    in_sem,
    halo_send,
    halo_recv,
    ssem_a,
    ssem_b,
    ssem_c,
    ssem_d,
    ssem_e,
    rsem_a,
    rsem_b,
    rsem_c,
    rsem_d,
    rsem_e,
):
    ny_dev, nzh, nx_dev, nzl, ncore = sizes
    my_y = lax.axis_index("lat_0")
    my_zh = lax.axis_index("lat_1")
    my_x = lax.axis_index("lat_2")
    my_zl = lax.axis_index("lon_0")
    my_c = lax.axis_index("lon_1")
    n_lat = ny_dev * nzh * nx_dev
    n_lon = nzl * ncore
    my_lat = (my_y * nzh + my_zh) * nx_dev + my_x
    my_lon = my_zl * ncore + my_c
    na, nb, nc = nx_dev * ncore, ny_dev, nzh * nzl
    nd, ne = nx_dev * ny_dev, nzh * nzl * ncore
    my_a = my_x * ncore + my_c
    my_z = my_zh * nzl + my_zl
    my_d = my_y * nx_dev + my_x
    my_e = my_z * ncore + my_c

    def at_cell(up, right):
        lat = lax.rem(my_lat + (up + n_lat), n_lat)
        lon = lax.rem(my_lon + (right + n_lon), n_lon)
        rest = lat // nx_dev
        return (
            rest // nzh,
            lax.rem(rest, nzh),
            lax.rem(lat, nx_dev),
            lon // ncore,
            lax.rem(lon, ncore),
        )

    def at_a(index):
        return (my_y, my_zh, index // ncore, my_zl, lax.rem(index, ncore))

    def at_b(index):
        return (index, my_zh, my_x, my_zl, my_c)

    def at_c(index):
        return (my_y, index // nzl, my_x, lax.rem(index, nzl), my_c)

    def at_d(index):
        return (index // nx_dev, my_zh, lax.rem(index, nx_dev), my_zl, my_c)

    def at_e(index):
        z = index // ncore
        return (my_y, z // nzl, my_x, lax.rem(z, nzl), lax.rem(index, ncore))

    north_of, south_of = at_cell(1, 0), at_cell(-1, 0)
    east_of, west_of = at_cell(0, 1), at_cell(0, -1)
    corners = (at_cell(1, 1), at_cell(1, -1), at_cell(-1, 1), at_cell(-1, -1))

    plain = (
        (east_hbm, EAST),
        (north_hbm, NORTH),
        (surf_hbm, SURF),
        (rhs_hbm, RHS),
        (guess_hbm, GUESS),
    )
    loads = [pltpu.make_async_copy(mask_hbm, mask_v, in_sem.at[0])]
    for i, (src, field) in enumerate(plain):
        loads.append(
            pltpu.make_async_copy(
                src, nat.at[field, pl.ds(8, NY), pl.ds(0, NX)], in_sem.at[1 + i]
            )
        )
    for k in range(K):
        loads.append(
            pltpu.make_async_copy(
                rec_hbm.at[k], vec.at[pl.ds(DEPTH, NY), k, pl.ds(0, NX)], in_sem.at[6 + k]
            )
        )
    for load in loads:
        load.start()

    barrier = pltpu.get_barrier_semaphore()
    peers = [north_of, south_of, *corners, east_of, west_of]
    groups = [
        [at(lax.rem(me + d, n)) for d in far_first(n)]
        for n, me, at in ((ne, my_e, at_e), (nd, my_d, at_d), (na, my_a, at_a))
    ]
    for i in range(max(len(group) for group in groups)):
        peers += [group[i] for group in groups if i < len(group)]
    for peer in peers:
        pl.semaphore_signal(barrier, inc=1, device_id=peer, device_id_type=MESH)

    nat[:, 0:8, :] = jnp.zeros((6, 8, WIDE), f32)
    nat[:, 24:32, :] = jnp.zeros((6, 8, WIDE), f32)
    nat[:, 8:24, NX:] = jnp.zeros((6, NY, 128), f32)
    res[:, 0:8, :] = jnp.zeros((5, 8, WIDE), f32)
    res[:, 24:32, :] = jnp.zeros((5, 8, WIDE), f32)

    for load in loads:
        load.wait()
    nat[WET, 8:24, 0:NX] = mask_v[...].astype(f32)

    def remote(src, dst, at, slot):
        return pltpu.make_async_remote_copy(
            src_ref=src,
            dst_ref=dst,
            send_sem=halo_send.at[slot],
            recv_sem=halo_recv.at[slot],
            device_id=at,
            device_id_type=MESH,
        )

    def start_all(copies):
        for copy in copies:
            copy.start()

    def wait_all(copies):
        for copy in copies:
            copy.wait()

    lanes = pl.ds(0, NX)
    lane16 = iota((K, 128), 1)
    sub16 = iota((K, 128), 0)
    zero16 = jnp.zeros((K, 128), f32)

    def pack_vectors():
        def row(y, carry):
            to_west, to_east = carry
            e, lane = y + DEPTH, DEPTH * y
            first = pltpu.roll(vec[e, :, 0:128], lane, 1)
            last = pltpu.roll(vec[e, :, NX - 128 : NX], lane + DEPTH, 1)
            mine = (lane16 >= lane) & (lane16 < lane + DEPTH)
            return jnp.where(mine, first, to_west), jnp.where(mine, last, to_east)

        to_west, to_east = lax.fori_loop(0, NY, row, (zero16, zero16), unroll=4)
        pack_vec[0] = to_west
        pack_vec[1] = to_east

    def edge_columns(from_east, from_west, lane):
        return jnp.where(
            lane < DEPTH, from_east, jnp.where(lane >= 128 - DEPTH, from_west, 0.0)
        )

    def unpack_vectors(first, count, y0, place):
        def row(i, carry):
            lane = DEPTH * (y0 + i)
            from_east = pltpu.roll(got_vec[place], lax.rem(128 - lane, 128), 1)
            from_west = pltpu.roll(got_vec[place + 1], 128 - DEPTH - lane, 1)
            vec[first + i, :, NX:] = edge_columns(from_east, from_west, lane16)
            return carry

        lax.fori_loop(0, count, row, 0, unroll=4)

    def pack_plain():
        to_west, to_east = zero16, zero16
        for i in range(6):
            lane = DEPTH * i
            first, last = nat[i, 8:24, 0:128], nat[i, 8:24, NX - 128 : NX]
            if i:
                first = pltpu.roll(first, lane, 1)
            last = pltpu.roll(last, lane + DEPTH, 1)
            mine = (lane16 >= lane) & (lane16 < lane + DEPTH)
            to_west = jnp.where(mine, first, to_west)
            to_east = jnp.where(mine, last, to_east)
        pack_nat[0] = to_west
        pack_nat[1] = to_east

    def unpack_plain(first, count, y0, place):
        lane = lane16[0:count]
        for i in range(6):
            from_east = got_nat[place, y0 : y0 + count, :]
            from_west = got_nat[place + 1, y0 : y0 + count, :]
            if i:
                from_east = pltpu.roll(from_east, 128 - DEPTH * i, 1)
            from_west = pltpu.roll(from_west, 128 - DEPTH - DEPTH * i, 1)
            nat[i, first : first + count, NX:] = edge_columns(from_east, from_west, lane)

    def landed(first, count, near, far):
        for i in range(first, first + count):
            nat[i, 8 - far : 9 - near, 0:NX] = land[i, 8 - far : 9 - near, :]
            nat[i, 23 + near : 24 + far, 0:NX] = land[i, 23 + near : 24 + far, :]

    def vector_rows(near, far, slot):
        n = far - near + 1
        return [
            remote(
                vec.at[pl.ds(20 - far, n), :, lanes],
                vec.at[pl.ds(4 - far, n), :, lanes],
                north_of,
                slot,
            ),
            remote(
                vec.at[pl.ds(3 + near, n), :, lanes],
                vec.at[pl.ds(19 + near, n), :, lanes],
                south_of,
                slot + 1,
            ),
        ]

    def far_rows():
        ahead, behind = lax.rem(my_zh + 1, nzh), lax.rem(my_zh + (nzh - 1), nzh)
        next_y = jnp.where(my_zh == nzh - 1, lax.rem(my_y + 1, ny_dev), my_y)
        last_y = jnp.where(my_zh == 0, lax.rem(my_y + (ny_dev - 1), ny_dev), my_y)
        ways = (
            (
                my_x == nx_dev - 1,
                my_x == 0,
                vec.at[pl.ds(16, 2), :, lanes],
                vec.at[pl.ds(0, 2), :, lanes],
                north_of,
                (next_y, my_zh, 0, my_zl, my_c),
                (my_y, ahead, my_x, my_zl, my_c),
            ),
            (
                my_x == 0,
                my_x == nx_dev - 1,
                vec.at[pl.ds(6, 2), :, lanes],
                vec.at[pl.ds(22, 2), :, lanes],
                south_of,
                (last_y, my_zh, nx_dev - 1, my_zl, my_c),
                (my_y, behind, my_x, my_zl, my_c),
            ),
        )

        def copy(src, dst, at, send_slot, recv_slot):
            return pltpu.make_async_remote_copy(
                src_ref=src,
                dst_ref=dst,
                send_sem=halo_send.at[send_slot],
                recv_sem=halo_recv.at[recv_slot],
                device_id=at,
                device_id_type=MESH,
            )

        hops = []
        for i, (crosses, forwards, src, dst, straight, first_hop, last_hop) in enumerate(ways):
            held = relay.at[i]
            hops.append(
                (
                    crosses,
                    forwards,
                    copy(src, dst, straight, 22 + i, 22 + i),
                    copy(src, held, first_hop, 24 + i, 24 + i),
                    copy(held, dst, last_hop, 26 + i, 22 + i),
                )
            )

        def begin():
            for crosses, _, straight, first, _ in hops:
                pl.when(jnp.logical_not(crosses))(straight.start)
                pl.when(crosses)(first.start)

        def forward():
            for _, forwards, _, first, last in hops:

                @pl.when(forwards)
                def _():
                    first.wait_recv()
                    last.start()

        def finish():
            for crosses, forwards, straight, first, last in hops:
                pl.when(jnp.logical_not(crosses))(straight.wait_send)
                pl.when(crosses)(first.wait_send)
                pl.when(forwards)(last.wait_send)
                straight.wait_recv()

        return begin, forward, finish

    def columns(pack, got, slot):
        return [
            remote(pack.at[0], got.at[0], west_of, slot),
            remote(pack.at[1], got.at[1], east_of, slot + 1),
        ]

    def corner_columns(pack, got, slot, south_rows, north_rows):
        north_east, north_west, south_east, south_west = corners
        return [
            remote(pack.at[0, south_rows], got.at[2, south_rows], south_west, slot),
            remote(pack.at[1, south_rows], got.at[3, south_rows], south_east, slot + 1),
            remote(pack.at[0, north_rows], got.at[4, north_rows], north_west, slot + 2),
            remote(pack.at[1, north_rows], got.at[5, north_rows], north_east, slot + 3),
        ]

    def plain_rows(first, count, near, far, slot):
        fields, n = pl.ds(first, count), far - near + 1
        return [
            remote(
                nat.at[fields, pl.ds(24 - far, n), lanes],
                land.at[fields, pl.ds(8 - far, n)],
                north_of,
                slot,
            ),
            remote(
                nat.at[fields, pl.ds(7 + near, n), lanes],
                land.at[fields, pl.ds(23 + near, n)],
                south_of,
                slot + 1,
            ),
        ]

    pack_vectors()
    pack_plain()
    pl.semaphore_wait(barrier, len(peers))

    near_rows = plain_rows(0, 3, 1, 1, 0)
    vec_rows = vector_rows(1, 1, 2)
    vec_columns = columns(pack_vec, got_vec, 4)
    near_columns = columns(pack_nat, got_nat, 6)
    all_rows = pl.ds(0, NY)
    far = far_rows()
    deep = (
        corner_columns(pack_nat, got_nat, 18, pl.ds(0, 8), pl.ds(8, 8))
        + plain_rows(0, 3, 2, DEPTH, 8)
        + plain_rows(3, 3, 1, DEPTH - 1, 10)
        + corner_columns(pack_vec, got_vec, 14, all_rows, all_rows)
        + vector_rows(2, 2, 12)
    )
    start_all(near_columns)
    start_all(vec_columns)
    start_all(near_rows)
    start_all(vec_rows)
    far[0]()

    def east(v):
        return pltpu.roll(v, WIDE - 1, 1)

    def west(v):
        return pltpu.roll(v, 1, 1)

    def north(v):
        return pltpu.roll(v, NAT - 1, 0)

    def south(v):
        return pltpu.roll(v, 1, 0)

    def coefficients():
        row_n = iota((NAT, WIDE), 0)
        beyond = ((row_n < 8) & (my_lat == 0)) | ((row_n >= 24) & (my_lat == n_lat - 1))
        wet = jnp.where(beyond, 0.0, nat[WET])
        k_east = nat[EAST] * wet * east(wet)
        k_north = nat[NORTH] * wet * north(wet)
        k_west = west(k_east)
        k_south = south(k_north)
        coef[1] = k_east
        coef[2] = k_west
        coef[3] = k_north
        coef[4] = k_south
        coef[0] = nat[SURF] * wet + k_east + k_west + k_north + k_south + (1.0 - wet)

    def operate(v):
        return coef[0] * v - (
            coef[1] * east(v) + coef[2] * west(v) + coef[3] * north(v) + coef[4] * south(v)
        )

    def image_row(src, e):
        at = pl.ds(e + 4, 1)
        v = src[e]
        return coef[0, at, :] * v - (
            coef[1, at, :] * east(v)
            + coef[2, at, :] * west(v)
            + coef[3, at, :] * src[e + 1]
            + coef[4, at, :] * src[e - 1]
        )

    def fold(v):
        total = v[:, 0:128]
        for i in range(1, NX // 128):
            total = total + v[:, 128 * i : 128 * i + 128]
        return total

    def contract(a, b):
        return lax.dot_general(
            a, b, (((1,), (1,)), ((), ())), precision=HIGHEST, preferred_element_type=f32
        )

    def first_pair(rows, carry):
        acc, w_s, b_s = carry
        both = []
        for y in rows:
            w = vec[y + DEPTH, :, 0:NX]
            image = image_row(vec, y + DEPTH)
            img1[y + DEPTH] = image
            b = image[:, 0:NX]
            s = st[pl.ds(y + 8, 1), 0:NX]
            w_s = w_s + fold(w * s)
            b_s = b_s + fold(b * s)
            both.append(jnp.concatenate([w, b], axis=0))
        both = jnp.concatenate(both, axis=1)
        return acc + contract(both, both), w_s, b_s

    def start_residual():
        st[...] = nat[RHS] - operate(nat[GUESS])

    wait_all(near_columns)
    unpack_plain(8, NY, 0, 0)
    coefficients()
    start_residual()
    wait_all(vec_columns)
    unpack_vectors(DEPTH, NY, 0, 0)
    carry = (jnp.zeros((2 * K, 2 * K), f32), zero16, zero16)
    carry = lax.fori_loop(
        0, NY // 2 - 1, lambda i, c: first_pair((2 * i + 1, 2 * i + 2), c), carry
    )
    start_all(deep)
    far[1]()
    wait_all(near_rows)
    landed(0, 3, 1, 1)
    coefficients()
    start_residual()
    wait_all(vec_rows)
    acc, w_s, b_s = first_pair((0, NY - 1), carry)

    def put(block, lane):
        wide = jnp.concatenate([block, jnp.zeros((K, 128 - block.shape[1]), f32)], axis=1)
        return pltpu.roll(wide, lane, 1) if lane else wide

    lane8 = lax.rem(lane16, 8)

    def column(payload, lane, total):
        return jnp.where(lane8 == lane, jnp.sum(total, axis=1, keepdims=True), payload)

    def pick(row, lane):
        return jnp.sum(jnp.where(lane16 == 8 * sub16 + lane, row, 0.0), axis=1, keepdims=True)

    def pack(v, width):
        per, shift = 128 // width, 128 if width == 8 else width
        while shift < 128:
            v = v + pltpu.roll(v, shift, 1)
            shift *= 2
        v = jnp.where(lane16 // width == lax.rem(sub16, per), v, 0.0)
        return [
            jnp.sum(jnp.where(sub16 // per == i, v, 0.0), axis=0, keepdims=True)
            for i in range(K // per)
        ]

    def unpack(rows, width):
        per, shift = 128 // width, width
        v = jnp.broadcast_to(rows[0], (K, 128))
        for i in range(1, K // per):
            v = jnp.where(sub16 // per == i, rows[i], v)
        v = jnp.where(lane16 // width == lax.rem(sub16, per), v, 0.0)
        while shift < 128:
            v = v + pltpu.roll(v, shift, 1)
            shift *= 2
        return jnp.where(lane16 < width, v, 0.0)

    def send_phase(phase, value):
        send, buf, ssem, rsem, n, me, at, count = phase
        if count == 1:
            send[0:1, :] = value
            src, dst = send.at[pl.ds(0, 1)], buf.at[pl.ds(me, 1)]
        else:
            for i, row in enumerate(value):
                send[i : i + 1, :] = row
            src, dst = send.at[pl.ds(0, count)], buf.at[me, pl.ds(0, count)]
        for d in far_first(n):
            pltpu.make_async_remote_copy(
                src_ref=src,
                dst_ref=dst,
                send_sem=ssem.at[d],
                recv_sem=rsem.at[me],
                device_id=at(lax.rem(me + d, n)),
                device_id_type=MESH,
            ).start()
        if count == 1:
            buf[pl.ds(me, 1), :] = value
        else:
            for i, row in enumerate(value):
                buf[me, i : i + 1, :] = row

    def wait_phase(phase):
        send, buf, ssem, rsem, n, me, at, count = phase
        for d in reversed(far_first(n)):
            peer = lax.rem(me + d, n)
            if count == 1:
                src, dst = send.at[pl.ds(0, 1)], buf.at[pl.ds(peer, 1)]
            else:
                src, dst = send.at[pl.ds(0, count)], buf.at[peer, pl.ds(0, count)]
            pltpu.make_async_remote_copy(
                src_ref=src,
                dst_ref=dst,
                send_sem=ssem.at[d],
                recv_sem=rsem.at[peer],
                device_id=at(peer),
                device_id_type=MESH,
            ).wait_recv()
        if count == 1:
            return jnp.sum(buf[...], axis=0, keepdims=True)
        total = buf[0]
        for i in range(1, n):
            total = total + buf[i]
        return [total[i : i + 1, :] for i in range(count)]

    def finish_sends(phase):
        send, buf, ssem, rsem, n, me, at, count = phase
        src = send.at[pl.ds(0, count)]
        for d in range(1, n):
            pltpu.make_async_remote_copy(
                src_ref=src,
                dst_ref=src,
                send_sem=ssem.at[d],
                recv_sem=rsem.at[me],
                device_id=at(lax.rem(me + d, n)),
                device_id_type=MESH,
            ).wait_send()

    def three_phases(turn, count):
        return (
            (ar_send.at[turn, 0], ar_a.at[turn], ssem_a.at[turn], rsem_a.at[turn], na, my_a, at_a, count),
            (ar_send.at[turn, 1], ar_b.at[turn], ssem_b.at[turn], rsem_b.at[turn], nb, my_y, at_b, count),
            (ar_send.at[turn, 2], ar_c.at[turn], ssem_c.at[turn], rsem_c.at[turn], nc, my_z, at_c, count),
        )

    two_phases = (
        (ar_send.at[2, 0], ar_d, ssem_d, rsem_d, nd, my_d, at_d, 1),
        (ar_send.at[2, 1], ar_e, ssem_e, rsem_e, ne, my_e, at_e, 1),
    )

    def all_reduce(phases, value, between):
        for step, phase in enumerate(phases):
            send_phase(phase, value)
            if between[step] is not None:
                between[step]()
            value = wait_phase(phase)
        return value

    first_phases = three_phases(0, 5)
    g3_phases = three_phases(1, 2)
    kept = {}

    def second_pair(rows, acc):
        left, right = [], []
        for y in rows:
            left.append(img1[y + DEPTH, :, 0:NX])
            right.append(image_row(img1, y + DEPTH)[:, 0:NX])
            img2[y] = right[-1]
        left, right = jnp.concatenate(left, axis=1), jnp.concatenate(right, axis=1)
        return acc + contract(left, right)

    def between_a():
        acc = jnp.zeros((K, K), f32)
        kept["g3"] = lax.fori_loop(
            0, NY // 2 - 1, lambda i, c: second_pair((2 * i + 1, 2 * i + 2), c), acc
        )

    def between_c():
        wait_all(deep)
        far[2]()
        landed(0, 3, 2, DEPTH)
        landed(3, 3, 1, DEPTH - 1)
        unpack_plain(24, 8, 0, 2)
        unpack_plain(0, 8, 8, 4)
        unpack_vectors(NY + DEPTH, DEPTH, 0, 2)
        unpack_vectors(0, DEPTH, NY - DEPTH, 4)
        coefficients()
        start_residual()

        def outer_row(i, carry):
            img1[i + 1] = image_row(vec, i + 1)
            img1[i + 19] = image_row(vec, i + 19)
            return carry

        lax.fori_loop(0, DEPTH, outer_row, 0)
        acc = second_pair((0, NY - 1), kept["g3"])
        send_phase(g3_phases[0], pack(put(acc, 0), K))
        finish_sends(first_phases[0])
        finish_sends(first_phases[1])

    grams = 0.5 * (put(acc[0:K, K:], 0) + put(acc[K:, 0:K], 0)) + put(acc[K:, K:], K)
    rows = pack(grams, 2 * K) + pack(column(column(zero16, 0, w_s), 1, b_s), 8)
    rows = all_reduce(first_phases, rows, (between_a, None, between_c))
    grams = unpack(rows[0:4], 2 * K)
    starts = [pick(rows[4], lane) for lane in (0, 1)]


    def at_zero(v, lane):
        v = jnp.where((lane16 >= lane) & (lane16 < lane + K), v, 0.0)
        return pltpu.roll(v, (128 - lane) % 128, 1) if lane else v

    aug = jnp.where(lane16 < K, grams, 0.0)
    aug = jnp.where(lane16 == sub16 + K, 1.0, aug)
    aug = jnp.where(lane16 == 2 * K, starts[0], aug)
    pivots = jnp.broadcast_to(aug[:, 0:1], (K, 128))
    for i in range(K):
        scale = 1.0 / pivots[i : i + 1, :]
        pivot_row = aug[i : i + 1, :] * scale
        column_now = pivots
        if i + 1 < K:
            coming = jnp.broadcast_to(aug[:, i + 1 : i + 2], (K, 128))
            coming_row = coming[i : i + 1, :] * scale
            pivots = jnp.where(sub16 == i, coming_row, coming - column_now * coming_row)
        aug = jnp.where(sub16 == i, pivot_row, aug - column_now * pivot_row)
    coarse = aug[:, 2 * K : 2 * K + 1]
    inverse = at_zero(aug, K)
    g1, g2 = at_zero(grams, 0), at_zero(grams, K)

    def as_row(col):
        return jnp.sum(jnp.where(lane16 == sub16, col, 0.0), axis=0, keepdims=True)

    def row_times(mat, row):
        return jnp.sum(mat * row, axis=1, keepdims=True)

    def times_column(mat, col):
        return jnp.sum(mat * col, axis=0, keepdims=True)

    def apply(mat, col):
        return row_times(mat, as_row(col))

    def dot(a, b):
        return jnp.sum(a * b, axis=0, keepdims=True)

    w_row, b_row = as_row(starts[0]), as_row(starts[1])
    coarse = coarse + row_times(inverse, w_row - times_column(g1, coarse))
    mu0 = row_times(inverse, b_row - times_column(g2, coarse))


    def residual_row(e, carry):
        at = pl.ds(e + 4, 1)
        r = st[at, :] - jnp.sum(coarse * img1[e], axis=0, keepdims=True)
        res[4, at, :] = r
        res[0, at, :] = r - jnp.sum(mu0 * vec[e], axis=0, keepdims=True)
        return carry

    lax.fori_loop(1, ROWS - 1, residual_row, 0, unroll=11)
    send_phase(g3_phases[1], wait_phase(g3_phases[0]))
    for i, base in enumerate((4, 1, 2)):
        res[i + 1] = operate(res[i]) - SHIFT * res[base]

    def moment_row(y, carry):
        b1, b2 = img1[y + DEPTH, :, 0:NX], img2[y]
        v1, a1 = (res[i, pl.ds(y + 8, 1), 0:NX] for i in (1, 2))
        terms = (b1 * v1, b1 * a1, b2 * a1)
        return tuple(total + fold(term) for total, term in zip(carry, terms))

    defl = lax.fori_loop(0, NY, moment_row, (zero16,) * 3, unroll=4)
    payload = zero16
    for i, total in enumerate(defl):
        payload = column(payload, i, total)
    inner = [res[i, 8:24, 0:NX] for i in (4, 1, 2, 3)]
    for i, (a, b) in enumerate(((0, 0), (0, 1), (1, 1), (1, 2), (2, 2), (2, 3))):
        total = jnp.sum(fold(inner[a] * inner[b]), axis=0, keepdims=True)
        total = jnp.sum(total, axis=1, keepdims=True)
        payload = jnp.where((lane8 == 3) & (sub16 == i), total, payload)

    def before_scalars():
        def row(y, carry):
            at = pl.ds(y + 8, 1)
            along = jnp.sum(coarse * vec[y + DEPTH, :, 0:NX], axis=0, keepdims=True)
            st[at, 0:NX] = nat[GUESS, at, 0:NX] + along
            return carry

        lax.fori_loop(0, NY, row, 0, unroll=4)
        send_phase(g3_phases[2], wait_phase(g3_phases[1]))
        for phase in (first_phases[2], g3_phases[0], g3_phases[1]):
            finish_sends(phase)

    def last_gram():
        kept["g3"] = unpack(wait_phase(g3_phases[2]), K)
        for phase in (g3_phases[2], *two_phases):
            finish_sends(phase)

    row = all_reduce(two_phases, pack(payload, 8)[0], (before_scalars, last_gram))

    g3 = kept["g3"]
    e = [pick(row, i) for i in range(3)]
    t_all = pick(row, 3)
    t = [t_all[i : i + 1, :] for i in range(6)]
    mu1 = apply(inverse, e[0])
    g2_1, g3_1 = apply(g2, mu1), apply(g3, mu1)
    defl2 = e[1] - g2_1
    mu2 = apply(inverse, defl2)
    m = [
        t[0],
        t[1],
        t[2],
        t[3] - dot(mu1, e[0]),
        t[4] - 2.0 * dot(mu1, e[1]) + dot(mu1, g2_1),
        t[5]
        - 2.0 * dot(mu1, e[2] - SHIFT * e[1])
        + dot(mu1, g3_1 - SHIFT * g2_1)
        - dot(mu2, defl2),
    ]

    def form(poly, shift):
        total = 0.0
        for i, a in enumerate(poly):
            for j, b in enumerate(poly):
                total = total + a * b * m[i + j + shift]
        return total

    one = jnp.ones((1, 1), f32)
    zero = jnp.zeros((1, 1), f32)
    r_poly = [one]
    y_poly = [zero]
    zeta = [zero, zero, zero]
    curv = prev_norm = one
    for turn in range(3):
        norm = form(r_poly, 0)
        r_image = form(r_poly, 1) + SHIFT * norm
        if turn == 0:
            y_poly = list(r_poly)
            curv = r_image
        else:
            ratio = norm / prev_norm
            y_poly = [a + ratio * b for a, b in zip(r_poly, y_poly + [zero])]
            curv = r_image - ratio * ratio * curv
        step_len = norm / curv
        for i, a in enumerate(y_poly):
            zeta[i] = zeta[i] + step_len * a
        y_image = [a + SHIFT * b for a, b in zip([zero] + y_poly, y_poly + [zero])]
        r_poly = [a - step_len * b for a, b in zip(r_poly + [zero], y_image)]
        prev_norm = norm

    along_w = zeta[1] * mu1 + zeta[2] * mu2
    along_b = zeta[2] * mu1
    res_b = (r_poly[2] - SHIFT * r_poly[3]) * mu1 + r_poly[3] * mu2
    res_bb = r_poly[3] * mu1

    def final_row(y, carry):
        w, b1, b2 = vec[y + DEPTH, :, 0:NX], img1[y + DEPTH, :, 0:NX], img2[y]
        at = pl.ds(y, 1)
        comb[0, at, :] = jnp.sum(along_w * w + along_b * b1, axis=0, keepdims=True)
        comb[1, at, :] = jnp.sum(res_b * b1 + res_bb * b2, axis=0, keepdims=True)
        return carry

    lax.fori_loop(0, NY, final_row, 0, unroll=8)
    p0, v1, a1, a2, r0 = (res[i, 8:24, 0:NX] for i in range(5))
    out[0] = (
        st[8:24, 0:NX] + (zeta[0] * p0 + zeta[1] * v1 + zeta[2] * a1) - comb[0]
    )
    out[1] = (
        r_poly[0] * r0 + (r_poly[1] * v1 + r_poly[2] * a1 + r_poly[3] * a2) - comb[1]
    )


def shards(right_side, first_guess, cell_mask, cond_east, cond_north, surface, recycled):
    sizes = tuple(lax.axis_size(axis) for axis in AXES)
    ny_dev, nzh, nx_dev, nzl, ncore = sizes
    na, nb, nc = nx_dev * ncore, ny_dev, nzh * nzl
    nd, ne = nx_dev * ny_dev, nzh * nzl * ncore
    vmem = pltpu.VMEM
    dma = pltpu.SemaphoreType.DMA
    both = pl.pallas_call(
        functools.partial(kernel, sizes),
        out_shape=jax.ShapeDtypeStruct((2, NY, NX), f32),
        in_specs=[pl.BlockSpec(memory_space=pl.ANY)] * 7,
        out_specs=pl.BlockSpec(memory_space=pltpu.VMEM),
        scratch_shapes=[
            vmem((ROWS, K, WIDE), f32),
            vmem((ROWS, K, WIDE), f32),
            vmem((NY, K, NX), f32),
            vmem((6, NAT, WIDE), f32),
            vmem((6, NAT, NX), f32),
            vmem((5, NAT, WIDE), f32),
            vmem((NAT, WIDE), f32),
            vmem((5, NAT, WIDE), f32),
            vmem((NY, NX), jnp.int32),
            vmem((2, K, 128), f32),
            vmem((6, K, 128), f32),
            vmem((2, NY, 128), f32),
            vmem((6, NY, 128), f32),
            vmem((3, 3, 8, 128), f32),
            vmem((2, na, 8, 128), f32),
            vmem((2, nb, 8, 128), f32),
            vmem((2, nc, 8, 128), f32),
            vmem((nd, 128), f32),
            vmem((ne, 128), f32),
            vmem((2, NY, NX), f32),
            vmem((2, 2, K, NX), f32),
            dma((22,)),
            dma((28,)),
            dma((28,)),
            dma((2, na)),
            dma((2, nb)),
            dma((2, nc)),
            dma((nd,)),
            dma((ne,)),
            dma((2, na)),
            dma((2, nb)),
            dma((2, nc)),
            dma((nd,)),
            dma((ne,)),
        ],
        compiler_params=pltpu.CompilerParams(collective_id=0, has_side_effects=True),
    )(right_side, first_guess, cell_mask, cond_east, cond_north, surface, recycled)
    return both[0], both[1]


def finer_mesh(mesh):
    return Mesh(mesh.devices.reshape(8, 3, 4, 4, 2), AXES)


def solution(mesh):
    in_specs = (P(LAT, LON),) * 6 + (P(None, LAT, LON),)
    out_specs = (P(LAT, LON), P(LAT, LON))
    return jax.shard_map(
        shards, mesh=finer_mesh(mesh), in_specs=in_specs, out_specs=out_specs, check_vma=False
    )
```

```python
import functools

import jax
import jax.numpy as jnp
from jax import lax
from jax.experimental import pallas as pl
from jax.experimental.pallas import tpu as pltpu
from jax.sharding import Mesh
from jax.sharding import PartitionSpec as P

LAT = ("lat_0", "lat_1", "lat_2")
LON = ("lon_0", "lon_1")
AXES = LAT + LON
MESH = pl.DeviceIdType.MESH
HIGHEST = lax.Precision.HIGHEST

K = 16
DEPTH = 4
SHIFT = 4.0
NY = 16
NX = 640
WIDE = NX + 128
ROWS = NY + 2 * DEPTH
NAT = NY + 16
WET, NORTH, GUESS, EAST, SURF, RHS = range(6)

f32 = jnp.float32


def far_first(n):
    return sorted(range(1, n), key=lambda d: -min(d, n - d))


def iota(shape, axis):
    return lax.broadcasted_iota(jnp.int32, shape, axis)


def kernel(
    sizes,
    rhs_hbm,
    guess_hbm,
    mask_hbm,
    east_hbm,
    north_hbm,
    surf_hbm,
    rec_hbm,
    out,
    vec,
    img1,
    img2,
    nat,
    land,
    coef,
    st,
    res,
    mask_v,
    pack_vec,
    got_vec,
    pack_nat,
    got_nat,
    ar_send,
    ar_a,
    ar_b,
    ar_c,
    ar_d,
    ar_e,
    comb,
    relay,
    in_sem,
    halo_send,
    halo_recv,
    ssem_a,
    ssem_b,
    ssem_c,
    ssem_d,
    ssem_e,
    rsem_a,
    rsem_b,
    rsem_c,
    rsem_d,
    rsem_e,
):
    ny_dev, nzh, nx_dev, nzl, ncore = sizes
    my_y = lax.axis_index("lat_0")
    my_zh = lax.axis_index("lat_1")
    my_x = lax.axis_index("lat_2")
    my_zl = lax.axis_index("lon_0")
    my_c = lax.axis_index("lon_1")
    n_lat = ny_dev * nzh * nx_dev
    n_lon = nzl * ncore
    my_lat = (my_y * nzh + my_zh) * nx_dev + my_x
    my_lon = my_zl * ncore + my_c
    na, nb, nc = nx_dev * ncore, ny_dev, nzh * nzl
    nd, ne = nx_dev * ny_dev, nzh * nzl * ncore
    my_a = my_x * ncore + my_c
    my_z = my_zh * nzl + my_zl
    my_d = my_y * nx_dev + my_x
    my_e = my_z * ncore + my_c

    def at_cell(up, right):
        lat = lax.rem(my_lat + (up + n_lat), n_lat)
        lon = lax.rem(my_lon + (right + n_lon), n_lon)
        rest = lat // nx_dev
        return (
            rest // nzh,
            lax.rem(rest, nzh),
            lax.rem(lat, nx_dev),
            lon // ncore,
            lax.rem(lon, ncore),
        )

    def at_a(index):
        return (my_y, my_zh, index // ncore, my_zl, lax.rem(index, ncore))

    def at_b(index):
        return (index, my_zh, my_x, my_zl, my_c)

    def at_c(index):
        return (my_y, index // nzl, my_x, lax.rem(index, nzl), my_c)

    def at_d(index):
        return (index // nx_dev, my_zh, lax.rem(index, nx_dev), my_zl, my_c)

    def at_e(index):
        z = index // ncore
        return (my_y, z // nzl, my_x, lax.rem(z, nzl), lax.rem(index, ncore))

    north_of, south_of = at_cell(1, 0), at_cell(-1, 0)
    east_of, west_of = at_cell(0, 1), at_cell(0, -1)
    corners = (at_cell(1, 1), at_cell(1, -1), at_cell(-1, 1), at_cell(-1, -1))

    plain = (
        (east_hbm, EAST),
        (north_hbm, NORTH),
        (surf_hbm, SURF),
        (rhs_hbm, RHS),
        (guess_hbm, GUESS),
    )
    loads = [pltpu.make_async_copy(mask_hbm, mask_v, in_sem.at[0])]
    for i, (src, field) in enumerate(plain):
        loads.append(
            pltpu.make_async_copy(
                src, nat.at[field, pl.ds(8, NY), pl.ds(0, NX)], in_sem.at[1 + i]
            )
        )
    for k in range(K):
        loads.append(
            pltpu.make_async_copy(
                rec_hbm.at[k], vec.at[pl.ds(DEPTH, NY), k, pl.ds(0, NX)], in_sem.at[6 + k]
            )
        )
    for load in loads:
        load.start()

    barrier = pltpu.get_barrier_semaphore()
    peers = [north_of, south_of, *corners, east_of, west_of]
    groups = [
        [at(lax.rem(me + d, n)) for d in far_first(n)]
        for n, me, at in ((ne, my_e, at_e), (nd, my_d, at_d), (na, my_a, at_a))
    ]
    for i in range(max(len(group) for group in groups)):
        peers += [group[i] for group in groups if i < len(group)]
    for peer in peers:
        pl.semaphore_signal(barrier, inc=1, device_id=peer, device_id_type=MESH)

    nat[:, 0:8, :] = jnp.zeros((6, 8, WIDE), f32)
    nat[:, 24:32, :] = jnp.zeros((6, 8, WIDE), f32)
    nat[:, 8:24, NX:] = jnp.zeros((6, NY, 128), f32)
    res[:, 0:8, :] = jnp.zeros((5, 8, WIDE), f32)
    res[:, 24:32, :] = jnp.zeros((5, 8, WIDE), f32)

    for load in loads:
        load.wait()
    nat[WET, 8:24, 0:NX] = mask_v[...].astype(f32)

    def remote(src, dst, at, slot):
        return pltpu.make_async_remote_copy(
            src_ref=src,
            dst_ref=dst,
            send_sem=halo_send.at[slot],
            recv_sem=halo_recv.at[slot],
            device_id=at,
            device_id_type=MESH,
        )

    def start_all(copies):
        for copy in copies:
            copy.start()

    def wait_all(copies):
        for copy in copies:
            copy.wait()

    lanes = pl.ds(0, NX)
    lane16 = iota((K, 128), 1)
    sub16 = iota((K, 128), 0)
    zero16 = jnp.zeros((K, 128), f32)

    def pack_vectors():
        def row(y, carry):
            to_west, to_east = carry
            e, lane = y + DEPTH, DEPTH * y
            first = pltpu.roll(vec[e, :, 0:128], lane, 1)
            last = pltpu.roll(vec[e, :, NX - 128 : NX], lane + DEPTH, 1)
            mine = (lane16 >= lane) & (lane16 < lane + DEPTH)
            return jnp.where(mine, first, to_west), jnp.where(mine, last, to_east)

        to_west, to_east = lax.fori_loop(0, NY, row, (zero16, zero16), unroll=4)
        pack_vec[0] = to_west
        pack_vec[1] = to_east

    def edge_columns(from_east, from_west, lane):
        return jnp.where(
            lane < DEPTH, from_east, jnp.where(lane >= 128 - DEPTH, from_west, 0.0)
        )

    def unpack_vectors(first, count, y0, place):
        def row(i, carry):
            lane = DEPTH * (y0 + i)
            from_east = pltpu.roll(got_vec[place], lax.rem(128 - lane, 128), 1)
            from_west = pltpu.roll(got_vec[place + 1], 128 - DEPTH - lane, 1)
            vec[first + i, :, NX:] = edge_columns(from_east, from_west, lane16)
            return carry

        lax.fori_loop(0, count, row, 0, unroll=4)

    def pack_plain():
        to_west, to_east = zero16, zero16
        for i in range(6):
            lane = DEPTH * i
            first, last = nat[i, 8:24, 0:128], nat[i, 8:24, NX - 128 : NX]
            if i:
                first = pltpu.roll(first, lane, 1)
            last = pltpu.roll(last, lane + DEPTH, 1)
            mine = (lane16 >= lane) & (lane16 < lane + DEPTH)
            to_west = jnp.where(mine, first, to_west)
            to_east = jnp.where(mine, last, to_east)
        pack_nat[0] = to_west
        pack_nat[1] = to_east

    def unpack_plain(first, count, y0, place):
        lane = lane16[0:count]
        for i in range(6):
            from_east = got_nat[place, y0 : y0 + count, :]
            from_west = got_nat[place + 1, y0 : y0 + count, :]
            if i:
                from_east = pltpu.roll(from_east, 128 - DEPTH * i, 1)
            from_west = pltpu.roll(from_west, 128 - DEPTH - DEPTH * i, 1)
            nat[i, first : first + count, NX:] = edge_columns(from_east, from_west, lane)

    def landed(first, count, near, far):
        for i in range(first, first + count):
            nat[i, 8 - far : 9 - near, 0:NX] = land[i, 8 - far : 9 - near, :]
            nat[i, 23 + near : 24 + far, 0:NX] = land[i, 23 + near : 24 + far, :]

    def vector_rows(near, far, slot):
        n = far - near + 1
        return [
            remote(
                vec.at[pl.ds(20 - far, n), :, lanes],
                vec.at[pl.ds(4 - far, n), :, lanes],
                north_of,
                slot,
            ),
            remote(
                vec.at[pl.ds(3 + near, n), :, lanes],
                vec.at[pl.ds(19 + near, n), :, lanes],
                south_of,
                slot + 1,
            ),
        ]

    def far_rows():
        ahead, behind = lax.rem(my_zh + 1, nzh), lax.rem(my_zh + (nzh - 1), nzh)
        next_y = jnp.where(my_zh == nzh - 1, lax.rem(my_y + 1, ny_dev), my_y)
        last_y = jnp.where(my_zh == 0, lax.rem(my_y + (ny_dev - 1), ny_dev), my_y)
        ways = (
            (
                my_x == nx_dev - 1,
                my_x == 0,
                vec.at[pl.ds(16, 2), :, lanes],
                vec.at[pl.ds(0, 2), :, lanes],
                north_of,
                (next_y, my_zh, 0, my_zl, my_c),
                (my_y, ahead, my_x, my_zl, my_c),
            ),
            (
                my_x == 0,
                my_x == nx_dev - 1,
                vec.at[pl.ds(6, 2), :, lanes],
                vec.at[pl.ds(22, 2), :, lanes],
                south_of,
                (last_y, my_zh, nx_dev - 1, my_zl, my_c),
                (my_y, behind, my_x, my_zl, my_c),
            ),
        )

        def copy(src, dst, at, send_slot, recv_slot):
            return pltpu.make_async_remote_copy(
                src_ref=src,
                dst_ref=dst,
                send_sem=halo_send.at[send_slot],
                recv_sem=halo_recv.at[recv_slot],
                device_id=at,
                device_id_type=MESH,
            )

        hops = []
        for i, (crosses, forwards, src, dst, straight, first_hop, last_hop) in enumerate(ways):
            held = relay.at[i]
            hops.append(
                (
                    crosses,
                    forwards,
                    copy(src, dst, straight, 22 + i, 22 + i),
                    copy(src, held, first_hop, 24 + i, 24 + i),
                    copy(held, dst, last_hop, 26 + i, 22 + i),
                )
            )

        def begin():
            for crosses, _, straight, first, _ in hops:
                pl.when(jnp.logical_not(crosses))(straight.start)
                pl.when(crosses)(first.start)

        def forward():
            for _, forwards, _, first, last in hops:

                @pl.when(forwards)
                def _():
                    first.wait_recv()
                    last.start()

        def finish():
            for crosses, forwards, straight, first, last in hops:
                pl.when(jnp.logical_not(crosses))(straight.wait_send)
                pl.when(crosses)(first.wait_send)
                pl.when(forwards)(last.wait_send)
                straight.wait_recv()

        return begin, forward, finish

    def columns(pack, got, slot):
        return [
            remote(pack.at[0], got.at[0], west_of, slot),
            remote(pack.at[1], got.at[1], east_of, slot + 1),
        ]

    def corner_columns(pack, got, slot, south_rows, north_rows):
        north_east, north_west, south_east, south_west = corners
        return [
            remote(pack.at[0, south_rows], got.at[2, south_rows], south_west, slot),
            remote(pack.at[1, south_rows], got.at[3, south_rows], south_east, slot + 1),
            remote(pack.at[0, north_rows], got.at[4, north_rows], north_west, slot + 2),
            remote(pack.at[1, north_rows], got.at[5, north_rows], north_east, slot + 3),
        ]

    def plain_rows(first, count, near, far, slot):
        fields, n = pl.ds(first, count), far - near + 1
        return [
            remote(
                nat.at[fields, pl.ds(24 - far, n), lanes],
                land.at[fields, pl.ds(8 - far, n)],
                north_of,
                slot,
            ),
            remote(
                nat.at[fields, pl.ds(7 + near, n), lanes],
                land.at[fields, pl.ds(23 + near, n)],
                south_of,
                slot + 1,
            ),
        ]

    pack_vectors()
    pack_plain()
    pl.semaphore_wait(barrier, len(peers))

    near_rows = plain_rows(0, 3, 1, 1, 0)
    vec_rows = vector_rows(1, 1, 2)
    vec_columns = columns(pack_vec, got_vec, 4)
    near_columns = columns(pack_nat, got_nat, 6)
    all_rows = pl.ds(0, NY)
    far = far_rows()
    deep = (
        corner_columns(pack_nat, got_nat, 18, pl.ds(0, 8), pl.ds(8, 8))
        + plain_rows(0, 3, 2, DEPTH, 8)
        + plain_rows(3, 3, 1, DEPTH - 1, 10)
        + corner_columns(pack_vec, got_vec, 14, all_rows, all_rows)
        + vector_rows(2, 2, 12)
    )
    start_all(near_columns)
    start_all(vec_columns)
    start_all(near_rows)
    start_all(vec_rows)
    far[0]()

    def east(v):
        return pltpu.roll(v, WIDE - 1, 1)

    def west(v):
        return pltpu.roll(v, 1, 1)

    def north(v):
        return pltpu.roll(v, NAT - 1, 0)

    def south(v):
        return pltpu.roll(v, 1, 0)

    def coefficients():
        row_n = iota((NAT, WIDE), 0)
        beyond = ((row_n < 8) & (my_lat == 0)) | ((row_n >= 24) & (my_lat == n_lat - 1))
        wet = jnp.where(beyond, 0.0, nat[WET])
        k_east = nat[EAST] * wet * east(wet)
        k_north = nat[NORTH] * wet * north(wet)
        k_west = west(k_east)
        k_south = south(k_north)
        coef[1] = k_east
        coef[2] = k_west
        coef[3] = k_north
        coef[4] = k_south
        coef[0] = nat[SURF] * wet + k_east + k_west + k_north + k_south + (1.0 - wet)

    def operate(v):
        return coef[0] * v - (
            coef[1] * east(v) + coef[2] * west(v) + coef[3] * north(v) + coef[4] * south(v)
        )

    def image_row(src, e):
        at = pl.ds(e + 4, 1)
        v = src[e]
        return coef[0, at, :] * v - (
            coef[1, at, :] * east(v)
            + coef[2, at, :] * west(v)
            + coef[3, at, :] * src[e + 1]
            + coef[4, at, :] * src[e - 1]
        )

    def fold(v):
        total = v[:, 0:128]
        for i in range(1, NX // 128):
            total = total + v[:, 128 * i : 128 * i + 128]
        return total

    def contract(a, b):
        return lax.dot_general(
            a, b, (((1,), (1,)), ((), ())), precision=HIGHEST, preferred_element_type=f32
        )

    def first_pair(rows, carry):
        acc, w_s, b_s = carry
        both = []
        for y in rows:
            w = vec[y + DEPTH, :, 0:NX]
            image = image_row(vec, y + DEPTH)
            img1[y + DEPTH] = image
            b = image[:, 0:NX]
            s = st[pl.ds(y + 8, 1), 0:NX]
            w_s = w_s + fold(w * s)
            b_s = b_s + fold(b * s)
            both.append(jnp.concatenate([w, b], axis=0))
        both = jnp.concatenate(both, axis=1)
        return acc + contract(both, both), w_s, b_s

    def start_residual():
        st[...] = nat[RHS] - operate(nat[GUESS])

    wait_all(near_columns)
    unpack_plain(8, NY, 0, 0)
    coefficients()
    start_residual()
    wait_all(vec_columns)
    unpack_vectors(DEPTH, NY, 0, 0)
    carry = (jnp.zeros((2 * K, 2 * K), f32), zero16, zero16)
    carry = lax.fori_loop(
        0, NY // 2 - 1, lambda i, c: first_pair((2 * i + 1, 2 * i + 2), c), carry
    )
    start_all(deep)
    far[1]()
    wait_all(near_rows)
    landed(0, 3, 1, 1)
    coefficients()
    start_residual()
    wait_all(vec_rows)
    acc, w_s, b_s = first_pair((0, NY - 1), carry)

    def put(block, lane):
        wide = jnp.concatenate([block, jnp.zeros((K, 128 - block.shape[1]), f32)], axis=1)
        return pltpu.roll(wide, lane, 1) if lane else wide

    lane8 = lax.rem(lane16, 8)

    def column(payload, lane, total):
        return jnp.where(lane8 == lane, jnp.sum(total, axis=1, keepdims=True), payload)

    def pick(row, lane):
        return jnp.sum(jnp.where(lane16 == 8 * sub16 + lane, row, 0.0), axis=1, keepdims=True)

    def pack(v, width):
        per, shift = 128 // width, 128 if width == 8 else width
        while shift < 128:
            v = v + pltpu.roll(v, shift, 1)
            shift *= 2
        v = jnp.where(lane16 // width == lax.rem(sub16, per), v, 0.0)
        return [
            jnp.sum(jnp.where(sub16 // per == i, v, 0.0), axis=0, keepdims=True)
            for i in range(K // per)
        ]

    def unpack(rows, width):
        per, shift = 128 // width, width
        v = jnp.broadcast_to(rows[0], (K, 128))
        for i in range(1, K // per):
            v = jnp.where(sub16 // per == i, rows[i], v)
        v = jnp.where(lane16 // width == lax.rem(sub16, per), v, 0.0)
        while shift < 128:
            v = v + pltpu.roll(v, shift, 1)
            shift *= 2
        return jnp.where(lane16 < width, v, 0.0)

    def send_phase(phase, value):
        send, buf, ssem, rsem, n, me, at, count = phase
        if count == 1:
            send[0:1, :] = value
            src, dst = send.at[pl.ds(0, 1)], buf.at[pl.ds(me, 1)]
        else:
            for i, row in enumerate(value):
                send[i : i + 1, :] = row
            src, dst = send.at[pl.ds(0, count)], buf.at[me, pl.ds(0, count)]
        for d in far_first(n):
            pltpu.make_async_remote_copy(
                src_ref=src,
                dst_ref=dst,
                send_sem=ssem.at[d],
                recv_sem=rsem.at[me],
                device_id=at(lax.rem(me + d, n)),
                device_id_type=MESH,
            ).start()
        if count == 1:
            buf[pl.ds(me, 1), :] = value
        else:
            for i, row in enumerate(value):
                buf[me, i : i + 1, :] = row

    def wait_phase(phase):
        send, buf, ssem, rsem, n, me, at, count = phase
        for d in reversed(far_first(n)):
            peer = lax.rem(me + d, n)
            if count == 1:
                src, dst = send.at[pl.ds(0, 1)], buf.at[pl.ds(peer, 1)]
            else:
                src, dst = send.at[pl.ds(0, count)], buf.at[peer, pl.ds(0, count)]
            pltpu.make_async_remote_copy(
                src_ref=src,
                dst_ref=dst,
                send_sem=ssem.at[d],
                recv_sem=rsem.at[peer],
                device_id=at(peer),
                device_id_type=MESH,
            ).wait_recv()
        if count == 1:
            return jnp.sum(buf[...], axis=0, keepdims=True)
        total = buf[0]
        for i in range(1, n):
            total = total + buf[i]
        return [total[i : i + 1, :] for i in range(count)]

    def finish_sends(phase):
        send, buf, ssem, rsem, n, me, at, count = phase
        src = send.at[pl.ds(0, count)]
        for d in range(1, n):
            pltpu.make_async_remote_copy(
                src_ref=src,
                dst_ref=src,
                send_sem=ssem.at[d],
                recv_sem=rsem.at[me],
                device_id=at(lax.rem(me + d, n)),
                device_id_type=MESH,
            ).wait_send()

    def three_phases(turn, count):
        return (
            (ar_send.at[turn, 0], ar_a.at[turn], ssem_a.at[turn], rsem_a.at[turn], na, my_a, at_a, count),
            (ar_send.at[turn, 1], ar_b.at[turn], ssem_b.at[turn], rsem_b.at[turn], nb, my_y, at_b, count),
            (ar_send.at[turn, 2], ar_c.at[turn], ssem_c.at[turn], rsem_c.at[turn], nc, my_z, at_c, count),
        )

    two_phases = (
        (ar_send.at[2, 0], ar_d, ssem_d, rsem_d, nd, my_d, at_d, 1),
        (ar_send.at[2, 1], ar_e, ssem_e, rsem_e, ne, my_e, at_e, 1),
    )

    def all_reduce(phases, value, between):
        for step, phase in enumerate(phases):
            send_phase(phase, value)
            if between[step] is not None:
                between[step]()
            value = wait_phase(phase)
        return value

    first_phases = three_phases(0, 5)
    g3_phases = three_phases(1, 2)
    kept = {}

    def second_pair(rows, acc):
        left, right = [], []
        for y in rows:
            left.append(img1[y + DEPTH, :, 0:NX])
            right.append(image_row(img1, y + DEPTH)[:, 0:NX])
            img2[y] = right[-1]
        left, right = jnp.concatenate(left, axis=1), jnp.concatenate(right, axis=1)
        return acc + contract(left, right)

    def between_a():
        acc = jnp.zeros((K, K), f32)
        kept["g3"] = lax.fori_loop(
            0, NY // 2 - 1, lambda i, c: second_pair((2 * i + 1, 2 * i + 2), c), acc
        )

    def between_c():
        wait_all(deep)
        far[2]()
        landed(0, 3, 2, DEPTH)
        landed(3, 3, 1, DEPTH - 1)
        unpack_plain(24, 8, 0, 2)
        unpack_plain(0, 8, 8, 4)
        unpack_vectors(NY + DEPTH, DEPTH, 0, 2)
        unpack_vectors(0, DEPTH, NY - DEPTH, 4)
        coefficients()
        start_residual()

        def outer_row(i, carry):
            img1[i + 1] = image_row(vec, i + 1)
            img1[i + 19] = image_row(vec, i + 19)
            return carry

        lax.fori_loop(0, DEPTH, outer_row, 0)
        acc = second_pair((0, NY - 1), kept["g3"])
        send_phase(g3_phases[0], pack(put(acc, 0), K))
        finish_sends(first_phases[0])
        finish_sends(first_phases[1])

    grams = 0.5 * (put(acc[0:K, K:], 0) + put(acc[K:, 0:K], 0)) + put(acc[K:, K:], K)
    rows = pack(grams, 2 * K) + pack(column(column(zero16, 0, w_s), 1, b_s), 8)
    rows = all_reduce(first_phases, rows, (between_a, None, between_c))
    grams = unpack(rows[0:4], 2 * K)
    starts = [pick(rows[4], lane) for lane in (0, 1)]


    def at_zero(v, lane):
        v = jnp.where((lane16 >= lane) & (lane16 < lane + K), v, 0.0)
        return pltpu.roll(v, (128 - lane) % 128, 1) if lane else v

    aug = jnp.where(lane16 < K, grams, 0.0)
    aug = jnp.where(lane16 == sub16 + K, 1.0, aug)
    aug = jnp.where(lane16 == 2 * K, starts[0], aug)
    pivots = jnp.broadcast_to(aug[:, 0:1], (K, 128))
    for i in range(K):
        scale = 1.0 / pivots[i : i + 1, :]
        pivot_row = aug[i : i + 1, :] * scale
        column_now = pivots
        if i + 1 < K:
            coming = jnp.broadcast_to(aug[:, i + 1 : i + 2], (K, 128))
            coming_row = coming[i : i + 1, :] * scale
            pivots = jnp.where(sub16 == i, coming_row, coming - column_now * coming_row)
        aug = jnp.where(sub16 == i, pivot_row, aug - column_now * pivot_row)
    coarse = aug[:, 2 * K : 2 * K + 1]
    inverse = at_zero(aug, K)
    g1, g2 = at_zero(grams, 0), at_zero(grams, K)

    def as_row(col):
        return jnp.sum(jnp.where(lane16 == sub16, col, 0.0), axis=0, keepdims=True)

    def row_times(mat, row):
        return jnp.sum(mat * row, axis=1, keepdims=True)

    def times_column(mat, col):
        return jnp.sum(mat * col, axis=0, keepdims=True)

    def apply(mat, col):
        return row_times(mat, as_row(col))

    def dot(a, b):
        return jnp.sum(a * b, axis=0, keepdims=True)

    w_row, b_row = as_row(starts[0]), as_row(starts[1])
    coarse = coarse + row_times(inverse, w_row - times_column(g1, coarse))
    mu0 = row_times(inverse, b_row - times_column(g2, coarse))


    def residual_row(e, carry):
        at = pl.ds(e + 4, 1)
        r = st[at, :] - jnp.sum(coarse * img1[e], axis=0, keepdims=True)
        res[4, at, :] = r
        res[0, at, :] = r - jnp.sum(mu0 * vec[e], axis=0, keepdims=True)
        return carry

    lax.fori_loop(1, ROWS - 1, residual_row, 0, unroll=11)
    send_phase(g3_phases[1], wait_phase(g3_phases[0]))
    for i, base in enumerate((4, 1, 2)):
        res[i + 1] = operate(res[i]) - SHIFT * res[base]

    def moment_row(y, carry):
        b1, b2 = img1[y + DEPTH, :, 0:NX], img2[y]
        v1, a1 = (res[i, pl.ds(y + 8, 1), 0:NX] for i in (1, 2))
        terms = (b1 * v1, b1 * a1, b2 * a1)
        return tuple(total + fold(term) for total, term in zip(carry, terms))

    defl = lax.fori_loop(0, NY, moment_row, (zero16,) * 3, unroll=8)
    payload = zero16
    for i, total in enumerate(defl):
        payload = column(payload, i, total)
    inner = [res[i, 8:24, 0:NX] for i in (4, 1, 2, 3)]
    for i, (a, b) in enumerate(((0, 0), (0, 1), (1, 1), (1, 2), (2, 2), (2, 3))):
        total = jnp.sum(fold(inner[a] * inner[b]), axis=0, keepdims=True)
        total = jnp.sum(total, axis=1, keepdims=True)
        payload = jnp.where((lane8 == 3) & (sub16 == i), total, payload)

    def before_scalars():
        def row(y, carry):
            at = pl.ds(y + 8, 1)
            along = jnp.sum(coarse * vec[y + DEPTH, :, 0:NX], axis=0, keepdims=True)
            st[at, 0:NX] = nat[GUESS, at, 0:NX] + along
            return carry

        lax.fori_loop(0, NY, row, 0, unroll=4)
        send_phase(g3_phases[2], wait_phase(g3_phases[1]))
        for phase in (first_phases[2], g3_phases[0], g3_phases[1]):
            finish_sends(phase)

    def last_gram():
        kept["g3"] = unpack(wait_phase(g3_phases[2]), K)
        for phase in (g3_phases[2], *two_phases):
            finish_sends(phase)

    row = all_reduce(two_phases, pack(payload, 8)[0], (before_scalars, last_gram))

    g3 = kept["g3"]
    e = [pick(row, i) for i in range(3)]
    t_all = pick(row, 3)
    t = [t_all[i : i + 1, :] for i in range(6)]
    mu1 = apply(inverse, e[0])
    g2_1, g3_1 = apply(g2, mu1), apply(g3, mu1)
    defl2 = e[1] - g2_1
    mu2 = apply(inverse, defl2)
    m = [
        t[0],
        t[1],
        t[2],
        t[3] - dot(mu1, e[0]),
        t[4] - 2.0 * dot(mu1, e[1]) + dot(mu1, g2_1),
        t[5]
        - 2.0 * dot(mu1, e[2] - SHIFT * e[1])
        + dot(mu1, g3_1 - SHIFT * g2_1)
        - dot(mu2, defl2),
    ]

    def form(poly, shift):
        total = 0.0
        for i, a in enumerate(poly):
            for j, b in enumerate(poly):
                total = total + a * b * m[i + j + shift]
        return total

    one = jnp.ones((1, 1), f32)
    zero = jnp.zeros((1, 1), f32)
    r_poly = [one]
    y_poly = [zero]
    zeta = [zero, zero, zero]
    curv = prev_norm = one
    for turn in range(3):
        norm = form(r_poly, 0)
        r_image = form(r_poly, 1) + SHIFT * norm
        if turn == 0:
            y_poly = list(r_poly)
            curv = r_image
        else:
            ratio = norm / prev_norm
            y_poly = [a + ratio * b for a, b in zip(r_poly, y_poly + [zero])]
            curv = r_image - ratio * ratio * curv
        step_len = norm / curv
        for i, a in enumerate(y_poly):
            zeta[i] = zeta[i] + step_len * a
        y_image = [a + SHIFT * b for a, b in zip([zero] + y_poly, y_poly + [zero])]
        r_poly = [a - step_len * b for a, b in zip(r_poly + [zero], y_image)]
        prev_norm = norm

    along_w = zeta[1] * mu1 + zeta[2] * mu2
    along_b = zeta[2] * mu1
    res_b = (r_poly[2] - SHIFT * r_poly[3]) * mu1 + r_poly[3] * mu2
    res_bb = r_poly[3] * mu1

    def final_row(y, carry):
        w, b1, b2 = vec[y + DEPTH, :, 0:NX], img1[y + DEPTH, :, 0:NX], img2[y]
        at = pl.ds(y, 1)
        comb[0, at, :] = jnp.sum(along_w * w + along_b * b1, axis=0, keepdims=True)
        comb[1, at, :] = jnp.sum(res_b * b1 + res_bb * b2, axis=0, keepdims=True)
        return carry

    lax.fori_loop(0, NY, final_row, 0, unroll=16)
    p0, v1, a1, a2, r0 = (res[i, 8:24, 0:NX] for i in range(5))
    out[0] = (
        st[8:24, 0:NX] + (zeta[0] * p0 + zeta[1] * v1 + zeta[2] * a1) - comb[0]
    )
    out[1] = (
        r_poly[0] * r0 + (r_poly[1] * v1 + r_poly[2] * a1 + r_poly[3] * a2) - comb[1]
    )


def shards(right_side, first_guess, cell_mask, cond_east, cond_north, surface, recycled):
    sizes = tuple(lax.axis_size(axis) for axis in AXES)
    ny_dev, nzh, nx_dev, nzl, ncore = sizes
    na, nb, nc = nx_dev * ncore, ny_dev, nzh * nzl
    nd, ne = nx_dev * ny_dev, nzh * nzl * ncore
    vmem = pltpu.VMEM
    dma = pltpu.SemaphoreType.DMA
    both = pl.pallas_call(
        functools.partial(kernel, sizes),
        out_shape=jax.ShapeDtypeStruct((2, NY, NX), f32),
        in_specs=[pl.BlockSpec(memory_space=pl.ANY)] * 7,
        out_specs=pl.BlockSpec(memory_space=pltpu.VMEM),
        scratch_shapes=[
            vmem((ROWS, K, WIDE), f32),
            vmem((ROWS, K, WIDE), f32),
            vmem((NY, K, NX), f32),
            vmem((6, NAT, WIDE), f32),
            vmem((6, NAT, NX), f32),
            vmem((5, NAT, WIDE), f32),
            vmem((NAT, WIDE), f32),
            vmem((5, NAT, WIDE), f32),
            vmem((NY, NX), jnp.int32),
            vmem((2, K, 128), f32),
            vmem((6, K, 128), f32),
            vmem((2, NY, 128), f32),
            vmem((6, NY, 128), f32),
            vmem((3, 3, 8, 128), f32),
            vmem((2, na, 8, 128), f32),
            vmem((2, nb, 8, 128), f32),
            vmem((2, nc, 8, 128), f32),
            vmem((nd, 128), f32),
            vmem((ne, 128), f32),
            vmem((2, NY, NX), f32),
            vmem((2, 2, K, NX), f32),
            dma((22,)),
            dma((28,)),
            dma((28,)),
            dma((2, na)),
            dma((2, nb)),
            dma((2, nc)),
            dma((nd,)),
            dma((ne,)),
            dma((2, na)),
            dma((2, nb)),
            dma((2, nc)),
            dma((nd,)),
            dma((ne,)),
        ],
        compiler_params=pltpu.CompilerParams(collective_id=0, has_side_effects=True),
    )(right_side, first_guess, cell_mask, cond_east, cond_north, surface, recycled)
    return both[0], both[1]


def finer_mesh(mesh):
    return Mesh(mesh.devices.reshape(8, 3, 4, 4, 2), AXES)


def solution(mesh):
    in_specs = (P(LAT, LON),) * 6 + (P(None, LAT, LON),)
    out_specs = (P(LAT, LON), P(LAT, LON))
    return jax.shard_map(
        shards, mesh=finer_mesh(mesh), in_specs=in_specs, out_specs=out_specs, check_vma=False
    )
```
